16 devices in a mesh: rep: 1, dp: 16 (over x, y, z, core).
Axes of the slice: x: 2, y: 2, z: 2, core: 2. Of those that a mesh axis runs over, the one named last changes fastest.
Arguments:
- x: bfloat16 [16, 2048, 1280], P(('rep', 'dp'))
- dy: bfloat16 [16, 2048, 1280], P(('rep', 'dp'))
- wq: bfloat16 [2, 1280, 1024], replicated
- wk: bfloat16 [2, 1280, 256], replicated
- wv: bfloat16 [2, 1280, 256], replicated
- wo: bfloat16 [2, 1024, 1280], replicated
- w_gate: bfloat16 [2, 1280, 3584], replicated
- w_up: bfloat16 [2, 1280, 3584], replicated
- w_down: bfloat16 [2, 3584, 1280], replicated
- m_wq: float32 [2, 1280, 1024], replicated
- m_wk: float32 [2, 1280, 256], replicated
- m_wv: float32 [2, 1280, 256], replicated
- m_wo: float32 [2, 1024, 1280], replicated
- m_w_gate: float32 [2, 1280, 3584], replicated
- m_w_up: float32 [2, 1280, 3584], replicated
- m_w_down: float32 [2, 3584, 1280], replicated
- v_wq: float32 [2, 1280, 1024], replicated
- v_wk: float32 [2, 1280, 256], replicated
- v_wv: float32 [2, 1280, 256], replicated
- v_wo: float32 [2, 1024, 1280], replicated
- v_w_gate: float32 [2, 1280, 3584], replicated
- v_w_up: float32 [2, 1280, 3584], replicated
- v_w_down: float32 [2, 3584, 1280], replicated
Outputs:
- output 1: bfloat16 [2, 1280, 1024], P('rep')
- output 2: bfloat16 [2, 1280, 256], P('rep')
- output 3: bfloat16 [2, 1280, 256], P('rep')
- output 4: bfloat16 [2, 1024, 1280], P('rep')
- output 5: bfloat16 [2, 1280, 3584], P('rep')
- output 6: bfloat16 [2, 1280, 3584], P('rep')
- output 7: bfloat16 [2, 3584, 1280], P('rep')
- output 8: float32 [2, 1280, 1024], P('rep')
- output 9: float32 [2, 1280, 256], P('rep')
- output 10: float32 [2, 1280, 256], P('rep')
- output 11: float32 [2, 1024, 1280], P('rep')
- output 12: float32 [2, 1280, 3584], P('rep')
- output 13: float32 [2, 1280, 3584], P('rep')
- output 14: float32 [2, 3584, 1280], P('rep')
- output 15: float32 [2, 1280, 1024], P('rep')
- output 16: float32 [2, 1280, 256], P('rep')
- output 17: float32 [2, 1280, 256], P('rep')
- output 18: float32 [2, 1024, 1280], P('rep')
- output 19: float32 [2, 1280, 3584], P('rep')
- output 20: float32 [2, 1280, 3584], P('rep')
- output 21: float32 [2, 3584, 1280], P('rep')
All inputs are finite; a program needn't handle non-finite values.
Results may differ from the reference program's by a relative error of at most 0.0243.
Values are sent between devices in bfloat16 or wider.
A program may use at most 3.25 GiB of HBM per device.

```python
import jax
import jax.numpy as jnp
from jax import lax

SEQUENCES = 16
TOKENS = 2048
D = 1280
HEADS = 8
KV_HEADS = 2
HEAD = 128
FF = 3584
LAYERS = 2
THETA = 10000
NAMES = ("wq", "wk", "wv", "wo", "w_gate", "w_up", "w_down")
SHAPES = {
    "wq": (LAYERS, D, HEADS * HEAD),
    "wk": (LAYERS, D, KV_HEADS * HEAD),
    "wv": (LAYERS, D, KV_HEADS * HEAD),
    "wo": (LAYERS, HEADS * HEAD, D),
    "w_gate": (LAYERS, D, FF),
    "w_up": (LAYERS, D, FF),
    "w_down": (LAYERS, FF, D),
}


def bump(key, n, height):
    away = (jnp.arange(n, dtype=jnp.int32) - jax.random.randint(key, (), 0, n, jnp.int32)) % n
    return jnp.where(away < n // 8, height, 1.0)


def together(key, own, strength):
    shared = jax.random.normal(key, own.shape[1:], jnp.float32)
    return (own + strength * shared) * lax.rsqrt(1 + strength * strength)


def setup_inputs(seed: int = 0, part: int = 0) -> dict:
    kx, kdy, ka, kb, kz, kf, kh, kl, *keys = jax.random.split(jax.random.key(seed), 8 + 3 * len(NAMES))
    kx, kdy, ka, kb = (jax.random.fold_in(k, part) for k in (kx, kdy, ka, kb))
    kw, km, kv = (keys[i::3] for i in range(3))
    shape = (SEQUENCES, TOKENS, D)
    much_x, much_dy = jax.random.uniform(kz, (2,), jnp.float32, 0.0, 1.0)
    loud = 2.0 ** jax.random.uniform(jax.random.fold_in(kz, 1), (), jnp.float32, -1.0, 2.0)
    layers = 2.0 ** jax.random.uniform(kl, (LAYERS, 1, 1), jnp.float32, -1.0, 1.0)
    times = {"wq": 1.0, "wk": 1.0, "wv": 2.0, "wo": layers, "w_gate": 1.0, "w_up": bump(kh, FF, 4.0), "w_down": layers}
    x = together(ka, jax.random.normal(kx, shape, jnp.float32), much_x) * bump(kf, D, 4.0)
    dy = together(kb, jax.random.normal(kdy, shape, jnp.float32), much_dy)
    drawn = {"x": x.astype(jnp.bfloat16), "dy": (loud * dy * (SEQUENCES * TOKENS) ** -0.5).astype(jnp.bfloat16)}
    for key, name in zip(kw, NAMES, strict=True):
        drawn[name] = (jax.random.normal(key, SHAPES[name], jnp.float32) * SHAPES[name][1] ** -0.5 * times[name]).astype(jnp.bfloat16)
    for key, name in zip(km, NAMES, strict=True):
        drawn[f"m_{name}"] = 0.1 * jax.random.normal(key, SHAPES[name], jnp.float32)
    for key, name in zip(kv, NAMES, strict=True):
        drawn[f"v_{name}"] = jax.random.uniform(key, SHAPES[name], jnp.float32, 0.02, 0.06)
    return drawn


def matmul(a, w):
    return jnp.dot(a, w, preferred_element_type=jnp.float32).astype(jnp.bfloat16)


def normed(h):
    wide = h.astype(jnp.float32)
    scale = lax.rsqrt(jnp.mean(wide**2, -1, keepdims=True) + 1e-6)
    return (wide * scale).astype(jnp.bfloat16)


def turned(t, theta):
    half = t.shape[-1] // 2
    angle = jnp.arange(t.shape[0], dtype=jnp.float32)[:, None] * theta ** (-jnp.arange(half, dtype=jnp.float32) / half)
    cos, sin = jnp.cos(angle)[:, None], jnp.sin(angle)[:, None]
    a, b = t[..., :half].astype(jnp.float32), t[..., half:].astype(jnp.float32)
    return jnp.concatenate([a * cos - b * sin, b * cos + a * sin], -1).astype(jnp.bfloat16)


def seen_by(q, k, v):
    tokens, kv = q.shape[0], k.shape[1]
    q = q.reshape(tokens, kv, -1, q.shape[-1])
    scores = jnp.einsum("tgsd,ugd->gstu", q.astype(jnp.float32), k.astype(jnp.float32)) * q.shape[-1] ** -0.5
    place = jnp.arange(tokens)
    weights = jax.nn.softmax(jnp.where(place[:, None] >= place, scores, -jnp.inf), -1).astype(jnp.bfloat16)
    return jnp.einsum("gstu,ugd->tgsd", weights.astype(jnp.float32), v.astype(jnp.float32)).astype(jnp.bfloat16).reshape(tokens, -1)


def layer(h, w):
    a = normed(h)
    q, k = (turned(matmul(a, w[name]).reshape(h.shape[0], -1, HEAD), THETA) for name in ("wq", "wk"))
    h = h + matmul(seen_by(q, k, matmul(a, w["wv"]).reshape(h.shape[0], -1, HEAD)), w["wo"])
    b = normed(h)
    gate = jnp.dot(b, w["w_gate"], preferred_element_type=jnp.float32)
    up = jnp.dot(b, w["w_up"], preferred_element_type=jnp.float32)
    return h + matmul((jax.nn.silu(gate) * up).astype(jnp.bfloat16), w["w_down"])


def adamw(w, m, v, g):
    m = 0.9 * m + 0.1 * g
    v = 0.95 * v + 0.05 * g * g
    step = m * lax.rsqrt(v + 1e-8) + 0.1 * w
    return (w - 0.02 * step).astype(jnp.bfloat16), m, v


def clipped(gradients, sum_of_squares, count):
    factor = jnp.minimum(1.0, 0.5 * lax.rsqrt(sum_of_squares / count + 1e-30))
    return [g * factor for g in gradients]


def stack(weights, h):
    return lax.scan(lambda h, w: (layer(h, w), None), h, weights)[0]


def reference(x, dy, wq, wk, wv, wo, w_gate, w_up, w_down, m_wq, m_wk, m_wv, m_wo, m_w_gate, m_w_up, m_w_down, v_wq, v_wk, v_wv, v_wo, v_w_gate, v_w_up, v_w_down):
    weights = dict(zip(NAMES, (wq, wk, wv, wo, w_gate, w_up, w_down), strict=True))

    def take(so_far, sequence):
        h, by_y = sequence
        _, back = jax.vjp(stack, weights, h)
        by_weights, by_h = back(by_y)
        return jax.tree.map(lambda total, term: total + term.astype(jnp.float32), so_far, by_weights), by_h

    none_yet = {name: jnp.zeros(w.shape, jnp.float32) for name, w in weights.items()}
    by_weights, by_x = lax.scan(take, none_yet, (x, dy))
    gradients = [by_weights[name].astype(jnp.bfloat16).astype(jnp.float32) for name in NAMES]
    gradients = clipped(gradients, sum(jnp.sum(g * g) for g in gradients), sum(g.size for g in gradients))
    first = (m_wq, m_wk, m_wv, m_wo, m_w_gate, m_w_up, m_w_down)
    second = (v_wq, v_wk, v_wv, v_wo, v_w_gate, v_w_up, v_w_down)
    new = [adamw(weights[name].astype(jnp.float32), m, v, g) for name, m, v, g in zip(NAMES, first, second, gradients, strict=True)]
    return tuple(one[which] for which in range(3) for one in new)
```

```python
import functools

import jax
import jax.numpy as jnp
from jax import lax
from jax.experimental import pallas as pl
from jax.experimental.pallas import tpu as pltpu
from jax.sharding import PartitionSpec as P

NAMES = ("wq", "wk", "wv", "wo", "w_gate", "w_up", "w_down")
HEAD = 128
THETA = 10000
NEG = -1e30
HIDDEN = 2 * NEG
LOG2E = 1.4426950408889634
BF, F32 = jnp.bfloat16, jnp.float32
MIB = 2**20


def _dot(a, b, ca, cb):
    return lax.dot_general(a, b, (((ca,), (cb,)), ((), ())), preferred_element_type=F32)


def shape_of(shape, dtype=BF):
    return jax.ShapeDtypeStruct(shape, dtype)


def rows(bt, width):
    return pl.BlockSpec((bt, width), lambda i, *_: (i, 0))


def whole(*shape):
    return pl.BlockSpec(shape, lambda *_: (0,) * len(shape), pipeline_mode=pl.Buffered(1))


def call(body, name, grid, ins, in_specs, outs, out_specs, scratch=(), flops=0, limit=40):
    size = lambda a: a.size * jnp.dtype(a.dtype).itemsize
    return pl.pallas_call(
        body,
        name=name,
        grid=grid,
        in_specs=in_specs,
        out_specs=out_specs,
        out_shape=outs,
        scratch_shapes=scratch,
        compiler_params=pltpu.CompilerParams(vmem_limit_bytes=int(limit * MIB)),
        cost_estimate=pl.CostEstimate(flops=int(flops), transcendentals=0, bytes_accessed=sum(map(size, ins)) + sum(map(size, outs))),
    )(*ins)


def scale_of(wide):
    return lax.rsqrt(jnp.mean(wide * wide, -1, keepdims=True) + 1e-6)


def through_norm(by_out, wide):
    scale = scale_of(wide)
    return (scale * by_out - wide * (scale * scale * scale * jnp.mean(by_out * wide, -1, keepdims=True))).astype(BF)


def added(a, b):
    return (a.astype(F32) + b.astype(F32)).astype(BF)


def turn(t, cos, sin):
    return t * cos + pltpu.roll(t, HEAD // 2, 1) * sin


def angles(tokens):
    half = HEAD // 2
    angle = jnp.arange(tokens, dtype=F32)[:, None] * THETA ** (-jnp.arange(half, dtype=F32) / half)
    cos, sin = jnp.cos(angle), jnp.sin(angle)
    return jnp.concatenate([cos, cos], 1), jnp.concatenate([-sin, sin], 1)


def qkv(h, wq, wk, wv, cos, sin, bt=512):
    (t, d), nq, nk = h.shape, wq.shape[1], wk.shape[1]

    def body(h, wq, wk, wv, cos, sin, a, q, k, v):
        wide = h[...].astype(F32)
        n = (wide * scale_of(wide)).astype(BF)
        a[...] = n
        c, s = cos[...], sin[...]
        for w, out in ((wq, q), (wk, k)):
            for at in range(0, w.shape[1], 256):
                r = _dot(n, w[:, at : at + 256], 1, 0).astype(BF).astype(F32)
                for x in range(0, 256, HEAD):
                    out[:, at + x : at + x + HEAD] = turn(r[:, x : x + HEAD], c, s).astype(BF)
        v[...] = _dot(n, wv[...], 1, 0).astype(BF)

    return call(body, "qkv", (t // bt,), (h, wq, wk, wv, cos, sin),
                [rows(bt, d), whole(d, nq), whole(d, nk), whole(d, nk), rows(bt, HEAD), rows(bt, HEAD)],
                [shape_of((t, d)), shape_of((t, nq)), shape_of((t, nk)), shape_of((t, nk))],
                [rows(bt, d), rows(bt, nq), rows(bt, nk), rows(bt, nk)], flops=2 * t * d * (nq + 2 * nk), limit=24)


def _gap(bk, cols, bq):
    return lax.rem(lax.broadcasted_iota(jnp.int32, (bk, cols), 1), bq) - lax.broadcasted_iota(jnp.int32, (bk, cols), 0)


def attend(q, k, v, bq=512, bk=512):
    t, nq = q.shape
    heads, kv = nq // HEAD, k.shape[1] // HEAD
    g = heads // kv
    e, scale = HEAD**-0.5 * LOG2E, HEAD**-0.5

    def body(q, k, v, out, lse, top_s, mix_s, gap_s):
        iq = pl.program_id(0)

        @pl.when(iq == 0)
        def _():
            gap_s[...] = _gap(bk, bq, bq)

        top_s[...] = jnp.full(top_s.shape, NEG, F32)
        mix_s[...] = jnp.zeros(mix_s.shape, F32)
        ones = jnp.ones((8, bk), BF)

        def block(j, masked):
            here = pl.ds(pl.multiple_of(j * bk, bk), bk)
            keys = [k[here, i * HEAD : (i + 1) * HEAD] for i in range(kv)]
            values = [jnp.concatenate([v[here, i * HEAD : (i + 1) * HEAD].T, ones], axis=0) for i in range(kv)]
            scores = [_dot(keys[n // g], q[:, n * HEAD : (n + 1) * HEAD], 1, 1) for n in range(heads)]
            ok = gap_s[...] >= (j * bk - iq * bq) if masked else None
            weights, keeps = [], []
            for n, s in enumerate(scores):
                if masked:
                    s = jnp.where(ok, s, HIDDEN)
                old = top_s[n : n + 1, :]
                top = jnp.maximum(old, s.max(axis=0, keepdims=True))
                top_s[n : n + 1, :] = top
                weights.append(jnp.exp2((s - top) * e).astype(BF))
                keeps.append(jnp.exp2((old - top) * e))
            for n, (p, keep) in enumerate(zip(weights, keeps)):
                mix_s[n] = mix_s[n] * keep + _dot(values[n // g], p, 1, 0)

        clear = lax.div(iq * bq + 1, bk)
        lax.fori_loop(0, clear, lambda j, _: block(j, False), None)
        lax.fori_loop(clear, lax.div(iq * bq + bq - 1 + bk, bk), lambda j, _: block(j, True), None)
        for n in range(heads):
            total = mix_s[n, HEAD : HEAD + 1, :]
            out[:, n * HEAD : (n + 1) * HEAD] = (mix_s[n, :HEAD, :] * (1 / total)).T.astype(BF)
            lse[n : n + 1, :] = top_s[n : n + 1, :] * scale + jnp.log(total)

    return call(body, "attend", (t // bq,), (q, k, v), [rows(bq, nq), whole(*k.shape), whole(*v.shape)],
                [shape_of((t, nq)), shape_of((heads, t), F32)], [rows(bq, nq), pl.BlockSpec((heads, bq), lambda i: (0, i))],
                [pltpu.VMEM((heads, bq), F32), pltpu.VMEM((heads, HEAD + 8, bq), F32), pltpu.VMEM((bk, bq), jnp.int32)],
                flops=4 * heads * t * t * HEAD, limit=ATT_LIMIT)


ATT_LIMIT = 32


def silu_parts(gate):
    sg = 1 / (1 + jnp.exp(-gate))
    return sg


def post(h, attn, wo, wg, wu, bt=256, step=512):
    (t, d), f = h.shape, wg.shape[1]

    def body(h, attn, wo, wg, wu, h1, b, gate, up, p):
        s = added(h[...], _dot(attn[...], wo[...], 1, 0).astype(BF))
        h1[...] = s
        wide = s.astype(F32)
        n = (wide * scale_of(wide)).astype(BF)
        b[...] = n
        for at in range(0, f, step):
            x = _dot(n, wg[:, at : at + step], 1, 0)
            y = _dot(n, wu[:, at : at + step], 1, 0)
            gate[:, at : at + step] = x
            up[:, at : at + step] = y
            p[:, at : at + step] = (jax.nn.silu(x) * y).astype(BF)

    return call(body, "post", (t // bt,), (h, attn, wo, wg, wu),
                [rows(bt, d), rows(bt, attn.shape[1]), whole(*wo.shape), whole(d, f), whole(d, f)],
                [shape_of((t, d)), shape_of((t, d)), shape_of((t, f), F32), shape_of((t, f), F32), shape_of((t, f))],
                [rows(bt, d), rows(bt, d), rows(bt, f), rows(bt, f), rows(bt, f)], flops=2 * t * d * (2 * f + wo.shape[0]), limit=POST_LIMIT)


POST_LIMIT = 48


def down(h1, p, wd, bt=512):
    (t, d), f = h1.shape, p.shape[1]

    def body(h1, p, wd, out):
        out[...] = added(h1[...], _dot(p[...], wd[...], 1, 0).astype(BF))

    return call(body, "down", (t // bt,), (h1, p, wd), [rows(bt, d), rows(bt, f), whole(f, d)], [shape_of((t, d))], [rows(bt, d)],
                flops=2 * t * d * f, limit=28)[0]


def _through_gate(by_p, x, y):
    s = 1 / (1 + jnp.exp(-x))
    act = x * s
    return (by_p * y * (s + act * (1 - s))).astype(BF), (by_p * act).astype(BF)


def gate_bwd(dy, wd, gate, up, bt=256, step=512):
    (t, d), f = dy.shape, wd.shape[0]

    def body(dy, wd, gate, up, by_gate, by_up):
        x = dy[...]
        for at in range(0, f, step):
            by_p = _dot(x, wd[at : at + step, :], 1, 1).astype(BF).astype(F32)
            by_gate[:, at : at + step], by_up[:, at : at + step] = _through_gate(by_p, gate[:, at : at + step], up[:, at : at + step])

    return call(body, "gate_bwd", (t // bt,), (dy, wd, gate, up), [rows(bt, d), whole(f, d), rows(bt, f), rows(bt, f)],
                [shape_of((t, f)), shape_of((t, f))], [rows(bt, f), rows(bt, f)], flops=2 * t * d * f, limit=36)


def turnaround(h, attn, dy, wo, wg, wu, wd, bt=256, step=512):
    (t, d), f = h.shape, wg.shape[1]

    def body(h, attn, dy, wo, wg, wu, wd, h1, b, p, by_gate, by_up):
        s = added(h[...], _dot(attn[...], wo[...], 1, 0).astype(BF))
        h1[...] = s
        wide = s.astype(F32)
        n = (wide * scale_of(wide)).astype(BF)
        b[...] = n
        back = dy[...]
        for at in range(0, f, step):
            x = _dot(n, wg[:, at : at + step], 1, 0)
            y = _dot(n, wu[:, at : at + step], 1, 0)
            p[:, at : at + step] = (jax.nn.silu(x) * y).astype(BF)
            by_p = _dot(back, wd[at : at + step, :], 1, 1).astype(BF).astype(F32)
            by_gate[:, at : at + step], by_up[:, at : at + step] = _through_gate(by_p, x, y)

    return call(body, "turnaround", (t // bt,), (h, attn, dy, wo, wg, wu, wd),
                [rows(bt, d), rows(bt, attn.shape[1]), rows(bt, d), whole(*wo.shape), whole(d, f), whole(d, f), whole(f, d)],
                [shape_of((t, d)), shape_of((t, d)), shape_of((t, f)), shape_of((t, f)), shape_of((t, f))],
                [rows(bt, d), rows(bt, d), rows(bt, f), rows(bt, f), rows(bt, f)], flops=2 * t * d * (3 * f + wo.shape[0]), limit=TURN_LIMIT)


TURN_LIMIT = 52


def ffn_bwd(by_gate, by_up, wg, wu, h1, dy, wo, bt=256):
    (t, f), d, n = by_gate.shape, h1.shape[1], wo.shape[0]

    def body(by_gate, by_up, wg, wu, h1, dy, wo, by_h, by_attn):
        by_b = added(_dot(by_gate[...], wg[...], 1, 1).astype(BF), _dot(by_up[...], wu[...], 1, 1).astype(BF))
        total = added(dy[...], through_norm(by_b.astype(F32), h1[...].astype(F32)))
        by_h[...] = total
        by_attn[...] = _dot(total, wo[...], 1, 1).astype(BF)

    return call(body, "ffn_bwd", (t // bt,), (by_gate, by_up, wg, wu, h1, dy, wo),
                [rows(bt, f), rows(bt, f), whole(d, f), whole(d, f), rows(bt, d), rows(bt, d), whole(n, d)],
                [shape_of((t, d)), shape_of((t, n))], [rows(bt, d), rows(bt, n)], flops=2 * t * d * (2 * f + n), limit=FFN_LIMIT)


FFN_LIMIT = 40


def attend_bwd(q, k, v, out, by_out, lse, cos, sin, bq=256, bk=512):
    t, nq = q.shape
    heads, kv = nq // HEAD, k.shape[1] // HEAD
    g = heads // kv
    e, scale = HEAD**-0.5 * LOG2E, HEAD**-0.5
    pair = 2
    wide = pair * bq
    strips = range(0, heads, pair)
    width = (g + 2) * HEAD

    def laid(ref, n):
        return jnp.concatenate([ref[:, (n + x) * HEAD : (n + x + 1) * HEAD] for x in range(pair)], axis=0)

    def body(q, k, v, out, by_out, lse, cos, sin, *rest):
        res, (dq_s, dk_s, dv_s, gap_s) = rest[:kv], rest[kv:]
        iq = pl.program_id(0)

        @pl.when(iq == 0)
        def _():
            gap_s[...] = _gap(bk, wide, bq)
            dk_s[...] = jnp.zeros_like(dk_s)
            dv_s[...] = jnp.zeros_like(dv_s)

        dq_s[...] = jnp.zeros_like(dq_s)
        lses = [jnp.concatenate([lse[n + x : n + x + 1, :] for x in range(pair)], axis=1) * LOG2E for n in strips]
        deltas = [(laid(by_out, n).astype(F32) * laid(out, n).astype(F32)).T.sum(axis=0, keepdims=True) for n in strips]

        def block(j, masked):
            here = pl.ds(pl.multiple_of(j * bk, bk), bk)
            qs, dos = [laid(q, n) for n in strips], [laid(by_out, n) for n in strips]
            keys = [k[here, i * HEAD : (i + 1) * HEAD] for i in range(kv)]
            values = [v[here, i * HEAD : (i + 1) * HEAD] for i in range(kv)]
            scores = [_dot(keys[n // g], x, 1, 1) for n, x in zip(strips, qs)]
            dps = [_dot(values[n // g], x, 1, 1) for n, x in zip(strips, dos)]
            ok = gap_s[...] >= (j * bk - iq * bq) if masked else None
            for s, n in enumerate(strips):
                i = n // g
                p = jnp.exp2(scores[s] * e - lses[s])
                if masked:
                    p = jnp.where(ok, p, 0.0)
                ds = (p * (dps[s] - deltas[s])).astype(BF)
                dv_s[i, here, :] += _dot(p.astype(BF), dos[s], 1, 0)
                dk_s[i, here, :] += _dot(ds, qs[s], 1, 0)
                dq_s[s] += _dot(keys[i].T, ds, 1, 0)

        clear = lax.div(iq * bq + 1, bk)
        lax.fori_loop(0, clear, lambda j, _: block(j, False), None)
        lax.fori_loop(clear, lax.div(iq * bq + bq - 1 + bk, bk), lambda j, _: block(j, True), None)
        at = pl.ds(pl.multiple_of(iq * bq, bq), bq)
        c, s_ = cos[at, :], -sin[at, :]
        for s, n in enumerate(strips):
            got = (dq_s[s] * scale).T.astype(BF).astype(F32)
            for x in range(pair):
                m = (n + x) % g
                res[(n + x) // g][at, m * HEAD : (m + 1) * HEAD] = turn(got[x * bq : (x + 1) * bq], c, s_).astype(BF)

        @pl.when(iq == pl.num_programs(0) - 1)
        def _():
            for i in range(kv):
                for r in range(0, t, bk):
                    part = pl.ds(r, bk)
                    got = (dk_s[i, part, :] * scale).astype(BF).astype(F32)
                    res[i][part, g * HEAD : (g + 1) * HEAD] = turn(got, cos[part, :], -sin[part, :]).astype(BF)
                    res[i][part, (g + 1) * HEAD :] = dv_s[i, part, :].astype(BF)

    return call(body, "attend_bwd", (t // bq,), (q, k, v, out, by_out, lse, cos, sin),
                [rows(bq, nq), whole(*k.shape), whole(*v.shape), rows(bq, nq), rows(bq, nq), pl.BlockSpec((heads, bq), lambda i: (0, i)),
                 whole(t, HEAD), whole(t, HEAD)],
                [shape_of((t, width))] * kv, [whole(t, width)] * kv,
                [pltpu.VMEM((heads // pair, HEAD, wide), F32), pltpu.VMEM((kv, t, HEAD), F32), pltpu.VMEM((kv, t, HEAD), F32),
                 pltpu.VMEM((bk, wide), jnp.int32)],
                flops=10 * heads * t * t * HEAD, limit=AB_LIMIT)


AB_LIMIT = 40


def qkv_bwd(by_qkv, wq, wk, wv, h, by_h1, bt=512):
    (t, d), kv = h.shape, len(by_qkv)
    nq = wq.shape[1] // kv

    def body(*refs):
        parts, (wq, wk, wv, h, by_h1, out) = refs[:kv], refs[kv:]
        got = [sum(_dot(p[:, a:b], w[:, i * (b - a) : (i + 1) * (b - a)], 1, 1) for i, p in enumerate(parts)).astype(BF).astype(F32)
               for w, a, b in ((wq, 0, nq), (wk, nq, nq + HEAD), (wv, nq + HEAD, nq + 2 * HEAD))]
        by_a = (got[0] + got[1]).astype(BF).astype(F32) + got[2]
        out[...] = added(by_h1[...], through_norm(by_a.astype(BF).astype(F32), h[...].astype(F32)))

    return call(body, "qkv_bwd", (t // bt,), (*by_qkv, wq, wk, wv, h, by_h1),
                [rows(bt, nq + 2 * HEAD)] * kv + [whole(*wq.shape), whole(*wk.shape), whole(*wv.shape), rows(bt, d), rows(bt, d)],
                [shape_of((t, d))], [rows(bt, d)], flops=2 * t * d * (kv * (nq + 2 * HEAD)), limit=24)[0]


def adamw(w, m, v, g):
    m = 0.9 * m + 0.1 * g
    v = 0.95 * v + 0.05 * g * g
    step = m * lax.rsqrt(v + 1e-8) + 0.1 * w
    return (w - 0.02 * step).astype(BF), m, v


def clipped(gradients, sum_of_squares, count):
    factor = jnp.minimum(1.0, 0.5 * lax.rsqrt(sum_of_squares / count + 1e-30))
    return [g * factor for g in gradients]


def product(a, b):
    return _dot(a, b, 0, 0).astype(BF)


def solution(mesh):
    def step(x, dy, *arrays):
        weights, m, v = (arrays[i : i + 7] for i in (0, 7, 14))
        layers = weights[0].shape[0]
        cos, sin = angles(x.shape[1])
        h, kept, mine = x[0], [], [None] * layers
        for number in range(layers):
            wq, wk, wv, wo, wg, wu, wd = (w[number] for w in weights)
            a, q, k, v_ = qkv(h, wq, wk, wv, cos, sin)
            attn, lse = attend(q, k, v_)
            if number < layers - 1:
                h1, b, gate, up, p = post(h, attn, wo, wg, wu)
                kept.append((h, a, q, k, v_, attn, lse, h1, b, gate, up, p))
                h = down(h1, p, wd)
        by_h = dy[0]
        for number in reversed(range(layers)):
            wq, wk, wv, wo, wg, wu, wd = (w[number] for w in weights)
            if number == layers - 1:
                h1, b, p, by_gate, by_up = turnaround(h, attn, by_h, wo, wg, wu, wd)
            else:
                h, a, q, k, v_, attn, lse, h1, b, gate, up, p = kept[number]
                by_gate, by_up = gate_bwd(by_h, wd, gate, up)
            g_down = product(p, by_h)
            g_gate, g_up = product(b, by_gate), product(b, by_up)
            by_h1, by_attn = ffn_bwd(by_gate, by_up, wg, wu, h1, by_h, wo)
            g_o = product(attn, by_h1)
            by_qkv = attend_bwd(q, k, v_, attn, by_attn, lse, cos, sin)
            nq = by_qkv[0].shape[1] - 2 * HEAD
            g_qkv = [product(a, part) for part in by_qkv]
            g_q = jnp.concatenate([g[:, :nq] for g in g_qkv], 1)
            g_k = jnp.concatenate([g[:, nq : nq + HEAD] for g in g_qkv], 1)
            g_v = jnp.concatenate([g[:, nq + HEAD :] for g in g_qkv], 1)
            mine[number] = [lax.psum(g, "dp") for g in (g_q, g_k, g_v, g_o, g_gate, g_up, g_down)]
            if number:
                by_h = qkv_bwd(by_qkv, wq, wk, wv, h, by_h1)
        gradients = [jnp.stack([mine[number][i] for number in range(layers)]).astype(F32) for i in range(7)]
        gradients = clipped(gradients, sum(jnp.sum(g * g) for g in gradients), sum(g.size for g in gradients))
        new = [adamw(w.astype(F32), m, v, g) for w, m, v, g in zip(weights, m, v, gradients, strict=True)]
        return tuple(one[which] for which in range(3) for one in new)

    states, all_of = P(("rep", "dp"), None, None), P(None, None, None)
    return jax.shard_map(step, mesh=mesh, in_specs=(states, states) + (all_of,) * 21, out_specs=(P("rep", None, None),) * 21, check_vma=False)
```

```python
import itertools

import jax
import jax.numpy as jnp
from jax import lax
from jax.experimental import pallas as pl
from jax.experimental.pallas import tpu as pltpu
from jax.sharding import PartitionSpec as P

NAMES = ("wq", "wk", "wv", "wo", "w_gate", "w_up", "w_down")
HEAD = 128
THETA = 10000
NEG = -1e30
HIDDEN = 2 * NEG
LOG2E = 1.4426950408889634
BF, F32 = jnp.bfloat16, jnp.float32
MIB = 2**20


def _dot(a, b, ca, cb):
    return lax.dot_general(a, b, (((ca,), (cb,)), ((), ())), preferred_element_type=F32)


def shape_of(shape, dtype=BF):
    return jax.ShapeDtypeStruct(shape, dtype)


def rows(bt, width):
    return pl.BlockSpec((bt, width), lambda i, *_: (i, 0))


def whole(*shape):
    return pl.BlockSpec(shape, lambda *_: (0,) * len(shape), pipeline_mode=pl.Buffered(1))


def layer_of(number, *shape):
    return pl.BlockSpec((None, *shape), lambda *_: (number,) + (0,) * len(shape), pipeline_mode=pl.Buffered(1))


IN_HBM = pl.BlockSpec(memory_space=pltpu.HBM)


def bit(me, axis):
    return (me // axis) % 2


def across(me, axes):
    return me + sum(axis * (1 - 2 * bit(me, axis)) for axis in axes)


CORE = (1,)


class Send:
    def __init__(self, array, shape, copies):
        self.array, self.result, self.copies = array, shape_of(shape, array.dtype), copies


def everything(me):
    return ()


def to_core(array, shape=None, part=everything):
    return Send(array, shape or array.shape, [(part, everything, CORE)])


def place(ref, at):
    return ref.at[at] if at else ref


def call(body, name, grid, ins, in_specs, outs, out_specs, scratch=(), flops=0, limit=40, sends=(), ids=None, eager=False, aliases={}, after=()):
    if after:
        inner, kept = body, len(ins)
        body = lambda *refs: inner(*refs[:kept], *refs[kept + len(after) :])
        ins, in_specs = (*ins, *after), [*in_specs, *[IN_HBM] * len(after)]
    size = lambda a: a.size * jnp.dtype(a.dtype).itemsize
    cost = pl.CostEstimate(flops=int(flops), transcendentals=0, bytes_accessed=sum(map(size, ins)) + sum(map(size, outs)))
    params = dict(vmem_limit_bytes=60 * MIB)
    if not sends:
        return pl.pallas_call(body, name=name, grid=grid, in_specs=in_specs, out_specs=out_specs, out_shape=outs, scratch_shapes=scratch,
                              input_output_aliases=aliases, compiler_params=pltpu.CompilerParams(**params), cost_estimate=cost)(*ins)
    n_in, n_out, n_s = len(ins), len(outs), len(sends)
    copies = [(s, c) for s, send in enumerate(sends) for c in send.copies]
    partners = sorted({c[2] for _, c in copies})

    def both(*refs):
        given, sources = refs[:n_in], refs[n_in : n_in + n_s]
        refs = refs[n_in + n_s :]
        made, landed, rest = refs[:n_out], refs[n_out : n_out + n_s], refs[n_out + n_s :]
        rest, (out_sem, in_sem) = rest[:-2], rest[-2:]
        me = lax.axis_index("dp")
        barrier = pltpu.get_barrier_semaphore()
        moves = [pltpu.make_async_remote_copy(place(sources[s], a(me)), place(landed[s], b(me)), out_sem.at[n], in_sem.at[n],
                                              device_id={"dp": across(me, axes)}, device_id_type=pl.DeviceIdType.MESH)
                 for n, (s, (a, b, axes)) in enumerate(copies)]
        step, last = pl.program_id(0), grid[0] - 1

        def greet():
            for axes in partners:
                pl.semaphore_signal(barrier, 1, device_id={"dp": across(me, axes)}, device_id_type=pl.DeviceIdType.MESH)

        def begin():
            pl.semaphore_wait(barrier, len(partners))
            for move in moves:
                move.start()

        @pl.when(step == 0)
        def _():
            greet()
            if eager or last == 0:
                begin()

        if body is not None:
            body(*given, *made, *rest)
        if not (eager or last == 0):

            @pl.when(step == 0)
            def _():
                begin()

        @pl.when(step == last)
        def _():
            for move in moves:
                move.wait()

    got = pl.pallas_call(both, name=name, grid=grid, in_specs=[*in_specs, *[IN_HBM] * n_s], out_specs=[*out_specs, *[IN_HBM] * n_s],
                         out_shape=[*outs, *[send.result for send in sends]],
                         scratch_shapes=[*scratch, pltpu.SemaphoreType.DMA((len(copies),)), pltpu.SemaphoreType.DMA((len(copies),))],
                         compiler_params=pltpu.CompilerParams(collective_id=next(ids), has_side_effects=True, **params),
                         cost_estimate=cost)(*ins, *[send.array for send in sends])
    return got[:n_out], got[n_out:]


def scale_of(wide):
    return lax.rsqrt(jnp.mean(wide * wide, -1, keepdims=True) + 1e-6)


def through_norm(by_out, wide):
    scale = scale_of(wide)
    return (scale * by_out - wide * (scale * scale * scale * jnp.mean(by_out * wide, -1, keepdims=True))).astype(BF)


def added(a, b):
    return (a.astype(F32) + b.astype(F32)).astype(BF)


def turn(t, cos, sin):
    return t * cos + pltpu.roll(t, HEAD // 2, 1) * sin


def angles(tokens):
    half = HEAD // 2
    angle = jnp.arange(tokens, dtype=F32)[:, None] * THETA ** (-jnp.arange(half, dtype=F32) / half)
    cos, sin = jnp.cos(angle), jnp.sin(angle)
    return jnp.concatenate([cos, cos], 1), jnp.concatenate([-sin, sin], 1)


def qkv(h, number, wq, wk, wv, cos, sin, bt=512):
    (t, d), nq, nk = h.shape, wq.shape[2], wk.shape[2]

    def body(h, wq, wk, wv, cos, sin, a, q, k, v):
        wide = h[...].astype(F32)
        n = (wide * scale_of(wide)).astype(BF)
        a[...] = n
        c, s = cos[...], sin[...]
        for w, out in ((wq, q), (wk, k)):
            for at in range(0, w.shape[1], 256):
                r = _dot(n, w[:, at : at + 256], 1, 0).astype(BF).astype(F32)
                for x in range(0, 256, HEAD):
                    out[:, at + x : at + x + HEAD] = turn(r[:, x : x + HEAD], c, s).astype(BF)
        v[...] = _dot(n, wv[...], 1, 0).astype(BF)

    return call(body, "qkv", (t // bt,), (h, wq, wk, wv, cos, sin),
                [rows(bt, d), layer_of(number, d, nq), layer_of(number, d, nk), layer_of(number, d, nk), rows(bt, HEAD), rows(bt, HEAD)],
                [shape_of((t, d)), shape_of((t, nq)), shape_of((t, nk)), shape_of((t, nk))],
                [rows(bt, d), rows(bt, nq), rows(bt, nk), rows(bt, nk)], flops=2 * t * d * (nq + 2 * nk), limit=24)


def _gap(bk, cols, bq):
    return lax.rem(lax.broadcasted_iota(jnp.int32, (bk, cols), 1), bq) - lax.broadcasted_iota(jnp.int32, (bk, cols), 0)


def attend(q, k, v, bq=512, bk=512, **more):
    t, nq = q.shape
    heads, kv = nq // HEAD, k.shape[1] // HEAD
    g = heads // kv
    e, scale = HEAD**-0.5 * LOG2E, HEAD**-0.5

    def body(q, k, v, out, lse, top_s, mix_s, gap_s):
        iq = pl.program_id(0)

        @pl.when(iq == 0)
        def _():
            gap_s[...] = _gap(bk, bq, bq)

        top_s[...] = jnp.full(top_s.shape, NEG, F32)
        mix_s[...] = jnp.zeros(mix_s.shape, F32)
        ones = jnp.ones((8, bk), BF)

        def block(j, masked):
            here = pl.ds(pl.multiple_of(j * bk, bk), bk)
            keys = [k[here, i * HEAD : (i + 1) * HEAD] for i in range(kv)]
            values = [jnp.concatenate([v[here, i * HEAD : (i + 1) * HEAD].T, ones], axis=0) for i in range(kv)]
            scores = [_dot(keys[n // g], q[:, n * HEAD : (n + 1) * HEAD], 1, 1) for n in range(heads)]
            ok = gap_s[...] >= (j * bk - iq * bq) if masked else None
            weights, keeps = [], []
            for n, s in enumerate(scores):
                if masked:
                    s = jnp.where(ok, s, HIDDEN)
                old = top_s[n : n + 1, :]
                top = jnp.maximum(old, s.max(axis=0, keepdims=True))
                top_s[n : n + 1, :] = top
                weights.append(jnp.exp2((s - top) * e).astype(BF))
                keeps.append(jnp.exp2((old - top) * e))
            for n, (p, keep) in enumerate(zip(weights, keeps)):
                mix_s[n] = mix_s[n] * keep + _dot(values[n // g], p, 1, 0)

        clear = lax.div(iq * bq + 1, bk)
        lax.fori_loop(0, clear, lambda j, _: block(j, False), None)
        lax.fori_loop(clear, lax.div(iq * bq + bq - 1 + bk, bk), lambda j, _: block(j, True), None)
        for n in range(heads):
            total = mix_s[n, HEAD : HEAD + 1, :]
            out[:, n * HEAD : (n + 1) * HEAD] = (mix_s[n, :HEAD, :] * (1 / total)).T.astype(BF)
            lse[n : n + 1, :] = top_s[n : n + 1, :] * scale + jnp.log(total)

    return call(body, "attend", (t // bq,), (q, k, v), [rows(bq, nq), whole(*k.shape), whole(*v.shape)],
                [shape_of((t, nq)), shape_of((heads, t), F32)], [rows(bq, nq), pl.BlockSpec((heads, bq), lambda i: (0, i))],
                [pltpu.VMEM((heads, bq), F32), pltpu.VMEM((heads, HEAD + 8, bq), F32), pltpu.VMEM((bk, bq), jnp.int32)],
                flops=4 * heads * t * t * HEAD, limit=ATT_LIMIT, **more)


ATT_LIMIT = 32


def silu_parts(gate):
    sg = 1 / (1 + jnp.exp(-gate))
    return sg


def post(h, attn, number, wo, wg, wu, bt=256, step=512, **more):
    (t, d), n, f = h.shape, wo.shape[1], wg.shape[2]

    def body(h, attn, wo, wg, wu, h1, b, gate, up, p):
        s = added(h[...], _dot(attn[...], wo[...], 1, 0).astype(BF))
        h1[...] = s
        wide = s.astype(F32)
        c = (wide * scale_of(wide)).astype(BF)
        b[...] = c
        for at in range(0, f, step):
            x = _dot(c, wg[:, at : at + step], 1, 0)
            y = _dot(c, wu[:, at : at + step], 1, 0)
            gate[:, at : at + step] = x
            up[:, at : at + step] = y
            p[:, at : at + step] = (jax.nn.silu(x) * y).astype(BF)

    return call(body, "post", (t // bt,), (h, attn, wo, wg, wu),
                [rows(bt, d), rows(bt, n), layer_of(number, n, d), layer_of(number, d, f), layer_of(number, d, f)],
                [shape_of((t, d)), shape_of((t, d)), shape_of((t, f), F32), shape_of((t, f), F32), shape_of((t, f))],
                [rows(bt, d), rows(bt, d), rows(bt, f), rows(bt, f), rows(bt, f)], flops=2 * t * d * (2 * f + n), limit=POST_LIMIT, **more)


POST_LIMIT = 48


def down(h1, p, number, wd, bt=512, **more):
    (t, d), f = h1.shape, p.shape[1]

    def body(h1, p, wd, out):
        out[...] = added(h1[...], _dot(p[...], wd[...], 1, 0).astype(BF))

    return call(body, "down", (t // bt,), (h1, p, wd), [rows(bt, d), rows(bt, f), layer_of(number, f, d)], [shape_of((t, d))], [rows(bt, d)],
                flops=2 * t * d * f, limit=28, **more)


def _through_gate(by_p, x, y):
    s = 1 / (1 + jnp.exp(-x))
    act = x * s
    return (by_p * y * (s + act * (1 - s))).astype(BF), (by_p * act).astype(BF)


def gate_bwd(dy, number, wd, gate, up, bt=256, step=512, **more):
    (t, d), f = dy.shape, wd.shape[1]

    def body(dy, wd, gate, up, by):
        x = dy[...]
        for at in range(0, f, step):
            here = slice(at, at + step)
            by_p = _dot(x, wd[here, :], 1, 1).astype(BF).astype(F32)
            by[0, :, here], by[1, :, here] = _through_gate(by_p, gate[:, here], up[:, here])

    return call(body, "gate_bwd", (t // bt,), (dy, wd, gate, up), [rows(bt, d), layer_of(number, f, d), rows(bt, f), rows(bt, f)],
                [shape_of((2, t, f))], [pl.BlockSpec((2, bt, f), lambda i: (0, i, 0))], flops=2 * t * d * f, limit=GATE_LIMIT, **more)


GATE_LIMIT = 36


def turnaround(h, attn, dy, number, wo, wg, wu, wd, bt=256, step=512, **more):
    (t, d), n, f = h.shape, wo.shape[1], wg.shape[2]

    def body(h, attn, dy, wo, wg, wu, wd, h1, b, p, by):
        s = added(h[...], _dot(attn[...], wo[...], 1, 0).astype(BF))
        h1[...] = s
        wide = s.astype(F32)
        c = (wide * scale_of(wide)).astype(BF)
        b[...] = c
        back = dy[...]
        for at in range(0, f, step):
            here = slice(at, at + step)
            x, y = _dot(c, wg[:, here], 1, 0), _dot(c, wu[:, here], 1, 0)
            p[:, here] = (jax.nn.silu(x) * y).astype(BF)
            by_p = _dot(back, wd[here, :], 1, 1).astype(BF).astype(F32)
            by[0, :, here], by[1, :, here] = _through_gate(by_p, x, y)

    return call(body, "turnaround", (t // bt,), (h, attn, dy, wo, wg, wu, wd),
                [rows(bt, d), rows(bt, n), rows(bt, d), layer_of(number, n, d), layer_of(number, d, f), layer_of(number, d, f),
                 layer_of(number, f, d)],
                [shape_of((t, d)), shape_of((t, d)), shape_of((t, f)), shape_of((2, t, f))],
                [rows(bt, d), rows(bt, d), rows(bt, f), pl.BlockSpec((2, bt, f), lambda i: (0, i, 0))],
                flops=2 * t * d * (3 * f + n), limit=TURN_LIMIT, **more)


TURN_LIMIT = 52


def ffn_bwd(by_gu, number, wg, wu, h1, dy, wo, bt=256, **more):
    (_, t, f), d, n = by_gu.shape, h1.shape[1], wo.shape[1]

    def body(by_gu, wg, wu, h1, dy, wo, by_h, by_attn):
        by_b = added(_dot(by_gu[0], wg[...], 1, 1).astype(BF), _dot(by_gu[1], wu[...], 1, 1).astype(BF))
        total = added(dy[...], through_norm(by_b.astype(F32), h1[...].astype(F32)))
        by_h[...] = total
        by_attn[...] = _dot(total, wo[...], 1, 1).astype(BF)

    return call(body, "ffn_bwd", (t // bt,), (by_gu, wg, wu, h1, dy, wo),
                [pl.BlockSpec((2, bt, f), lambda i: (0, i, 0)), layer_of(number, d, f), layer_of(number, d, f), rows(bt, d), rows(bt, d),
                 layer_of(number, n, d)],
                [shape_of((t, d)), shape_of((t, n))], [rows(bt, d), rows(bt, n)], flops=2 * t * d * (2 * f + n), limit=FFN_LIMIT, **more)


FFN_LIMIT = 40


def attend_bwd(q, k, v, out, by_out, lse, cos, sin, bq=256, bk=512, **more):
    t, nq = q.shape
    heads, kv = nq // HEAD, k.shape[1] // HEAD
    g = heads // kv
    e, scale = HEAD**-0.5 * LOG2E, HEAD**-0.5
    pair = 2
    wide = pair * bq
    strips = range(0, heads, pair)
    width = (g + 2) * HEAD

    def laid(ref, n):
        return jnp.concatenate([ref[:, (n + x) * HEAD : (n + x + 1) * HEAD] for x in range(pair)], axis=0)

    def body(q, k, v, out, by_out, lse, cos, sin, res, dq_s, dk_s, dv_s, gap_s):
        iq = pl.program_id(0)

        @pl.when(iq == 0)
        def _():
            gap_s[...] = _gap(bk, wide, bq)
            dk_s[...] = jnp.zeros_like(dk_s)
            dv_s[...] = jnp.zeros_like(dv_s)

        dq_s[...] = jnp.zeros_like(dq_s)
        lses = [jnp.concatenate([lse[n + x : n + x + 1, :] for x in range(pair)], axis=1) * LOG2E for n in strips]
        deltas = [(laid(by_out, n).astype(F32) * laid(out, n).astype(F32)).T.sum(axis=0, keepdims=True) for n in strips]

        def block(j, masked):
            here = pl.ds(pl.multiple_of(j * bk, bk), bk)
            qs, dos = [laid(q, n) for n in strips], [laid(by_out, n) for n in strips]
            keys = [k[here, i * HEAD : (i + 1) * HEAD] for i in range(kv)]
            values = [v[here, i * HEAD : (i + 1) * HEAD] for i in range(kv)]
            scores = [_dot(keys[n // g], x, 1, 1) for n, x in zip(strips, qs)]
            dps = [_dot(values[n // g], x, 1, 1) for n, x in zip(strips, dos)]
            ok = gap_s[...] >= (j * bk - iq * bq) if masked else None
            for s, n in enumerate(strips):
                i = n // g
                p = jnp.exp2(scores[s] * e - lses[s])
                if masked:
                    p = jnp.where(ok, p, 0.0)
                ds = (p * (dps[s] - deltas[s])).astype(BF)
                dv_s[i, here, :] += _dot(p.astype(BF), dos[s], 1, 0)
                dk_s[i, here, :] += _dot(ds, qs[s], 1, 0)
                dq_s[s] += _dot(keys[i].T, ds, 1, 0)

        clear = lax.div(iq * bq + 1, bk)
        lax.fori_loop(0, clear, lambda j, _: block(j, False), None)
        lax.fori_loop(clear, lax.div(iq * bq + bq - 1 + bk, bk), lambda j, _: block(j, True), None)
        at = pl.ds(pl.multiple_of(iq * bq, bq), bq)
        c, s_ = cos[at, :], -sin[at, :]
        for s, n in enumerate(strips):
            got = (dq_s[s] * scale).T.astype(BF).astype(F32)
            for x in range(pair):
                m = (n + x) % g
                res[(n + x) // g, at, m * HEAD : (m + 1) * HEAD] = turn(got[x * bq : (x + 1) * bq], c, s_).astype(BF)

        @pl.when(iq == pl.num_programs(0) - 1)
        def _():
            for i in range(kv):
                for r in range(0, t, bk):
                    part = pl.ds(r, bk)
                    got = (dk_s[i, part, :] * scale).astype(BF).astype(F32)
                    res[i, part, g * HEAD : (g + 1) * HEAD] = turn(got, cos[part, :], -sin[part, :]).astype(BF)
                    res[i, part, (g + 1) * HEAD :] = dv_s[i, part, :].astype(BF)

    return call(body, "attend_bwd", (t // bq,), (q, k, v, out, by_out, lse, cos, sin),
                [rows(bq, nq), whole(*k.shape), whole(*v.shape), rows(bq, nq), rows(bq, nq), pl.BlockSpec((heads, bq), lambda i: (0, i)),
                 whole(t, HEAD), whole(t, HEAD)],
                [shape_of((kv, t, width))], [whole(kv, t, width)],
                [pltpu.VMEM((heads // pair, HEAD, wide), F32), pltpu.VMEM((kv, t, HEAD), F32), pltpu.VMEM((kv, t, HEAD), F32),
                 pltpu.VMEM((bk, wide), jnp.int32)],
                flops=10 * heads * t * t * HEAD, limit=AB_LIMIT, **more)


AB_LIMIT = 40


def qkv_bwd(by_qkv, number, wq, wk, wv, h, by_h1, bt=512, **more):
    (t, d), kv = h.shape, by_qkv.shape[0]
    nq = wq.shape[2] // kv

    def body(by, wq, wk, wv, h, by_h1, out):
        got = [sum(_dot(by[i, :, a:b], w[:, i * (b - a) : (i + 1) * (b - a)], 1, 1) for i in range(kv)).astype(BF).astype(F32)
               for w, a, b in ((wq, 0, nq), (wk, nq, nq + HEAD), (wv, nq + HEAD, nq + 2 * HEAD))]
        by_a = (got[0] + got[1]).astype(BF).astype(F32) + got[2]
        out[...] = added(by_h1[...], through_norm(by_a.astype(BF).astype(F32), h[...].astype(F32)))

    return call(body, "qkv_bwd", (t // bt,), (by_qkv, wq, wk, wv, h, by_h1),
                [pl.BlockSpec((kv, bt, nq + 2 * HEAD), lambda i: (0, i, 0)), *[layer_of(number, *w.shape[1:]) for w in (wq, wk, wv)],
                 rows(bt, d), rows(bt, d)],
                [shape_of((t, d))], [rows(bt, d)], flops=2 * t * d * (kv * (nq + 2 * HEAD)), limit=24, **more)


AXES = ((8, 4, 2), (4, 2, 8), (2, 8, 4))


def strips(block):
    tiles = block // 16
    sizes = [16 * ((tiles + 2 - n) // 3) for n in range(3)]
    return [(sum(sizes[:n]), sizes[n]) for n in range(3)]


def gradient(name, blocks, lhs, rhs, lhs_specs, rhs_specs, grid, shape, out_spec, flops, limit, **more):
    def body(l0, l1, r0, r1, out):
        out[...] = (_dot(l0[...], r0[...], 0, 0) + _dot(l1[...], r1[...], 0, 0)).astype(BF)

    got = call(body, name, grid, (*lhs, *rhs), [*lhs_specs, *rhs_specs], [shape_of(shape)], [out_spec], flops=flops, limit=limit, **more)
    made, landed = got if "sends" in more and more["sends"] else (got, [])
    return made[0].reshape(blocks, shape[0] // blocks, shape[1]), landed


def core():
    return lax.axis_index("dp") % 2


def for_down(p, p_other, by, by_other, bn=256, **more):
    (t, half), d = p_other.shape, by.shape[1]
    n = half // bn
    return gradient("for_down", 8, (p, p_other), (by, by_other),
                    [pl.BlockSpec((t, bn), lambda i: (0, core() * n + i)), pl.BlockSpec((t, bn), lambda i: (0, i))], [whole(t, d)] * 2,
                    (n,), (half, d), pl.BlockSpec((bn, d), lambda i: (i, 0)), 4 * t * half * d, DW_LIMIT, **more)


def for_gate_up(b, b_other, by, by_other, bn=256, **more):
    (_, t, half), d = by_other.shape, b.shape[1]
    n = half // bn
    return gradient("for_gate_up", 8, (b, b_other), (by, by_other), [whole(t, d)] * 2,
                    [pl.BlockSpec((None, t, bn), lambda i: (i // n, 0, core() * n + i % n)), pl.BlockSpec((None, t, bn), lambda i: (i // n, 0, i % n))],
                    (2 * n,), (d, 2 * half), pl.BlockSpec((d, bn), lambda i: (0, i)), 8 * t * half * d, DW_LIMIT, **more)


DW_LIMIT = 26


def for_o(attn, attn_other, by, by_other, bn=256, **more):
    (t, n), half = attn.shape, by_other.shape[1]
    return gradient("for_o", 8, (attn, attn_other), (by, by_other), [pl.BlockSpec((t, bn), lambda i: (0, i))] * 2,
                    [pl.BlockSpec((t, half), lambda i: (0, core())), whole(t, half)],
                    (n // bn,), (n, half), pl.BlockSpec((bn, half), lambda i: (i, 0)), 4 * t * half * n, 24, **more)


def for_qkv(a, a_other, by, by_other, bn=256, **more):
    (t, d), width = a.shape, by_other.shape[1]
    return gradient("for_qkv", 8, (a, a_other), (by, by_other), [whole(t, d)] * 2,
                    [pl.BlockSpec((None, t, bn), lambda i: (core(), 0, i)), pl.BlockSpec((t, bn), lambda i: (0, i))],
                    (width // bn,), (d, width), pl.BlockSpec((d, bn), lambda i: (0, i)), 4 * t * d * width, 24, **more)


def first_sends(g):
    _, r, w = g.shape
    return Send(g, (4, r, w), [(lambda me, a=axes[0], at=at, n=n: (pl.ds(4 * (1 - bit(me, a)), 4), pl.ds(at, n)), lambda me, at=at, n=n: (slice(None), pl.ds(at, n)), axes[:1])
                               for axes, (at, n) in zip(AXES, strips(r))])


def second_sends(g, first=0, width=None):
    _, r, w = g.shape
    w = width or w
    columns = pl.ds(first, w)
    copies = []
    for axes, (at, n) in zip(AXES, strips(r)):
        for turn_ in (1, 2, 3):
            r1, r0 = turn_ // 2, turn_ % 2

            def source(me, axes=axes, r1=r1, r0=r0, at=at, n=n):
                b1, b0 = bit(me, axes[1]), bit(me, axes[2])
                return 2 * (b1 + r1 * (1 - 2 * b1)) + b0 + r0 * (1 - 2 * b0), pl.ds(at, n), columns

            copies.append((source, lambda me, k=turn_ - 1, at=at, n=n: (k, pl.ds(at, n)), axes[1:2] * r1 + axes[2:] * r0))
    return Send(g, (3, r, w), copies)


def block_specs(block, width, index):
    def spec(axes):
        def where(*i):
            first, column = index(axes, *i)
            return first, 0, column // width
        return pl.BlockSpec((1, block, width), where)
    return [spec(axes) for axes in AXES]


def strip_specs(block, width, index):
    def spec(axes, at, n):
        def where(*i):
            first, column = index(axes, *i)
            return first, at, column
        return pl.BlockSpec((pl.Element(1), pl.Element(n), pl.Element(width)), where)
    return [spec(axes, at, n) for axes, (at, n) in zip(AXES, strips(block))]


def first_sum(g, got, **more):
    _, r, w = g.shape
    sending = "sends" in more

    def body(*refs):
        own, (got, out) = refs[:3], refs[3:]
        for part, (at, n) in zip(own, strips(r)):
            mine = part[0, at : at + n] if sending else part[0]
            out[0, at : at + n] = added(mine, got[0, at : at + n])

    def index(axes, i):
        return 4 * bit(lax.axis_index("dp"), axes[0]) + i, 0

    block = pl.BlockSpec((1, r, w), lambda i: (i, 0, 0))
    return call(body, "first_sum", (4,), (g, g, g, got), [*(block_specs if sending else strip_specs)(r, w, index), block], [shape_of((4, r, w))], [block], flops=4 * r * w,
                limit=20, **more)


def second_sum(g, got, so_far, first=0, **more):
    _, r, w = got.shape
    sending = "sends" in more
    wide = max(n for n in range(128, min(w, 1024) + 1, 128) if w % n == 0)

    def body(*refs):
        own, (got, so_far, out, squares) = refs[:3], refs[3:]
        total = jnp.zeros((8, 128), F32)
        for part, (at, n) in zip(own, strips(r)):
            here = slice(at, at + n)
            mine = part[0, here] if sending else part[0]
            g = mine.astype(F32) + got[0, here].astype(F32) + got[1, here].astype(F32) + got[2, here].astype(F32)
            g = g.astype(BF)
            out[here] = g
            g = g.astype(F32)
            g = jnp.sum((g * g).reshape(n // 8, 8, wide), axis=0)
            total += sum(g[:, x : x + 128] for x in range(0, wide, 128))

        @pl.when(pl.program_id(0) == 0)
        def _():
            squares[...] = so_far[...]

        squares[...] += total

    def index(axes, j):
        me = lax.axis_index("dp")
        return 2 * bit(me, axes[1]) + bit(me, axes[2]), j * wide if sending else pl.multiple_of(first + j * wide, 128)

    small = pl.BlockSpec((8, 128), lambda j: (0, 0))
    return call(body, "second_sum", (w // wide,), (g, g, g, got, so_far),
                [*(block_specs if sending else strip_specs)(r, wide, index), pl.BlockSpec((3, r, wide), lambda j: (0, 0, j)), small],
                [shape_of((r, w)), shape_of((8, 128), F32)], [pl.BlockSpec((r, wide), lambda j: (0, j)), small],
                flops=4 * r * w, limit=20, **more)


def clip(own, count, devices, ids):
    others = [tuple(a for a in (8, 4, 2, 1) if n & a) for n in range(1, devices)]

    def body(own, out, sums, local_sem, out_sem, in_sem):
        me = lax.axis_index("dp")
        barrier = pltpu.get_barrier_semaphore()
        mine = pltpu.make_async_copy(own, sums.at[me], local_sem)
        mine.start()
        for axes in others:
            pl.semaphore_signal(barrier, 1, device_id={"dp": across(me, axes)}, device_id_type=pl.DeviceIdType.MESH)
        pl.semaphore_wait(barrier, len(others))
        moves = [pltpu.make_async_remote_copy(own, sums.at[me], out_sem.at[n], in_sem.at[n], device_id={"dp": across(me, axes)},
                                              device_id_type=pl.DeviceIdType.MESH) for n, axes in enumerate(others)]
        for move in moves:
            move.start()
        mine.wait()
        for move in moves:
            move.wait()
        total = sums[0]
        for n in range(1, devices):
            total = total + sums[n]
        out[...] = jnp.broadcast_to(jnp.minimum(1.0, 0.5 * lax.rsqrt(jnp.sum(total) / count + 1e-30)), (8, 128))

    return pl.pallas_call(body, name="clip", in_specs=[IN_HBM], out_specs=pl.BlockSpec(memory_space=pltpu.VMEM), out_shape=shape_of((8, 128), F32),
                          scratch_shapes=[pltpu.VMEM((devices, 8, 128), F32), pltpu.SemaphoreType.DMA, pltpu.SemaphoreType.DMA((devices - 1,)),
                                          pltpu.SemaphoreType.DMA((devices - 1,))],
                          compiler_params=pltpu.CompilerParams(collective_id=next(ids), has_side_effects=True))(own)


def adamw(number, ws, ms, vs, gathered, factor, split_rows, earlier=None, **more):
    _, r, _ = gathered.shape
    count = len(ws)
    if split_rows:
        ws, ms, vs = ([a.reshape(a.shape[0], 2, a.shape[1] // 2, a.shape[2]) for a in group] for group in (ws, ms, vs))
        earlier = earlier and [a.reshape(a.shape[0], 2, a.shape[1] // 2, a.shape[2]) for a in earlier]
    widths = [w.shape[-1] if split_rows else w.shape[-1] // 2 for w in ws]
    starts = [sum(widths[:n]) for n in range(count)]

    def body(*refs):
        f, refs = refs[0][0, 0], refs[1:]
        g, refs = refs[: 6 * count], refs[6 * count :]
        w, m, v = refs[:count], refs[count : 2 * count], refs[2 * count : 3 * count]
        out = refs[-3 * count :]
        for n, width in enumerate(widths):
            for side in range(2):
                for part, (at, rows_) in zip(g[6 * n + 3 * side : 6 * n + 3 * side + 3], strips(r)):
                    here = (side, slice(at, at + rows_)) if split_rows else (slice(at, at + rows_), slice(side * width, (side + 1) * width))
                    x = part[0].astype(F32) * f
                    m2 = 0.9 * m[n][here] + 0.1 * x
                    v2 = 0.95 * v[n][here] + 0.05 * x * x
                    wide = w[n][here].astype(F32)
                    out[n][here] = (wide - 0.02 * (m2 * lax.rsqrt(v2 + 1e-8) + 0.1 * wide)).astype(BF)
                    out[count + n][here] = m2
                    out[2 * count + n][here] = v2

    def blocks(width):
        if split_rows:
            return pl.BlockSpec((None, 2, r, width), lambda i: (number, 0, i, 0))
        return pl.BlockSpec((None, r, 2 * width), lambda i: (number, i, 0))

    def index_from(side, start):
        def index(axes, i):
            return axes[0] * (i // 4) + axes[1] * (i // 2 % 2) + axes[2] * (i % 2) + side, start
        return index

    own = [blocks(width) for width in widths] * 3
    specs = [pl.BlockSpec(memory_space=pltpu.SMEM)]
    for width, start in zip(widths, starts):
        for side in range(2):
            specs += strip_specs(r, width, index_from(side, start))
    ins = [factor, *[gathered] * (6 * count), *ws, *ms, *vs]
    specs += own
    aliases = {}
    if earlier is not None:
        aliases = {len(ins) + n: n for n in range(3 * count)}
        ins += list(earlier)
        specs += [IN_HBM] * (3 * count)
    outs = [shape_of(a.shape, a.dtype) for a in (*ws, *ms, *vs)]
    got = call(body, "adamw", (8,), ins, specs, outs, own, flops=20 * r * sum(widths) * 16, aliases=aliases, **more)
    return [a.reshape(a.shape[0], -1, a.shape[-1]) for a in got]


def solution(mesh):
    def step(x, dy, *arrays):
        weights, moments, squares = (arrays[i : i + 7] for i in (0, 7, 14))
        wq, wk, wv, wo, wg, wu, wd = weights
        count = sum(w.size for w in weights)
        ids = itertools.count()
        tokens, d = x.shape[1:]
        f, half = wg.shape[2], wg.shape[2] // 2
        cos, sin = angles(tokens)
        x, dy = x[0], dy[0]
        more = dict(ids=ids)
        core_half = lambda a, width, lead=0: to_core(a, (*a.shape[:-1], width), lambda me: (slice(None),) * (a.ndim - 1) + (pl.ds(pl.multiple_of((1 - bit(me, 1)) * width, 128), width),))
        other_head = lambda a: to_core(a, a.shape[1:], lambda me: (1 - bit(me, 1),))

        a0, q0, k0, v0 = qkv(x, 0, wq, wk, wv, cos, sin)
        (attn0, lse0), (a0_,) = attend(q0, k0, v0, sends=[to_core(a0)], **more)
        (h1_0, b0, gate0, up0, p0), (attn0_,) = post(x, attn0, 0, wo, wg, wu, sends=[to_core(attn0)], **more)
        (h,), (p0_,) = down(h1_0, p0, 0, wd, sends=[core_half(p0, half)], **more)
        a1, q1, k1, v1 = qkv(h, 1, wq, wk, wv, cos, sin)
        (attn1, lse1), (a1_, dy_, b0_) = attend(q1, k1, v1, sends=[to_core(a1), to_core(dy), to_core(b0)], **more)
        (h1_1, b1, p1, by_gu1), (attn1_,) = turnaround(h, attn1, dy, 1, wo, wg, wu, wd, sends=[to_core(attn1)], **more)

        (by_h1, by_attn1), (b1_, p1_, by_gu1_) = ffn_bwd(by_gu1, 1, wg, wu, h1_1, dy, wo, sends=[to_core(b1), core_half(p1, half), core_half(by_gu1, half)], **more)
        d1, (by_h1_,) = for_down(p1, p1_, dy, dy_, sends=[core_half(by_h1, d // 2)], **more)
        gu1, (d1_,) = for_gate_up(b1, b1_, by_gu1, by_gu1_, sends=[first_sends(d1)], **more)
        (d1,) = first_sum(d1, d1_)
        (by_qkv1,), (gu1_, d1_) = attend_bwd(q1, k1, v1, attn1, by_attn1, lse1, cos, sin, sends=[first_sends(gu1), second_sends(d1)], **more)
        d1, ss = second_sum(d1, d1_, jnp.zeros((8, 128), F32))
        (gu1,) = first_sum(gu1, gu1_, after=[ss])
        o1, (by_qkv1_,) = for_o(attn1, attn1_, by_h1, by_h1_, sends=[other_head(by_qkv1)], after=[gu1], **more)
        qkv1, (o1_,) = for_qkv(a1, a1_, by_qkv1, by_qkv1_, sends=[first_sends(o1)], **more)
        (by_h,), (qkv1_,) = qkv_bwd(by_qkv1, 1, wq, wk, wv, h, by_h1, sends=[first_sends(qkv1)], **more)
        (o1,), (qkv1,) = first_sum(o1, o1_), first_sum(qkv1, qkv1_)

        (by_gu0,), (by_h_, g1_) = gate_bwd(by_h, 0, wd, gate0, up0, sends=[to_core(by_h), second_sends(gu1, 0, half)], eager=True, after=[o1, qkv1], **more)
        g1, ss = second_sum(gu1, g1_, ss)
        d0, (by_gu0_, o1_, qkv1_) = for_down(p0, p0_, by_h, by_h_, sends=[core_half(by_gu0, half), second_sends(o1), second_sends(qkv1)], eager=True, after=[ss], **more)
        o1, ss = second_sum(o1, o1_, ss)
        qkv1, ss = second_sum(qkv1, qkv1_, ss)
        gu0, (d0_, u1_) = for_gate_up(b0, b0_, by_gu0, by_gu0_, sends=[first_sends(d0), second_sends(gu1, half, half)], after=[ss], **more)
        (d0,) = first_sum(d0, d0_)
        u1, ss = second_sum(gu1, u1_, ss, half)
        (by_h1, by_attn0), (gu0_,) = ffn_bwd(by_gu0, 0, wg, wu, h1_0, by_h, wo, sends=[first_sends(gu0)], after=[d0, ss], **more)
        (gu0,) = first_sum(gu0, gu0_)
        (by_qkv0,), (d0_, gu0_, by_h1_) = attend_bwd(q0, k0, v0, attn0, by_attn0, lse0, cos, sin, sends=[second_sends(d0), second_sends(gu0), core_half(by_h1, d // 2)], **more)
        d0, ss = second_sum(d0, d0_, ss)
        gu0, ss = second_sum(gu0, gu0_, ss)
        g1, o0_after = lax.optimization_barrier((g1, ss))
        o0, (by_qkv0_,) = for_o(attn0, attn0_, by_h1, by_h1_, sends=[other_head(by_qkv0)], after=[o0_after], **more)
        qkv0, (o0_,) = for_qkv(a0, a0_, by_qkv0, by_qkv0_, sends=[first_sends(o0)], **more)
        (o0,), (qkv0_,) = first_sum(o0, o0_, sends=[first_sends(qkv0)], eager=True, **more)
        (qkv0,), (o0_,) = first_sum(qkv0, qkv0_, sends=[second_sends(o0)], eager=True, **more)
        (o0, ss), (qkv0_,) = second_sum(o0, o0_, ss, sends=[second_sends(qkv0)], eager=True, **more)
        qkv0, ss = second_sum(qkv0, qkv0_, ss)

        factor = clip(ss, count, mesh.shape["dp"], ids)
        u1, d0, gu0, _ = lax.optimization_barrier((u1, d0, gu0, factor))
        everyone = lambda g: lax.all_gather(g, "dp", axis=0)

        def update(number, take, g, after, earlier=None):
            ws, ms, vs = ([group[n] for n in take] for group in (weights, moments, squares))
            return adamw(number, ws, ms, vs, everyone(g), factor, take == (6,), earlier, after=after)

        got_d = update(1, (6,), d1, ())
        got_o = update(1, (3,), o1, got_d[:1])
        got_q = update(1, (0, 1, 2), qkv1, got_o[:1])
        got_g = update(1, (4,), g1, got_q[:1])
        got_u = update(1, (5,), u1, got_g[:1])
        got_d = update(0, (6,), d0, got_u[:1], got_d)
        got_gu = update(0, (4, 5), gu0, got_d[:1], [x for pair in zip(got_g, got_u) for x in pair])
        got_o = update(0, (3,), o0, got_gu[:1], got_o)
        got_q = update(0, (0, 1, 2), qkv0, got_o[:1], got_q)
        new = [None] * 21
        for take, got in (((6,), got_d), ((4, 5), got_gu), ((3,), got_o), ((0, 1, 2), got_q)):
            for i, n in enumerate(take):
                for part in range(3):
                    new[7 * part + n] = got[part * len(take) + i]
        return tuple(new)

    states, all_of = P(("rep", "dp"), None, None), P(None, None, None)
    return jax.shard_map(step, mesh=mesh, in_specs=(states, states) + (all_of,) * 21, out_specs=(P("rep", None, None),) * 21, check_vma=False)
```

```python
import itertools

import jax
import jax.numpy as jnp
import numpy as np
from jax import lax
from jax.experimental import pallas as pl
from jax.experimental.pallas import tpu as pltpu
from jax.sharding import PartitionSpec as P

NAMES = ("wq", "wk", "wv", "wo", "w_gate", "w_up", "w_down")
HEAD = 128
THETA = 10000
NEG = -1e30
HIDDEN = 2 * NEG
LOG2E = 1.4426950408889634
BF, F32 = jnp.bfloat16, jnp.float32
MIB = 2**20


def _dot(a, b, ca, cb):
    return lax.dot_general(a, b, (((ca,), (cb,)), ((), ())), preferred_element_type=F32)


def shape_of(shape, dtype=BF):
    return jax.ShapeDtypeStruct(shape, dtype)


def rows(bt, width):
    return pl.BlockSpec((bt, width), lambda i, *_: (i, 0))


def whole(*shape):
    return pl.BlockSpec(shape, lambda *_: (0,) * len(shape), pipeline_mode=pl.Buffered(1))


def layer_of(number, *shape):
    return pl.BlockSpec((None, *shape), lambda *_: (number,) + (0,) * len(shape), pipeline_mode=pl.Buffered(1))


IN_HBM = pl.BlockSpec(memory_space=pltpu.HBM)


def bit(me, axis):
    return (me // axis) % 2


def across(me, axes):
    return me + sum(axis * (1 - 2 * bit(me, axis)) for axis in axes)


CORE = (1,)


class Send:
    def __init__(self, array, shape, copies):
        self.array, self.result, self.copies = array, shape_of(shape, array.dtype), copies


def everything(me):
    return ()


def to_core(array, shape=None, part=everything):
    return Send(array, shape or array.shape, [(part, everything, CORE)])


def place(ref, at):
    return ref.at[at] if at else ref


class Kept:
    def __init__(self, array, size, axis=0, number=None):
        self.array, self.size, self.axis, self.number = array, size, axis, number
        self.shape = array.shape[-2:]
        self.pieces = self.shape[axis] // size

    def copy(self, source, to, sems, n):
        part = pl.ds(n * self.size, self.size)
        at = (slice(None),) * self.axis + (part,)
        source = source if self.number is None else source.at[self.number]
        return pltpu.make_async_copy(source.at[at], to.at[at], sems.at[n])


WINDOW = 4


def FREE(n, piece):
    pass


def call(body, name, grid, ins, in_specs, outs, out_specs, scratch=(), flops=0, sends=(), ids=None, eager=False, aliases={}, after=(), kept=()):
    size = lambda a: a.size * jnp.dtype(a.dtype).itemsize
    cost = pl.CostEstimate(flops=int(flops), transcendentals=0, bytes_accessed=sum(map(size, ins)) + sum(map(size, outs)))
    n_in, n_kept, n_after, n_s, n_out = len(ins), len(kept), len(after), len(sends), len(outs)
    copies = [(s, c) for s, send in enumerate(sends) for c in send.copies]
    partners = sorted({c[2] for _, c in copies})
    order = [(n, piece) for piece in range(max([k.pieces for k in kept], default=0)) for n, k in enumerate(kept) if piece < k.pieces]

    def whole_body(*refs):
        take = iter(refs)
        part = lambda n: [next(take) for _ in range(n)]
        given, held, _, sources, made, landed = (part(n) for n in (n_in, n_kept, n_after, n_s, n_out, n_s))
        rest = list(take)
        rest, vmem, sems, remote = rest[: len(scratch)], rest[len(scratch) :][:n_kept], rest[len(scratch) + n_kept :][:n_kept], rest[len(scratch) + 2 * n_kept :]
        step, last = pl.program_id(0), grid[0] - 1
        if sends:
            out_sem, in_sem = remote
            me = lax.axis_index("dp")
            barrier = pltpu.get_barrier_semaphore()
            moves = [pltpu.make_async_remote_copy(place(sources[s], a(me)), place(landed[s], b(me)), out_sem.at[n], in_sem.at[n],
                                                  device_id={"dp": across(me, axes)}, device_id_type=pl.DeviceIdType.MESH)
                     for n, (s, (a, b, axes)) in enumerate(copies)]

            def begin():
                pl.semaphore_wait(barrier, len(partners))
                for move in moves:
                    move.start()

            @pl.when(step == 0)
            def _():
                for axes in partners:
                    pl.semaphore_signal(barrier, 1, device_id={"dp": across(me, axes)}, device_id_type=pl.DeviceIdType.MESH)
                if eager or last == 0:
                    begin()

        if kept:
            fetch = [kept[n].copy(held[n], vmem[n], sems[n], piece) for n, piece in order]

            @pl.when(step == 0)
            def _():
                for copy in fetch[:WINDOW]:
                    copy.start()
                done = [0]

                def need(n, piece):
                    while done[0] <= order.index((n, piece)):
                        fetch[done[0]].wait()
                        if done[0] + WINDOW < len(fetch):
                            fetch[done[0] + WINDOW].start()
                        done[0] += 1

                body(need, *given, *vmem, *made, *rest)

            @pl.when(step > 0)
            def _():
                body(FREE, *given, *vmem, *made, *rest)

        elif body is not None:
            body(*given, *made, *rest)
        if sends:
            if not (eager or last == 0):

                @pl.when(step == 0)
                def _():
                    begin()

            @pl.when(step == last)
            def _():
                for move in moves:
                    move.wait()

    more = dict(collective_id=next(ids), has_side_effects=True) if sends else {}
    remote = [pltpu.SemaphoreType.DMA((len(copies),))] * 2 if sends else []
    got = pl.pallas_call(whole_body, name=name, grid=grid, in_specs=[*in_specs, *[IN_HBM] * (n_kept + n_after + n_s)],
                         out_specs=[*out_specs, *[IN_HBM] * n_s], out_shape=[*outs, *[send.result for send in sends]],
                         scratch_shapes=[*scratch, *[pltpu.VMEM(k.shape, k.array.dtype) for k in kept],
                                         *[pltpu.SemaphoreType.DMA((k.pieces,)) for k in kept], *remote],
                         input_output_aliases=aliases, compiler_params=pltpu.CompilerParams(vmem_limit_bytes=60 * MIB, **more), cost_estimate=cost,
                         )(*ins, *[k.array for k in kept], *after, *[send.array for send in sends])
    return (got[:n_out], got[n_out:]) if sends else got


def scale_of(wide):
    return lax.rsqrt(jnp.mean(wide * wide, -1, keepdims=True) + 1e-6)


def through_norm(by_out, wide):
    scale = scale_of(wide)
    return (scale * by_out - wide * (scale * scale * scale * jnp.mean(by_out * wide, -1, keepdims=True))).astype(BF)


def added(a, b):
    return (a.astype(F32) + b.astype(F32)).astype(BF)


def turn(t, cos, sin):
    return t * cos + pltpu.roll(t, HEAD // 2, 1) * sin


def angles(tokens):
    angle = np.arange(tokens)[:, None] * float(THETA) ** (-np.arange(HEAD // 2) / (HEAD // 2))
    return np.concatenate([np.cos(angle), np.sin(angle)], 1).astype(np.float32)


def turns(angles):
    other, first = pltpu.roll(angles, HEAD // 2, 1), lax.broadcasted_iota(jnp.int32, angles.shape, 1) < HEAD // 2
    return jnp.where(first, angles, other), jnp.where(first, -other, angles)


def project(h, wq, wk, wv, table, a, q, k, v):
    wide = h.astype(F32)
    n = (wide * scale_of(wide)).astype(BF)
    a[...] = n
    c, s = turns(table[...])
    for w, out in ((wq, q), (wk, k)):
        for at in range(0, w.shape[1], 256):
            r = _dot(n, w[:, at : at + 256], 1, 0).astype(BF).astype(F32)
            for x in range(0, 256, HEAD):
                out[:, at + x : at + x + HEAD] = turn(r[:, x : x + HEAD], c, s).astype(BF)
    v[...] = _dot(n, wv[...], 1, 0).astype(BF)


def qkv(h, number, wq, wk, wv, table, bt=512):
    (t, d), nq, nk = h.shape, wq.shape[2], wk.shape[2]

    def body(h, wq, wk, wv, table, a, q, k, v):
        project(h[...], wq, wk, wv, table, a, q, k, v)

    return call(body, "qkv", (t // bt,), (h, wq, wk, wv, table),
                [rows(bt, d), layer_of(number, d, nq), layer_of(number, d, nk), layer_of(number, d, nk), rows(bt, HEAD)],
                [shape_of((t, d)), shape_of((t, nq)), shape_of((t, nk)), shape_of((t, nk))],
                [rows(bt, d), rows(bt, nq), rows(bt, nk), rows(bt, nk)], flops=2 * t * d * (nq + 2 * nk))


def _gap(bk, cols, bq):
    return lax.rem(lax.broadcasted_iota(jnp.int32, (bk, cols), 1), bq) - lax.broadcasted_iota(jnp.int32, (bk, cols), 0)


def attend(q, k, v, bq=512, bk=512, **more):
    t, nq = q.shape
    heads, kv = nq // HEAD, k.shape[1] // HEAD
    g = heads // kv
    e, scale = HEAD**-0.5 * LOG2E, HEAD**-0.5

    def body(q, k, v, out, lse, top_s, mix_s, gap_s):
        iq = pl.program_id(0)

        @pl.when(iq == 0)
        def _():
            gap_s[...] = _gap(bk, bq, bq)

        top_s[...] = jnp.full(top_s.shape, NEG, F32)
        mix_s[...] = jnp.zeros(mix_s.shape, F32)
        ones = jnp.ones((8, bk), BF)

        def block(j, masked):
            here = pl.ds(pl.multiple_of(j * bk, bk), bk)
            keys = [k[here, i * HEAD : (i + 1) * HEAD] for i in range(kv)]
            values = [jnp.concatenate([v[here, i * HEAD : (i + 1) * HEAD].T, ones], axis=0) for i in range(kv)]
            scores = [_dot(keys[n // g], q[:, n * HEAD : (n + 1) * HEAD], 1, 1) for n in range(heads)]
            ok = gap_s[...] >= (j * bk - iq * bq) if masked else None
            weights, keeps = [], []
            for n, s in enumerate(scores):
                if masked:
                    s = jnp.where(ok, s, HIDDEN)
                old = top_s[n : n + 1, :]
                top = jnp.maximum(old, s.max(axis=0, keepdims=True))
                top_s[n : n + 1, :] = top
                weights.append(jnp.exp2((s - top) * e).astype(BF))
                keeps.append(jnp.exp2((old - top) * e))
            for n, (p, keep) in enumerate(zip(weights, keeps)):
                mix_s[n] = mix_s[n] * keep + _dot(values[n // g], p, 1, 0)

        clear = lax.div(iq * bq + 1, bk)
        lax.fori_loop(0, clear, lambda j, _: block(j, False), None)
        lax.fori_loop(clear, lax.div(iq * bq + bq - 1 + bk, bk), lambda j, _: block(j, True), None)
        for n in range(heads):
            total = mix_s[n, HEAD : HEAD + 1, :]
            out[:, n * HEAD : (n + 1) * HEAD] = (mix_s[n, :HEAD, :] * (1 / total)).T.astype(BF)
            lse[n : n + 1, :] = top_s[n : n + 1, :] * scale + jnp.log(total)

    return call(body, "attend", (t // bq,), (q, k, v), [rows(bq, nq), whole(*k.shape), whole(*v.shape)],
                [shape_of((t, nq)), shape_of((heads, t), F32)], [rows(bq, nq), pl.BlockSpec((heads, bq), lambda i: (0, i))],
                [pltpu.VMEM((heads, bq), F32), pltpu.VMEM((heads, HEAD + 8, bq), F32), pltpu.VMEM((bk, bq), jnp.int32)],
                flops=4 * heads * t * t * HEAD, **more)


def post(h, attn, number, wo, wg, wu, bt=256, step=512, **more):
    (t, d), n, f = h.shape, wo.shape[1], wg.shape[2]

    def body(need, h, attn, wo, wg, wu, h1, b, gate, up, p):
        need(0, 0)
        s = added(h[...], _dot(attn[...], wo[...], 1, 0).astype(BF))
        h1[...] = s
        wide = s.astype(F32)
        c = (wide * scale_of(wide)).astype(BF)
        b[...] = c
        for at in range(0, f, step):
            need(1, at // step)
            need(2, at // step)
            x = _dot(c, wg[:, at : at + step], 1, 0)
            y = _dot(c, wu[:, at : at + step], 1, 0)
            gate[:, at : at + step] = x
            up[:, at : at + step] = y
            p[:, at : at + step] = (jax.nn.silu(x) * y).astype(BF)

    return call(body, "post", (t // bt,), (h, attn), [rows(bt, d), rows(bt, n)],
                [shape_of((t, d)), shape_of((t, d)), shape_of((t, f), F32), shape_of((t, f), F32), shape_of((t, f))],
                [rows(bt, d), rows(bt, d), rows(bt, f), rows(bt, f), rows(bt, f)], flops=2 * t * d * (2 * f + n),
                kept=[Kept(wo, n, 0, number), Kept(wg, step, 1, number), Kept(wu, step, 1, number)], **more)


def down(h1, p, number, wd, bt=512, **more):
    (t, d), f = h1.shape, p.shape[1]

    def body(h1, p, wd, out):
        out[...] = added(h1[...], _dot(p[...], wd[...], 1, 0).astype(BF))

    return call(body, "down", (t // bt,), (h1, p, wd), [rows(bt, d), rows(bt, f), layer_of(number, f, d)], [shape_of((t, d))], [rows(bt, d)],
                flops=2 * t * d * f, **more)


def _through_gate(by_p, x, y):
    s = 1 / (1 + jnp.exp(-x))
    act = x * s
    return (by_p * y * (s + act * (1 - s))).astype(BF), (by_p * act).astype(BF)


def gate_bwd(dy, number, wd, gate, up, bt=256, step=512, **more):
    (t, d), f = dy.shape, wd.shape[1]

    def body(need, dy, gate, up, wd, by):
        x = dy[...]
        for at in range(0, f, step):
            need(0, at // step)
            here = slice(at, at + step)
            by_p = _dot(x, wd[here, :], 1, 1).astype(BF).astype(F32)
            by[0, :, here], by[1, :, here] = _through_gate(by_p, gate[:, here], up[:, here])

    return call(body, "gate_bwd", (t // bt,), (dy, gate, up), [rows(bt, d), rows(bt, f), rows(bt, f)],
                [shape_of((2, t, f))], [pl.BlockSpec((2, bt, f), lambda i: (0, i, 0))], flops=2 * t * d * f,
                kept=[Kept(wd, step, 0, number)], **more)


def turnaround(h, attn, dy, number, wo, wg, wu, wd, bt=256, step=512, **more):
    (t, d), n, f = h.shape, wo.shape[1], wg.shape[2]

    def body(need, h, attn, dy, wo, wg, wu, wd, h1, b, p, by):
        need(0, 0)
        s = added(h[...], _dot(attn[...], wo[...], 1, 0).astype(BF))
        h1[...] = s
        wide = s.astype(F32)
        c = (wide * scale_of(wide)).astype(BF)
        b[...] = c
        back = dy[...]
        for at in range(0, f, step):
            here = slice(at, at + step)
            for n in (1, 2, 3):
                need(n, at // step)
            x, y = _dot(c, wg[:, here], 1, 0), _dot(c, wu[:, here], 1, 0)
            p[:, here] = (jax.nn.silu(x) * y).astype(BF)
            by_p = _dot(back, wd[here, :], 1, 1).astype(BF).astype(F32)
            by[0, :, here], by[1, :, here] = _through_gate(by_p, x, y)

    return call(body, "turnaround", (t // bt,), (h, attn, dy), [rows(bt, d), rows(bt, n), rows(bt, d)],
                [shape_of((t, d)), shape_of((t, d)), shape_of((t, f)), shape_of((2, t, f))],
                [rows(bt, d), rows(bt, d), rows(bt, f), pl.BlockSpec((2, bt, f), lambda i: (0, i, 0))],
                flops=2 * t * d * (3 * f + n),
                kept=[Kept(wo, n, 0, number), Kept(wg, step, 1, number), Kept(wu, step, 1, number), Kept(wd, step, 0, number)], **more)


def ffn_bwd(by_gu, number, wg, wu, h1, dy, wo, bt=256, step=256, **more):
    (_, t, f), d, n = by_gu.shape, h1.shape[1], wo.shape[1]

    def body(need, by_gu, h1, dy, wg, wu, wo, by_h, by_attn, by_b):
        for at in range(0, d, step):
            here = slice(at, at + step)
            need(0, at // step)
            need(1, at // step)
            by_b[:, here] = added(_dot(by_gu[0], wg[here, :], 1, 1).astype(BF), _dot(by_gu[1], wu[here, :], 1, 1).astype(BF)).astype(F32)
        total = added(dy[...], through_norm(by_b[...], h1[...].astype(F32)))
        by_h[...] = total
        need(2, 0)
        by_attn[...] = _dot(total, wo[...], 1, 1).astype(BF)

    return call(body, "ffn_bwd", (t // bt,), (by_gu, h1, dy), [pl.BlockSpec((2, bt, f), lambda i: (0, i, 0)), rows(bt, d), rows(bt, d)],
                [shape_of((t, d)), shape_of((t, n))], [rows(bt, d), rows(bt, n)], [pltpu.VMEM((bt, d), F32)], flops=2 * t * d * (2 * f + n),
                kept=[Kept(wg, step, 0, number), Kept(wu, step, 0, number), Kept(wo, n, 0, number)], **more)


def attend_bwd(q, k, v, out, by_out, lse, table, bq=256, bk=512, **more):
    t, nq = q.shape
    heads, kv = nq // HEAD, k.shape[1] // HEAD
    g = heads // kv
    e, scale = HEAD**-0.5 * LOG2E, HEAD**-0.5
    pair = 2
    wide = pair * bq
    strips = range(0, heads, pair)
    width = (g + 2) * HEAD

    def laid(ref, n):
        return jnp.concatenate([ref[:, (n + x) * HEAD : (n + x + 1) * HEAD] for x in range(pair)], axis=0)

    def body(q, k, v, out, by_out, lse, table, res, dq_s, dk_s, dv_s, gap_s):
        iq = pl.program_id(0)

        @pl.when(iq == 0)
        def _():
            gap_s[...] = _gap(bk, wide, bq)
            dk_s[...] = jnp.zeros_like(dk_s)
            dv_s[...] = jnp.zeros_like(dv_s)

        dq_s[...] = jnp.zeros_like(dq_s)
        lses = [jnp.concatenate([lse[n + x : n + x + 1, :] for x in range(pair)], axis=1) * LOG2E for n in strips]
        deltas = [(laid(by_out, n).astype(F32) * laid(out, n).astype(F32)).T.sum(axis=0, keepdims=True) for n in strips]

        def block(j, masked):
            here = pl.ds(pl.multiple_of(j * bk, bk), bk)
            qs, dos = [laid(q, n) for n in strips], [laid(by_out, n) for n in strips]
            keys = [k[here, i * HEAD : (i + 1) * HEAD] for i in range(kv)]
            values = [v[here, i * HEAD : (i + 1) * HEAD] for i in range(kv)]
            scores = [_dot(keys[n // g], x, 1, 1) for n, x in zip(strips, qs)]
            dps = [_dot(values[n // g], x, 1, 1) for n, x in zip(strips, dos)]
            ok = gap_s[...] >= (j * bk - iq * bq) if masked else None
            for s, n in enumerate(strips):
                i = n // g
                p = jnp.exp2(scores[s] * e - lses[s])
                if masked:
                    p = jnp.where(ok, p, 0.0)
                ds = (p * (dps[s] - deltas[s])).astype(BF)
                dv_s[i, here, :] += _dot(p.astype(BF), dos[s], 1, 0)
                dk_s[i, here, :] += _dot(ds, qs[s], 1, 0)
                dq_s[s] += _dot(keys[i].T, ds, 1, 0)

        clear = lax.div(iq * bq + 1, bk)
        lax.fori_loop(0, clear, lambda j, _: block(j, False), None)
        lax.fori_loop(clear, lax.div(iq * bq + bq - 1 + bk, bk), lambda j, _: block(j, True), None)
        at = pl.ds(pl.multiple_of(iq * bq, bq), bq)
        c, s_ = turns(table[at, :])
        for s, n in enumerate(strips):
            got = (dq_s[s] * scale).T.astype(BF).astype(F32)
            for x in range(pair):
                m = (n + x) % g
                res[(n + x) // g, at, m * HEAD : (m + 1) * HEAD] = turn(got[x * bq : (x + 1) * bq], c, -s_).astype(BF)

        @pl.when(iq == pl.num_programs(0) - 1)
        def _():
            for i in range(kv):
                for r in range(0, t, bk):
                    part = pl.ds(r, bk)
                    got = (dk_s[i, part, :] * scale).astype(BF).astype(F32)
                    c, s_ = turns(table[part, :])
                    res[i, part, g * HEAD : (g + 1) * HEAD] = turn(got, c, -s_).astype(BF)
                    res[i, part, (g + 1) * HEAD :] = dv_s[i, part, :].astype(BF)

    return call(body, "attend_bwd", (t // bq,), (q, k, v, out, by_out, lse, table),
                [rows(bq, nq), whole(*k.shape), whole(*v.shape), rows(bq, nq), rows(bq, nq), pl.BlockSpec((heads, bq), lambda i: (0, i)),
                 whole(t, HEAD)],
                [shape_of((kv, t, width))], [whole(kv, t, width)],
                [pltpu.VMEM((heads // pair, HEAD, wide), F32), pltpu.VMEM((kv, t, HEAD), F32), pltpu.VMEM((kv, t, HEAD), F32),
                 pltpu.VMEM((bk, wide), jnp.int32)],
                flops=10 * heads * t * t * HEAD, **more)


def qkv_bwd(by_qkv, number, wq, wk, wv, h, by_h1, bt=512, **more):
    (t, d), kv = h.shape, by_qkv.shape[0]
    nq = wq.shape[2] // kv

    def body(by, wq, wk, wv, h, by_h1, out):
        got = [sum(_dot(by[i, :, a:b], w[:, i * (b - a) : (i + 1) * (b - a)], 1, 1) for i in range(kv)).astype(BF).astype(F32)
               for w, a, b in ((wq, 0, nq), (wk, nq, nq + HEAD), (wv, nq + HEAD, nq + 2 * HEAD))]
        by_a = (got[0] + got[1]).astype(BF).astype(F32) + got[2]
        out[...] = added(by_h1[...], through_norm(by_a.astype(BF).astype(F32), h[...].astype(F32)))

    return call(body, "qkv_bwd", (t // bt,), (by_qkv, wq, wk, wv, h, by_h1),
                [pl.BlockSpec((kv, bt, nq + 2 * HEAD), lambda i: (0, i, 0)), *[layer_of(number, *w.shape[1:]) for w in (wq, wk, wv)],
                 rows(bt, d), rows(bt, d)],
                [shape_of((t, d))], [rows(bt, d)], flops=2 * t * d * (kv * (nq + 2 * HEAD)), **more)


AXES = ((8, 4, 2), (4, 2, 8), (2, 8, 4))


def strips(block):
    tiles = block // 16
    sizes = [16 * ((tiles + 2 - n) // 3) for n in range(3)]
    return [(sum(sizes[:n]), sizes[n]) for n in range(3)]


def gradient(name, blocks, lhs, rhs, lhs_specs, rhs_specs, grid, shape, out_spec, flops, **more):
    def body(l0, l1, r0, r1, out):
        out[...] = (_dot(l0[...], r0[...], 0, 0) + _dot(l1[...], r1[...], 0, 0)).astype(BF)

    got = call(body, name, grid, (*lhs, *rhs), [*lhs_specs, *rhs_specs], [shape_of(shape)], [out_spec], flops=flops, **more)
    made, landed = got if "sends" in more and more["sends"] else (got, [])
    return made[0].reshape(blocks, shape[0] // blocks, shape[1]), landed


def core():
    return lax.axis_index("dp") % 2


def for_down(p, p_other, by, by_other, bn=256, **more):
    (t, half), d = p_other.shape, by.shape[1]
    n = half // bn
    return gradient("for_down", 8, (p, p_other), (by, by_other),
                    [pl.BlockSpec((t, bn), lambda i: (0, core() * n + i)), pl.BlockSpec((t, bn), lambda i: (0, i))], [whole(t, d)] * 2,
                    (n,), (half, d), pl.BlockSpec((bn, d), lambda i: (i, 0)), 4 * t * half * d, **more)


def for_gate_up(b, b_other, by, by_other, bn=256, **more):
    (_, t, half), d = by_other.shape, b.shape[1]
    n = half // bn
    return gradient("for_gate_up", 8, (b, b_other), (by, by_other), [whole(t, d)] * 2,
                    [pl.BlockSpec((None, t, bn), lambda i: (i // n, 0, core() * n + i % n)), pl.BlockSpec((None, t, bn), lambda i: (i // n, 0, i % n))],
                    (2 * n,), (d, 2 * half), pl.BlockSpec((d, bn), lambda i: (0, i)), 8 * t * half * d, **more)


def for_o(attn, attn_other, by, by_other, bn=256, **more):
    (t, n), half = attn.shape, by_other.shape[1]
    return gradient("for_o", 8, (attn, attn_other), (by, by_other), [pl.BlockSpec((t, bn), lambda i: (0, i))] * 2,
                    [pl.BlockSpec((t, half), lambda i: (0, core())), whole(t, half)],
                    (n // bn,), (n, half), pl.BlockSpec((bn, half), lambda i: (i, 0)), 4 * t * half * n, **more)


def for_qkv(a, a_other, by, by_other, bn=256, **more):
    (t, d), width = a.shape, by_other.shape[1]
    return gradient("for_qkv", 8, (a, a_other), (by, by_other), [pl.BlockSpec((t, bn), lambda i: (0, i))] * 2,
                    [pl.BlockSpec((None, t, width), lambda i: (core(), 0, 0), pipeline_mode=pl.Buffered(1)), whole(t, width)],
                    (d // bn,), (d, width), pl.BlockSpec((bn, width), lambda i: (i, 0)), 4 * t * d * width, **more)


def first_sends(g):
    _, r, w = g.shape
    return Send(g, (4, r, w), [(lambda me, a=axes[0], at=at, n=n: (pl.ds(4 * (1 - bit(me, a)), 4), pl.ds(at, n)), lambda me, at=at, n=n: (slice(None), pl.ds(at, n)), axes[:1])
                               for axes, (at, n) in zip(AXES, strips(r))])


def second_sends(g, first=0, width=None):
    _, r, w = g.shape
    w = width or w
    columns = pl.ds(first, w)
    copies = []
    for axes, (at, n) in zip(AXES, strips(r)):
        for turn_ in (1, 2, 3):
            r1, r0 = turn_ // 2, turn_ % 2

            def source(me, axes=axes, r1=r1, r0=r0, at=at, n=n):
                b1, b0 = bit(me, axes[1]), bit(me, axes[2])
                return 2 * (b1 + r1 * (1 - 2 * b1)) + b0 + r0 * (1 - 2 * b0), pl.ds(at, n), columns

            copies.append((source, lambda me, k=turn_ - 1, at=at, n=n: (k, pl.ds(at, n)), axes[1:2] * r1 + axes[2:] * r0))
    return Send(g, (3, r, w), copies)


def block_specs(block, width, index):
    def spec(axes):
        def where(*i):
            first, column = index(axes, *i)
            return first, 0, column // width
        return pl.BlockSpec((1, block, width), where)
    return [spec(axes) for axes in AXES]


def strip_specs(block, width, index):
    def spec(axes, at, n):
        def where(*i):
            first, column = index(axes, *i)
            return first, at, column
        return pl.BlockSpec((pl.Element(1), pl.Element(n), pl.Element(width)), where)
    return [spec(axes, at, n) for axes, (at, n) in zip(AXES, strips(block))]


def first_sum(g, got, **more):
    _, r, w = g.shape
    sending = "sends" in more

    def body(*refs):
        own, (got, out) = refs[:3], refs[3:]
        for part, (at, n) in zip(own, strips(r)):
            mine = part[0, at : at + n] if sending else part[0]
            out[0, at : at + n] = added(mine, got[0, at : at + n])

    def index(axes, i):
        return 4 * bit(lax.axis_index("dp"), axes[0]) + i, 0

    block = pl.BlockSpec((1, r, w), lambda i: (i, 0, 0))
    return call(body, "first_sum", (4,), (g, g, g, got), [*(block_specs if sending else strip_specs)(r, w, index), block], [shape_of((4, r, w))], [block], flops=4 * r * w, **more)


def second_sum(g, got, so_far, first=0, **more):
    _, r, w = got.shape
    sending = "sends" in more
    wide = max(n for n in range(128, min(w, 1024) + 1, 128) if w % n == 0)

    def body(*refs):
        own, (got, so_far, out, squares) = refs[:3], refs[3:]
        total = jnp.zeros((8, 128), F32)
        for part, (at, n) in zip(own, strips(r)):
            here = slice(at, at + n)
            mine = part[0, here] if sending else part[0]
            g = mine.astype(F32) + got[0, here].astype(F32) + got[1, here].astype(F32) + got[2, here].astype(F32)
            g = g.astype(BF)
            out[here] = g
            g = g.astype(F32)
            g = jnp.sum((g * g).reshape(n // 8, 8, wide), axis=0)
            total += sum(g[:, x : x + 128] for x in range(0, wide, 128))

        @pl.when(pl.program_id(0) == 0)
        def _():
            squares[...] = so_far[...]

        squares[...] += total

    def index(axes, j):
        me = lax.axis_index("dp")
        return 2 * bit(me, axes[1]) + bit(me, axes[2]), j * wide if sending else pl.multiple_of(first + j * wide, 128)

    small = pl.BlockSpec((8, 128), lambda j: (0, 0))
    return call(body, "second_sum", (w // wide,), (g, g, g, got, so_far),
                [*(block_specs if sending else strip_specs)(r, wide, index), pl.BlockSpec((3, r, wide), lambda j: (0, 0, j)), small],
                [shape_of((r, w)), shape_of((8, 128), F32)], [pl.BlockSpec((r, wide), lambda j: (0, j)), small],
                flops=4 * r * w, **more)


def second_sums(pairs, so_far):
    sizes = [got.shape[1:] for _, got in pairs]
    starts = [sum(w for _, w in sizes[:n]) for n in range(len(sizes))]
    tall, all_columns = max(r for r, _ in sizes), sum(w for _, w in sizes)

    def body(*refs):
        so_far, out, squares = refs[-3:]
        total = so_far[...]
        for k, ((r, w), start) in enumerate(zip(sizes, starts)):
            columns, own, got = slice(start, start + w), refs[4 * k : 4 * k + 3], refs[4 * k + 3]
            for part, (at, n) in zip(own, strips(r)):
                here = slice(at, at + n)
                g = part[0].astype(F32) + got[0, here].astype(F32) + got[1, here].astype(F32) + got[2, here].astype(F32)
                g = g.astype(BF)
                out[here, columns] = g
                g = g.astype(F32)
                g = jnp.sum((g * g).reshape(n // 8, 8, w), axis=0)
                total += sum(g[:, x : x + 128] for x in range(0, w, 128))
            if r < tall:
                out[r:, columns] = jnp.zeros((tall - r, w), BF)
        squares[...] = total

    def index(axes, j):
        me = lax.axis_index("dp")
        return 2 * bit(me, axes[1]) + bit(me, axes[2]), 0

    ins, specs = [], []
    for (g, got), (r, w) in zip(pairs, sizes):
        ins += [g, g, g, got]
        specs += [*strip_specs(r, w, index), pl.BlockSpec((3, r, w), lambda j: (0, 0, 0))]
    small = pl.BlockSpec((8, 128), lambda j: (0, 0))
    return call(body, "second_sums", (1,), [*ins, so_far], [*specs, small], [shape_of((tall, all_columns)), shape_of((8, 128), F32)],
                [pl.BlockSpec((tall, all_columns), lambda j: (0, 0)), small], flops=4 * tall * all_columns)


def first_sums(pairs):
    sizes = [g.shape[1:] for g, _ in pairs]

    def body(*refs):
        outs = refs[4 * len(pairs) :]
        for k, (r, _) in enumerate(sizes):
            for part, (at, n) in zip(refs[4 * k : 4 * k + 3], strips(r)):
                outs[k][0, at : at + n] = added(part[0], refs[4 * k + 3][0, at : at + n])

    def index(axes, i):
        return 4 * bit(lax.axis_index("dp"), axes[0]) + i, 0

    blocks = [pl.BlockSpec((1, r, w), lambda i: (i, 0, 0)) for r, w in sizes]
    ins, specs = [], []
    for (g, got), (r, w), block in zip(pairs, sizes, blocks):
        ins += [g, g, g, got]
        specs += [*strip_specs(r, w, index), block]
    return call(body, "first_sums", (4,), ins, specs, [shape_of((4, r, w)) for r, w in sizes], blocks, flops=4 * sum(r * w for r, w in sizes))


def clip(own, count, devices, ids):
    others = [tuple(a for a in (8, 4, 2, 1) if n & a) for n in range(1, devices)]

    def body(own, out, sums, local_sem, out_sem, in_sem):
        me = lax.axis_index("dp")
        barrier = pltpu.get_barrier_semaphore()
        mine = pltpu.make_async_copy(own, sums.at[me], local_sem)
        mine.start()
        for axes in others:
            pl.semaphore_signal(barrier, 1, device_id={"dp": across(me, axes)}, device_id_type=pl.DeviceIdType.MESH)
        pl.semaphore_wait(barrier, len(others))
        moves = [pltpu.make_async_remote_copy(own, sums.at[me], out_sem.at[n], in_sem.at[n], device_id={"dp": across(me, axes)},
                                              device_id_type=pl.DeviceIdType.MESH) for n, axes in enumerate(others)]
        for move in moves:
            move.start()
        mine.wait()
        for move in moves:
            move.wait()
        total = sums[0]
        for n in range(1, devices):
            total = total + sums[n]
        out[...] = jnp.broadcast_to(jnp.minimum(1.0, 0.5 * lax.rsqrt(jnp.sum(total) / count + 1e-30)), (8, 128))

    return pl.pallas_call(body, name="clip", in_specs=[IN_HBM], out_specs=pl.BlockSpec(memory_space=pltpu.VMEM), out_shape=shape_of((8, 128), F32),
                          scratch_shapes=[pltpu.VMEM((devices, 8, 128), F32), pltpu.SemaphoreType.DMA, pltpu.SemaphoreType.DMA((devices - 1,)),
                                          pltpu.SemaphoreType.DMA((devices - 1,))],
                          compiler_params=pltpu.CompilerParams(collective_id=next(ids), has_side_effects=True))(own)


def adamw(number, parts, factor, earlier=None, **more):
    count = len(parts)
    halves = lambda a: a.reshape(a.shape[0], 2, a.shape[1] // 2, a.shape[2])
    lay = [halves if part[5] else (lambda a: a) for part in parts]
    ws, ms, vs = ([f(part[n]) for f, part in zip(lay, parts)] for n in range(3))

    def body(*refs):
        f, refs = refs[0][0, 0], refs[1:]
        g, refs = refs[: 6 * count], refs[6 * count :]
        w, m, v = refs[:count], refs[count : 2 * count], refs[2 * count : 3 * count]
        out = refs[-3 * count :]
        for n, (w_, *_, by_rows) in enumerate(parts):
            for side in range(2):
                for part, (at, size) in zip(g[6 * n + 3 * side : 6 * n + 3 * side + 3], strips(w_.shape[1] // (16 if by_rows else 8))):
                    width = part.shape[2]
                    here = (side, slice(at, at + size)) if by_rows else (slice(at, at + size), slice(side * width, (side + 1) * width))
                    x = part[0].astype(F32) * f
                    m2 = 0.9 * m[n][here] + 0.1 * x
                    v2 = 0.95 * v[n][here] + 0.05 * x * x
                    wide = w[n][here].astype(F32)
                    out[n][here] = (wide - 0.02 * (m2 * lax.rsqrt(v2 + 1e-8) + 0.1 * wide)).astype(BF)
                    out[count + n][here] = m2
                    out[2 * count + n][here] = v2

    specs, own = [pl.BlockSpec(memory_space=pltpu.SMEM)], []
    for w, _, _, _, start, by_rows in parts:
        r = w.shape[1] // (16 if by_rows else 8)
        width = w.shape[2] if by_rows else w.shape[2] // 2
        own.append(pl.BlockSpec((None, 2, r, width), lambda i: (number, 0, i, 0)) if by_rows else pl.BlockSpec((None, r, 2 * width), lambda i: (number, i, 0)))
        for side in range(2):
            specs += strip_specs(r, width, lambda axes, i, side=side, start=start:
                                 (axes[0] * (i // 4) + axes[1] * (i // 2 % 2) + axes[2] * (i % 2) + side, start))
    ins = [factor, *[part[3] for part in parts for _ in range(6)], *ws, *ms, *vs]
    own = own * 3
    specs += own
    aliases = {}
    if earlier is not None:
        aliases = {len(ins) + n: n for n in range(3 * count)}
        ins += [f(a) for f, a in zip(lay * 3, earlier)]
        specs += [IN_HBM] * (3 * count)
    outs = [shape_of(a.shape, a.dtype) for a in (*ws, *ms, *vs)]
    got = call(body, "adamw", (8,), ins, specs, outs, own, flops=20 * sum(w.size // w.shape[0] for w in ws), aliases=aliases, **more)
    return [a.reshape(a.shape[0], -1, a.shape[-1]) for a in got]


def solution(mesh):
    def step(x, dy, *arrays):
        weights, moments, squares = (arrays[i : i + 7] for i in (0, 7, 14))
        wq, wk, wv, wo, wg, wu, wd = weights
        count = sum(w.size for w in weights)
        ids = itertools.count()
        tokens, d = x.shape[1:]
        f, half = wg.shape[2], wg.shape[2] // 2
        table = jnp.asarray(angles(tokens))
        x, dy = x[0], dy[0]
        more = dict(ids=ids)
        core_half = lambda a, width, lead=0: to_core(a, (*a.shape[:-1], width), lambda me: (slice(None),) * (a.ndim - 1) + (pl.ds(pl.multiple_of((1 - bit(me, 1)) * width, 128), width),))
        other_head = lambda a: to_core(a, a.shape[1:], lambda me: (1 - bit(me, 1),))

        a0, q0, k0, v0 = qkv(x, 0, wq, wk, wv, table)
        (attn0, lse0), (a0_,) = attend(q0, k0, v0, sends=[to_core(a0)], **more)
        (h1_0, b0, gate0, up0, p0), (attn0_,) = post(x, attn0, 0, wo, wg, wu, sends=[to_core(attn0)], **more)
        (h,), (p0_,) = down(h1_0, p0, 0, wd, sends=[core_half(p0, half)], **more)
        a1, q1, k1, v1 = qkv(h, 1, wq, wk, wv, table)
        (attn1, lse1), (a1_, dy_, b0_) = attend(q1, k1, v1, sends=[to_core(a1), to_core(dy), to_core(b0)], **more)
        (h1_1, b1, p1, by_gu1), (attn1_,) = turnaround(h, attn1, dy, 1, wo, wg, wu, wd, sends=[to_core(attn1)], **more)

        (by_h1, by_attn1), (b1_, p1_, by_gu1_) = ffn_bwd(by_gu1, 1, wg, wu, h1_1, dy, wo, sends=[to_core(b1), core_half(p1, half), core_half(by_gu1, half)], **more)
        d1, (by_h1_,) = for_down(p1, p1_, dy, dy_, sends=[core_half(by_h1, d // 2)], **more)
        gu1, (d1_,) = for_gate_up(b1, b1_, by_gu1, by_gu1_, sends=[first_sends(d1)], **more)
        (d1,) = first_sum(d1, d1_)
        (by_qkv1,), (gu1_, d1_) = attend_bwd(q1, k1, v1, attn1, by_attn1, lse1, table, sends=[first_sends(gu1), second_sends(d1)], **more)
        d1, ss = second_sum(d1, d1_, jnp.zeros((8, 128), F32))
        (gu1,) = first_sum(gu1, gu1_, after=[ss])
        o1, (by_qkv1_,) = for_o(attn1, attn1_, by_h1, by_h1_, sends=[other_head(by_qkv1)], after=[gu1], **more)
        qkv1, (o1_,) = for_qkv(a1, a1_, by_qkv1, by_qkv1_, sends=[first_sends(o1)], **more)
        (by_h,), (qkv1_,) = qkv_bwd(by_qkv1, 1, wq, wk, wv, h, by_h1, sends=[first_sends(qkv1)], **more)
        qkv1, o1 = first_sums([(qkv1, qkv1_), (o1, o1_)])

        (by_gu0,), (by_h_, gu1_) = gate_bwd(by_h, 0, wd, gate0, up0, sends=[to_core(by_h), second_sends(gu1)], eager=True, after=[o1], **more)
        gu1, ss = second_sum(gu1, gu1_, ss)
        d0, (by_gu0_, o1_, qkv1_) = for_down(p0, p0_, by_h, by_h_, sends=[core_half(by_gu0, half), second_sends(o1), second_sends(qkv1)], eager=True, after=[ss], **more)
        oq1, ss = second_sums([(qkv1, qkv1_), (o1, o1_)], ss)
        gu0, (d0_,) = for_gate_up(b0, b0_, by_gu0, by_gu0_, sends=[first_sends(d0)], after=[ss], **more)
        (d0,) = first_sum(d0, d0_)
        (by_h1, by_attn0), (gu0_,) = ffn_bwd(by_gu0, 0, wg, wu, h1_0, by_h, wo, sends=[first_sends(gu0)], after=[d0], eager=True, **more)
        (gu0,) = first_sum(gu0, gu0_)
        (by_qkv0,), (d0_, gu0_, by_h1_) = attend_bwd(q0, k0, v0, attn0, by_attn0, lse0, table, sends=[second_sends(d0), second_sends(gu0), core_half(by_h1, d // 2)], **more)
        o0, (by_qkv0_,) = for_o(attn0, attn0_, by_h1, by_h1_, sends=[other_head(by_qkv0)], **more)
        qkv0, (o0_,) = for_qkv(a0, a0_, by_qkv0, by_qkv0_, sends=[first_sends(o0)], **more)
        (gu0, ss), (qkv0_,) = second_sum(gu0, gu0_, ss, sends=[first_sends(qkv0)], eager=True, **more)
        qkv0, o0 = first_sums([(qkv0, qkv0_), (o0, o0_)])
        (d0, ss), (qkv0_, o0_) = second_sum(d0, d0_, ss, sends=[second_sends(qkv0), second_sends(o0)], eager=True, **more)
        oq0, ss = second_sums([(qkv0, qkv0_), (o0, o0_)], ss)

        factor = clip(ss, count, mesh.shape["dp"], ids)
        everyone = lambda g: lax.all_gather(g, "dp", axis=0)
        starts = {0: 0, 1: wq.shape[2] // 2, 2: (wq.shape[2] + wk.shape[2]) // 2, 3: (wq.shape[2] + wk.shape[2] + wv.shape[2]) // 2, 4: 0, 5: half, 6: 0}

        def update(number, take, g, after, earlier=None):
            return adamw(number, [(weights[n], moments[n], squares[n], g, starts[n], n == 6) for n in take], factor, earlier, after=after)

        d_, gu_, oq_ = (6,), (4, 5), (3, 0, 1, 2)
        d1, gu1 = everyone(d1), everyone(gu1)
        oq1, gu0, d0, oq0, _ = lax.optimization_barrier((oq1, gu0, d0, oq0, factor))
        got_d = update(1, d_, d1, ())
        got_gu = update(1, gu_, gu1, got_d[:1])
        got_oq = update(1, oq_, everyone(oq1), got_gu[:1])
        got_gu = update(0, gu_, everyone(gu0), got_oq[:1], got_gu)
        got_d = update(0, d_, everyone(d0), got_gu[:1], got_d)
        got_oq = update(0, oq_, everyone(oq0), got_d[:1], got_oq)
        new = [None] * 21
        for take, got in ((d_, got_d), (gu_, got_gu), (oq_, got_oq)):
            for i, n in enumerate(take):
                for part in range(3):
                    new[7 * part + n] = got[part * len(take) + i]
        return tuple(new)

    states, all_of = P(("rep", "dp"), None, None), P(None, None, None)
    return jax.shard_map(step, mesh=mesh, in_specs=(states, states) + (all_of,) * 21, out_specs=(P("rep", None, None),) * 21, check_vma=False)
```

```python
import itertools

import jax
import jax.numpy as jnp
import numpy as np
from jax import lax
from jax.experimental import pallas as pl
from jax.experimental.pallas import tpu as pltpu
from jax.sharding import PartitionSpec as P

NAMES = ("wq", "wk", "wv", "wo", "w_gate", "w_up", "w_down")
HEAD = 128
THETA = 10000
NEG = -1e30
HIDDEN = 2 * NEG
LOG2E = 1.4426950408889634
BF, F32 = jnp.bfloat16, jnp.float32
MIB = 2**20


def _dot(a, b, ca, cb):
    return lax.dot_general(a, b, (((ca,), (cb,)), ((), ())), preferred_element_type=F32)


def shape_of(shape, dtype=BF):
    return jax.ShapeDtypeStruct(shape, dtype)


def rows(bt, width):
    return pl.BlockSpec((bt, width), lambda i, *_: (i, 0))


def whole(*shape):
    return pl.BlockSpec(shape, lambda *_: (0,) * len(shape), pipeline_mode=pl.Buffered(1))


def layer_of(number, *shape):
    return pl.BlockSpec((None, *shape), lambda *_: (number,) + (0,) * len(shape), pipeline_mode=pl.Buffered(1))


IN_HBM = pl.BlockSpec(memory_space=pltpu.HBM)


def bit(me, axis):
    return (me // axis) % 2


def across(me, axes):
    return me + sum(axis * (1 - 2 * bit(me, axis)) for axis in axes)


CORE = (1,)


class Send:
    def __init__(self, array, shape, copies):
        self.array, self.result, self.copies = array, shape_of(shape, array.dtype), copies


def everything(me):
    return ()


def to_core(array, shape=None, part=everything):
    return Send(array, shape or array.shape, [(part, everything, CORE)])


def place(ref, at):
    return ref.at[at] if at else ref


class Kept:
    def __init__(self, array, size, axis=0, number=None):
        self.array, self.size, self.axis, self.number = array, size, axis, number
        self.shape = array.shape[-2:]
        self.pieces = self.shape[axis] // size

    def copy(self, source, to, sems, n):
        part = pl.ds(n * self.size, self.size)
        at = (slice(None),) * self.axis + (part,)
        source = source if self.number is None else source.at[self.number]
        return pltpu.make_async_copy(source.at[at], to.at[at], sems.at[n])


WINDOW = 4


def FREE(n, piece):
    pass


def call(body, name, grid, ins, in_specs, outs, out_specs, scratch=(), flops=0, sends=(), ids=None, eager=False, aliases={}, after=(), kept=()):
    size = lambda a: a.size * jnp.dtype(a.dtype).itemsize
    cost = pl.CostEstimate(flops=int(flops), transcendentals=0, bytes_accessed=sum(map(size, ins)) + sum(map(size, outs)))
    n_in, n_kept, n_after, n_s, n_out = len(ins), len(kept), len(after), len(sends), len(outs)
    copies = [(s, c) for s, send in enumerate(sends) for c in send.copies]
    partners = sorted({c[2] for _, c in copies})
    order = [(n, piece) for piece in range(max([k.pieces for k in kept], default=0)) for n, k in enumerate(kept) if piece < k.pieces]

    def whole_body(*refs):
        take = iter(refs)
        part = lambda n: [next(take) for _ in range(n)]
        given, held, _, sources, made, landed = (part(n) for n in (n_in, n_kept, n_after, n_s, n_out, n_s))
        rest = list(take)
        rest, vmem, sems, remote = rest[: len(scratch)], rest[len(scratch) :][:n_kept], rest[len(scratch) + n_kept :][:n_kept], rest[len(scratch) + 2 * n_kept :]
        step, last = pl.program_id(0), grid[0] - 1
        if sends:
            out_sem, in_sem = remote
            me = lax.axis_index("dp")
            barrier = pltpu.get_barrier_semaphore()
            moves = [pltpu.make_async_remote_copy(place(sources[s], a(me)), place(landed[s], b(me)), out_sem.at[n], in_sem.at[n],
                                                  device_id={"dp": across(me, axes)}, device_id_type=pl.DeviceIdType.MESH)
                     for n, (s, (a, b, axes)) in enumerate(copies)]

            def begin():
                pl.semaphore_wait(barrier, len(partners))
                for move in moves:
                    move.start()

            @pl.when(step == 0)
            def _():
                for axes in partners:
                    pl.semaphore_signal(barrier, 1, device_id={"dp": across(me, axes)}, device_id_type=pl.DeviceIdType.MESH)
                if eager or last == 0:
                    begin()

        if kept:
            fetch = [kept[n].copy(held[n], vmem[n], sems[n], piece) for n, piece in order]

            @pl.when(step == 0)
            def _():
                for copy in fetch[:WINDOW]:
                    copy.start()
                done = [0]

                def need(n, piece):
                    while done[0] <= order.index((n, piece)):
                        fetch[done[0]].wait()
                        if done[0] + WINDOW < len(fetch):
                            fetch[done[0] + WINDOW].start()
                        done[0] += 1

                body(need, *given, *vmem, *made, *rest)

            @pl.when(step > 0)
            def _():
                body(FREE, *given, *vmem, *made, *rest)

        elif body is not None:
            body(*given, *made, *rest)
        if sends:
            if not (eager or last == 0):

                @pl.when(step == 0)
                def _():
                    begin()

            @pl.when(step == last)
            def _():
                for move in moves:
                    move.wait()

    more = dict(collective_id=next(ids), has_side_effects=True) if sends else {}
    remote = [pltpu.SemaphoreType.DMA((len(copies),))] * 2 if sends else []
    got = pl.pallas_call(whole_body, name=name, grid=grid, in_specs=[*in_specs, *[IN_HBM] * (n_kept + n_after + n_s)],
                         out_specs=[*out_specs, *[IN_HBM] * n_s], out_shape=[*outs, *[send.result for send in sends]],
                         scratch_shapes=[*scratch, *[pltpu.VMEM(k.shape, k.array.dtype) for k in kept],
                                         *[pltpu.SemaphoreType.DMA((k.pieces,)) for k in kept], *remote],
                         input_output_aliases=aliases, compiler_params=pltpu.CompilerParams(vmem_limit_bytes=60 * MIB, **more), cost_estimate=cost,
                         )(*ins, *[k.array for k in kept], *after, *[send.array for send in sends])
    return (got[:n_out], got[n_out:]) if sends else got


def scale_of(wide):
    return lax.rsqrt(jnp.mean(wide * wide, -1, keepdims=True) + 1e-6)


def through_norm(by_out, wide):
    scale = scale_of(wide)
    return (scale * by_out - wide * (scale * scale * scale * jnp.mean(by_out * wide, -1, keepdims=True))).astype(BF)


def added(a, b):
    return (a.astype(F32) + b.astype(F32)).astype(BF)


def turn(t, cos, sin):
    return t * cos + pltpu.roll(t, HEAD // 2, 1) * sin


def angles(tokens):
    angle = np.arange(tokens)[:, None] * float(THETA) ** (-np.arange(HEAD // 2) / (HEAD // 2))
    return np.concatenate([np.cos(angle), np.sin(angle)], 1).astype(np.float32)


def turns(angles):
    other, first = pltpu.roll(angles, HEAD // 2, 1), lax.broadcasted_iota(jnp.int32, angles.shape, 1) < HEAD // 2
    return jnp.where(first, angles, other), jnp.where(first, -other, angles)


def project(h, wq, wk, wv, table, a, q, k, v):
    wide = h.astype(F32)
    n = (wide * scale_of(wide)).astype(BF)
    a[...] = n
    c, s = turns(table[...])
    for w, out in ((wq, q), (wk, k)):
        for at in range(0, w.shape[1], 256):
            r = _dot(n, w[:, at : at + 256], 1, 0).astype(BF).astype(F32)
            for x in range(0, 256, HEAD):
                out[:, at + x : at + x + HEAD] = turn(r[:, x : x + HEAD], c, s).astype(BF)
    v[...] = _dot(n, wv[...], 1, 0).astype(BF)


def qkv(h, number, wq, wk, wv, table, bt=512):
    (t, d), nq, nk = h.shape, wq.shape[2], wk.shape[2]

    def body(h, wq, wk, wv, table, a, q, k, v):
        project(h[...], wq, wk, wv, table, a, q, k, v)

    return call(body, "qkv", (t // bt,), (h, wq, wk, wv, table),
                [rows(bt, d), layer_of(number, d, nq), layer_of(number, d, nk), layer_of(number, d, nk), rows(bt, HEAD)],
                [shape_of((t, d)), shape_of((t, nq)), shape_of((t, nk)), shape_of((t, nk))],
                [rows(bt, d), rows(bt, nq), rows(bt, nk), rows(bt, nk)], flops=2 * t * d * (nq + 2 * nk))


def _gap(bk, cols, bq):
    return lax.rem(lax.broadcasted_iota(jnp.int32, (bk, cols), 1), bq) - lax.broadcasted_iota(jnp.int32, (bk, cols), 0)


def attend(q, k, v, bq=512, bk=512, **more):
    t, nq = q.shape
    heads, kv = nq // HEAD, k.shape[1] // HEAD
    g = heads // kv
    e, scale = HEAD**-0.5 * LOG2E, HEAD**-0.5

    def body(q, k, v, out, lse, top_s, mix_s, gap_s):
        iq = pl.program_id(0)

        @pl.when(iq == 0)
        def _():
            gap_s[...] = _gap(bk, bq, bq)

        top_s[...] = jnp.full(top_s.shape, NEG, F32)
        mix_s[...] = jnp.zeros(mix_s.shape, F32)
        def block(start, size, first=0, masked=False):
            here = pl.ds(start, size)
            keys = [k[here, i * HEAD : (i + 1) * HEAD] for i in range(kv)]
            ones = jnp.ones((8, size), BF)
            values = [jnp.concatenate([v[here, i * HEAD : (i + 1) * HEAD].T, ones], axis=0) for i in range(kv)]
            scores = [_dot(keys[n // g], q[first:, n * HEAD : (n + 1) * HEAD], 1, 1) for n in range(heads)]
            ok = gap_s[:size, first:] >= (start - iq * bq) if masked else None
            weights, keeps = [], []
            for n, s in enumerate(scores):
                if masked:
                    s = jnp.where(ok, s, HIDDEN)
                old = top_s[n : n + 1, first:]
                top = jnp.maximum(old, s.max(axis=0, keepdims=True))
                top_s[n : n + 1, first:] = top
                weights.append(jnp.exp2((s - top) * e).astype(BF))
                keeps.append(jnp.exp2((old - top) * e))
            for n, (p, keep) in enumerate(zip(weights, keeps)):
                mix_s[n, :, first:] = mix_s[n, :, first:] * keep + _dot(values[n // g], p, 1, 0)

        lax.fori_loop(0, iq, lambda j, _: block(pl.multiple_of(j * bk, bk), bk), None)
        for part in range(2):
            block(pl.multiple_of(iq * bq + part * bq // 2, bq // 2), bq // 2, part * bq // 2, True)
        for n in range(heads):
            total = mix_s[n, HEAD : HEAD + 1, :]
            out[:, n * HEAD : (n + 1) * HEAD] = (mix_s[n, :HEAD, :] * (1 / total)).T.astype(BF)
            lse[n : n + 1, :] = top_s[n : n + 1, :] * scale + jnp.log(total)

    return call(body, "attend", (t // bq,), (q, k, v), [rows(bq, nq), whole(*k.shape), whole(*v.shape)],
                [shape_of((t, nq)), shape_of((heads, t), F32)], [rows(bq, nq), pl.BlockSpec((heads, bq), lambda i: (0, i))],
                [pltpu.VMEM((heads, bq), F32), pltpu.VMEM((heads, HEAD + 8, bq), F32), pltpu.VMEM((bk, bq), jnp.int32)],
                flops=4 * heads * t * t * HEAD, **more)


def post(h, attn, number, wo, wg, wu, bt=256, step=512, **more):
    (t, d), n, f = h.shape, wo.shape[1], wg.shape[2]

    def body(need, h, attn, wo, wg, wu, h1, b, gate, up, p):
        need(0, 0)
        s = added(h[...], _dot(attn[...], wo[...], 1, 0).astype(BF))
        h1[...] = s
        wide = s.astype(F32)
        c = (wide * scale_of(wide)).astype(BF)
        b[...] = c
        for at in range(0, f, step):
            need(1, at // step)
            need(2, at // step)
            x = _dot(c, wg[:, at : at + step], 1, 0)
            y = _dot(c, wu[:, at : at + step], 1, 0)
            gate[:, at : at + step] = x
            up[:, at : at + step] = y
            p[:, at : at + step] = (jax.nn.silu(x) * y).astype(BF)

    return call(body, "post", (t // bt,), (h, attn), [rows(bt, d), rows(bt, n)],
                [shape_of((t, d)), shape_of((t, d)), shape_of((t, f), F32), shape_of((t, f), F32), shape_of((t, f))],
                [rows(bt, d), rows(bt, d), rows(bt, f), rows(bt, f), rows(bt, f)], flops=2 * t * d * (2 * f + n),
                kept=[Kept(wo, n, 0, number), Kept(wg, step, 1, number), Kept(wu, step, 1, number)], **more)


def down(h1, p, number, wd, bt=512, **more):
    (t, d), f = h1.shape, p.shape[1]

    def body(h1, p, wd, out):
        out[...] = added(h1[...], _dot(p[...], wd[...], 1, 0).astype(BF))

    return call(body, "down", (t // bt,), (h1, p, wd), [rows(bt, d), rows(bt, f), layer_of(number, f, d)], [shape_of((t, d))], [rows(bt, d)],
                flops=2 * t * d * f, **more)


def _through_gate(by_p, x, y):
    s = 1 / (1 + jnp.exp(-x))
    act = x * s
    return (by_p * y * (s + act * (1 - s))).astype(BF), (by_p * act).astype(BF)


def gate_bwd(dy, number, wd, gate, up, bt=256, step=512, **more):
    (t, d), f = dy.shape, wd.shape[1]

    def body(need, dy, gate, up, wd, by):
        x = dy[...]
        for at in range(0, f, step):
            need(0, at // step)
            here = slice(at, at + step)
            by_p = _dot(x, wd[here, :], 1, 1).astype(BF).astype(F32)
            by[0, :, here], by[1, :, here] = _through_gate(by_p, gate[:, here], up[:, here])

    return call(body, "gate_bwd", (t // bt,), (dy, gate, up), [rows(bt, d), rows(bt, f), rows(bt, f)],
                [shape_of((2, t, f))], [pl.BlockSpec((2, bt, f), lambda i: (0, i, 0))], flops=2 * t * d * f,
                kept=[Kept(wd, step, 0, number)], **more)


def turnaround(h, attn, dy, number, wo, wg, wu, wd, bt=256, step=512, **more):
    (t, d), n, f = h.shape, wo.shape[1], wg.shape[2]

    def body(need, h, attn, dy, wo, wg, wu, wd, h1, b, p, by):
        need(0, 0)
        s = added(h[...], _dot(attn[...], wo[...], 1, 0).astype(BF))
        h1[...] = s
        wide = s.astype(F32)
        c = (wide * scale_of(wide)).astype(BF)
        b[...] = c
        back = dy[...]
        for at in range(0, f, step):
            here = slice(at, at + step)
            for n in (1, 2, 3):
                need(n, at // step)
            x, y = _dot(c, wg[:, here], 1, 0), _dot(c, wu[:, here], 1, 0)
            p[:, here] = (jax.nn.silu(x) * y).astype(BF)
            by_p = _dot(back, wd[here, :], 1, 1).astype(BF).astype(F32)
            by[0, :, here], by[1, :, here] = _through_gate(by_p, x, y)

    return call(body, "turnaround", (t // bt,), (h, attn, dy), [rows(bt, d), rows(bt, n), rows(bt, d)],
                [shape_of((t, d)), shape_of((t, d)), shape_of((t, f)), shape_of((2, t, f))],
                [rows(bt, d), rows(bt, d), rows(bt, f), pl.BlockSpec((2, bt, f), lambda i: (0, i, 0))],
                flops=2 * t * d * (3 * f + n),
                kept=[Kept(wo, n, 0, number), Kept(wg, step, 1, number), Kept(wu, step, 1, number), Kept(wd, step, 0, number)], **more)


def ffn_bwd(by_gu, number, wg, wu, h1, dy, wo, bt=256, step=256, **more):
    (_, t, f), d, n = by_gu.shape, h1.shape[1], wo.shape[1]

    def body(need, by_gu, h1, dy, wg, wu, wo, by_h, by_attn, by_b):
        for at in range(0, d, step):
            here = slice(at, at + step)
            need(0, at // step)
            need(1, at // step)
            by_b[:, here] = added(_dot(by_gu[0], wg[here, :], 1, 1).astype(BF), _dot(by_gu[1], wu[here, :], 1, 1).astype(BF)).astype(F32)
        total = added(dy[...], through_norm(by_b[...], h1[...].astype(F32)))
        by_h[...] = total
        need(2, 0)
        by_attn[...] = _dot(total, wo[...], 1, 1).astype(BF)

    return call(body, "ffn_bwd", (t // bt,), (by_gu, h1, dy), [pl.BlockSpec((2, bt, f), lambda i: (0, i, 0)), rows(bt, d), rows(bt, d)],
                [shape_of((t, d)), shape_of((t, n))], [rows(bt, d), rows(bt, n)], [pltpu.VMEM((bt, d), F32)], flops=2 * t * d * (2 * f + n),
                kept=[Kept(wg, step, 0, number), Kept(wu, step, 0, number), Kept(wo, n, 0, number)], **more)


def attend_bwd(q, k, v, out, by_out, lse, table, bq=256, bk=512, **more):
    t, nq = q.shape
    heads, kv = nq // HEAD, k.shape[1] // HEAD
    g = heads // kv
    e, scale = HEAD**-0.5 * LOG2E, HEAD**-0.5
    pair = 2
    wide = pair * bq
    strips = range(0, heads, pair)
    width = (g + 2) * HEAD

    def laid(ref, n):
        return jnp.concatenate([ref[:, (n + x) * HEAD : (n + x + 1) * HEAD] for x in range(pair)], axis=0)

    def body(q, k, v, out, by_out, lse, table, res, dq_s, dk_s, dv_s, gap_s):
        iq = pl.program_id(0)

        @pl.when(iq == 0)
        def _():
            gap_s[...] = _gap(bk, wide, bq)
            dk_s[...] = jnp.zeros_like(dk_s)
            dv_s[...] = jnp.zeros_like(dv_s)

        dq_s[...] = jnp.zeros_like(dq_s)
        lses = [jnp.concatenate([lse[n + x : n + x + 1, :] for x in range(pair)], axis=1) * LOG2E for n in strips]
        deltas = [(laid(by_out, n).astype(F32) * laid(out, n).astype(F32)).T.sum(axis=0, keepdims=True) for n in strips]

        def block(start, size, masked=False):
            here = pl.ds(start, size)
            qs, dos = [laid(q, n) for n in strips], [laid(by_out, n) for n in strips]
            keys = [k[here, i * HEAD : (i + 1) * HEAD] for i in range(kv)]
            values = [v[here, i * HEAD : (i + 1) * HEAD] for i in range(kv)]
            scores = [_dot(keys[n // g], x, 1, 1) for n, x in zip(strips, qs)]
            dps = [_dot(values[n // g], x, 1, 1) for n, x in zip(strips, dos)]
            ok = gap_s[:size] >= (start - iq * bq) if masked else None
            for s, n in enumerate(strips):
                i = n // g
                p = jnp.exp2(scores[s] * e - lses[s])
                if masked:
                    p = jnp.where(ok, p, 0.0)
                ds = (p * (dps[s] - deltas[s])).astype(BF)
                dv_s[i, here, :] += _dot(p.astype(BF), dos[s], 1, 0)
                dk_s[i, here, :] += _dot(ds, qs[s], 1, 0)
                dq_s[s] += _dot(keys[i].T, ds, 1, 0)

        whole_blocks = (iq * bq) // bk
        lax.fori_loop(0, whole_blocks, lambda j, _: block(pl.multiple_of(j * bk, bk), bk), None)
        lax.fori_loop(whole_blocks * (bk // bq), iq, lambda j, _: block(pl.multiple_of(j * bq, bq), bq), None)
        block(pl.multiple_of(iq * bq, bq), bq, True)
        at = pl.ds(pl.multiple_of(iq * bq, bq), bq)
        c, s_ = turns(table[at, :])
        for s, n in enumerate(strips):
            got = (dq_s[s] * scale).T.astype(BF).astype(F32)
            for x in range(pair):
                m = (n + x) % g
                res[(n + x) // g, at, m * HEAD : (m + 1) * HEAD] = turn(got[x * bq : (x + 1) * bq], c, -s_).astype(BF)

        @pl.when(iq == pl.num_programs(0) - 1)
        def _():
            for i in range(kv):
                for r in range(0, t, bk):
                    part = pl.ds(r, bk)
                    got = (dk_s[i, part, :] * scale).astype(BF).astype(F32)
                    c, s_ = turns(table[part, :])
                    res[i, part, g * HEAD : (g + 1) * HEAD] = turn(got, c, -s_).astype(BF)
                    res[i, part, (g + 1) * HEAD :] = dv_s[i, part, :].astype(BF)

    return call(body, "attend_bwd", (t // bq,), (q, k, v, out, by_out, lse, table),
                [rows(bq, nq), whole(*k.shape), whole(*v.shape), rows(bq, nq), rows(bq, nq), pl.BlockSpec((heads, bq), lambda i: (0, i)),
                 whole(t, HEAD)],
                [shape_of((kv, t, width))], [whole(kv, t, width)],
                [pltpu.VMEM((heads // pair, HEAD, wide), F32), pltpu.VMEM((kv, t, HEAD), F32), pltpu.VMEM((kv, t, HEAD), F32),
                 pltpu.VMEM((bk, wide), jnp.int32)],
                flops=10 * heads * t * t * HEAD, **more)


def qkv_bwd(by_qkv, number, wq, wk, wv, h, by_h1, bt=512, **more):
    (t, d), kv = h.shape, by_qkv.shape[0]
    nq = wq.shape[2] // kv

    def body(by, wq, wk, wv, h, by_h1, out):
        got = [sum(_dot(by[i, :, a:b], w[:, i * (b - a) : (i + 1) * (b - a)], 1, 1) for i in range(kv)).astype(BF).astype(F32)
               for w, a, b in ((wq, 0, nq), (wk, nq, nq + HEAD), (wv, nq + HEAD, nq + 2 * HEAD))]
        by_a = (got[0] + got[1]).astype(BF).astype(F32) + got[2]
        out[...] = added(by_h1[...], through_norm(by_a.astype(BF).astype(F32), h[...].astype(F32)))

    return call(body, "qkv_bwd", (t // bt,), (by_qkv, wq, wk, wv, h, by_h1),
                [pl.BlockSpec((kv, bt, nq + 2 * HEAD), lambda i: (0, i, 0)), *[layer_of(number, *w.shape[1:]) for w in (wq, wk, wv)],
                 rows(bt, d), rows(bt, d)],
                [shape_of((t, d))], [rows(bt, d)], flops=2 * t * d * (kv * (nq + 2 * HEAD)), **more)


AXES = ((8, 4, 2), (4, 2, 8), (2, 8, 4))


def strips(block):
    tiles = block // 16
    sizes = [16 * ((tiles + 2 - n) // 3) for n in range(3)]
    return [(sum(sizes[:n]), sizes[n]) for n in range(3)]


def gradient(name, blocks, lhs, rhs, lhs_specs, rhs_specs, grid, shape, out_spec, flops, **more):
    def body(l0, l1, r0, r1, out):
        out[...] = (_dot(l0[...], r0[...], 0, 0) + _dot(l1[...], r1[...], 0, 0)).astype(BF)

    got = call(body, name, grid, (*lhs, *rhs), [*lhs_specs, *rhs_specs], [shape_of(shape)], [out_spec], flops=flops, **more)
    made, landed = got if "sends" in more and more["sends"] else (got, [])
    return made[0].reshape(blocks, shape[0] // blocks, shape[1]), landed


def core():
    return lax.axis_index("dp") % 2


def for_down(p, p_other, by, by_other, bn=256, **more):
    (t, half), d = p_other.shape, by.shape[1]
    n = half // bn
    return gradient("for_down", 8, (p, p_other), (by, by_other),
                    [pl.BlockSpec((t, bn), lambda i: (0, core() * n + i)), pl.BlockSpec((t, bn), lambda i: (0, i))], [whole(t, d)] * 2,
                    (n,), (half, d), pl.BlockSpec((bn, d), lambda i: (i, 0)), 4 * t * half * d, **more)


def for_gate_up(b, b_other, by, by_other, bn=256, **more):
    (_, t, half), d = by_other.shape, b.shape[1]
    n = half // bn
    return gradient("for_gate_up", 8, (b, b_other), (by, by_other), [whole(t, d)] * 2,
                    [pl.BlockSpec((None, t, bn), lambda i: (i // n, 0, core() * n + i % n)), pl.BlockSpec((None, t, bn), lambda i: (i // n, 0, i % n))],
                    (2 * n,), (d, 2 * half), pl.BlockSpec((d, bn), lambda i: (0, i)), 8 * t * half * d, **more)


def for_o(attn, attn_other, by, by_other, bn=256, **more):
    (t, n), half = attn.shape, by_other.shape[1]
    return gradient("for_o", 8, (attn, attn_other), (by, by_other), [pl.BlockSpec((t, bn), lambda i: (0, i))] * 2,
                    [pl.BlockSpec((t, half), lambda i: (0, core())), whole(t, half)],
                    (n // bn,), (n, half), pl.BlockSpec((bn, half), lambda i: (i, 0)), 4 * t * half * n, **more)


def for_qkv(a, a_other, by, by_other, bn=256, **more):
    (t, d), width = a.shape, by_other.shape[1]
    return gradient("for_qkv", 8, (a, a_other), (by, by_other), [pl.BlockSpec((t, bn), lambda i: (0, i))] * 2,
                    [pl.BlockSpec((None, t, width), lambda i: (core(), 0, 0), pipeline_mode=pl.Buffered(1)), whole(t, width)],
                    (d // bn,), (d, width), pl.BlockSpec((bn, width), lambda i: (i, 0)), 4 * t * d * width, **more)


def first_sends(g):
    _, r, w = g.shape
    return Send(g, (4, r, w), [(lambda me, a=axes[0], at=at, n=n: (pl.ds(4 * (1 - bit(me, a)), 4), pl.ds(at, n)), lambda me, at=at, n=n: (slice(None), pl.ds(at, n)), axes[:1])
                               for axes, (at, n) in zip(AXES, strips(r))])


def second_sends(g, first=0, width=None):
    _, r, w = g.shape
    w = width or w
    columns = pl.ds(first, w)
    copies = []
    for axes, (at, n) in zip(AXES, strips(r)):
        for turn_ in (1, 2, 3):
            r1, r0 = turn_ // 2, turn_ % 2

            def source(me, axes=axes, r1=r1, r0=r0, at=at, n=n):
                b1, b0 = bit(me, axes[1]), bit(me, axes[2])
                return 2 * (b1 + r1 * (1 - 2 * b1)) + b0 + r0 * (1 - 2 * b0), pl.ds(at, n), columns

            copies.append((source, lambda me, k=turn_ - 1, at=at, n=n: (k, pl.ds(at, n)), axes[1:2] * r1 + axes[2:] * r0))
    return Send(g, (3, r, w), copies)


def block_specs(block, width, index):
    def spec(axes):
        def where(*i):
            first, column = index(axes, *i)
            return first, 0, column // width
        return pl.BlockSpec((1, block, width), where)
    return [spec(axes) for axes in AXES]


def strip_specs(block, width, index):
    def spec(axes, at, n):
        def where(*i):
            first, column = index(axes, *i)
            return first, at, column
        return pl.BlockSpec((pl.Element(1), pl.Element(n), pl.Element(width)), where)
    return [spec(axes, at, n) for axes, (at, n) in zip(AXES, strips(block))]


def first_sum(g, got, **more):
    _, r, w = g.shape
    sending = "sends" in more

    def body(*refs):
        own, (got, out) = refs[:3], refs[3:]
        for part, (at, n) in zip(own, strips(r)):
            mine = part[0, at : at + n] if sending else part[0]
            out[0, at : at + n] = added(mine, got[0, at : at + n])

    def index(axes, i):
        return 4 * bit(lax.axis_index("dp"), axes[0]) + i, 0

    block = pl.BlockSpec((1, r, w), lambda i: (i, 0, 0))
    return call(body, "first_sum", (4,), (g, g, g, got), [*(block_specs if sending else strip_specs)(r, w, index), block], [shape_of((4, r, w))], [block], flops=4 * r * w, **more)


def second_sum(g, got, so_far, first=0, **more):
    _, r, w = got.shape
    sending = "sends" in more
    wide = max(n for n in range(128, min(w, 1024) + 1, 128) if w % n == 0)

    def body(*refs):
        own, (got, so_far, out, squares) = refs[:3], refs[3:]
        total = jnp.zeros((8, 128), F32)
        for part, (at, n) in zip(own, strips(r)):
            here = slice(at, at + n)
            mine = part[0, here] if sending else part[0]
            g = mine.astype(F32) + got[0, here].astype(F32) + got[1, here].astype(F32) + got[2, here].astype(F32)
            g = g.astype(BF)
            out[here] = g
            g = g.astype(F32)
            g = jnp.sum((g * g).reshape(n // 8, 8, wide), axis=0)
            total += sum(g[:, x : x + 128] for x in range(0, wide, 128))

        @pl.when(pl.program_id(0) == 0)
        def _():
            squares[...] = so_far[...]

        squares[...] += total

    def index(axes, j):
        me = lax.axis_index("dp")
        return 2 * bit(me, axes[1]) + bit(me, axes[2]), j * wide if sending else pl.multiple_of(first + j * wide, 128)

    small = pl.BlockSpec((8, 128), lambda j: (0, 0))
    return call(body, "second_sum", (w // wide,), (g, g, g, got, so_far),
                [*(block_specs if sending else strip_specs)(r, wide, index), pl.BlockSpec((3, r, wide), lambda j: (0, 0, j)), small],
                [shape_of((r, w)), shape_of((8, 128), F32)], [pl.BlockSpec((r, wide), lambda j: (0, j)), small],
                flops=4 * r * w, **more)


def second_sums(pairs, so_far):
    sizes = [got.shape[1:] for _, got in pairs]
    starts = [sum(w for _, w in sizes[:n]) for n in range(len(sizes))]
    tall, all_columns = max(r for r, _ in sizes), sum(w for _, w in sizes)

    def body(*refs):
        so_far, out, squares = refs[-3:]
        total = so_far[...]
        for k, ((r, w), start) in enumerate(zip(sizes, starts)):
            columns, own, got = slice(start, start + w), refs[4 * k : 4 * k + 3], refs[4 * k + 3]
            for part, (at, n) in zip(own, strips(r)):
                here = slice(at, at + n)
                g = part[0].astype(F32) + got[0, here].astype(F32) + got[1, here].astype(F32) + got[2, here].astype(F32)
                g = g.astype(BF)
                out[here, columns] = g
                g = g.astype(F32)
                g = jnp.sum((g * g).reshape(n // 8, 8, w), axis=0)
                total += sum(g[:, x : x + 128] for x in range(0, w, 128))
            if r < tall:
                out[r:, columns] = jnp.zeros((tall - r, w), BF)
        squares[...] = total

    def index(axes, j):
        me = lax.axis_index("dp")
        return 2 * bit(me, axes[1]) + bit(me, axes[2]), 0

    ins, specs = [], []
    for (g, got), (r, w) in zip(pairs, sizes):
        ins += [g, g, g, got]
        specs += [*strip_specs(r, w, index), pl.BlockSpec((3, r, w), lambda j: (0, 0, 0))]
    small = pl.BlockSpec((8, 128), lambda j: (0, 0))
    return call(body, "second_sums", (1,), [*ins, so_far], [*specs, small], [shape_of((tall, all_columns)), shape_of((8, 128), F32)],
                [pl.BlockSpec((tall, all_columns), lambda j: (0, 0)), small], flops=4 * tall * all_columns)


def first_sums(pairs):
    sizes = [g.shape[1:] for g, _ in pairs]

    def body(*refs):
        outs = refs[4 * len(pairs) :]
        for k, (r, _) in enumerate(sizes):
            for part, (at, n) in zip(refs[4 * k : 4 * k + 3], strips(r)):
                outs[k][0, at : at + n] = added(part[0], refs[4 * k + 3][0, at : at + n])

    def index(axes, i):
        return 4 * bit(lax.axis_index("dp"), axes[0]) + i, 0

    blocks = [pl.BlockSpec((1, r, w), lambda i: (i, 0, 0)) for r, w in sizes]
    ins, specs = [], []
    for (g, got), (r, w), block in zip(pairs, sizes, blocks):
        ins += [g, g, g, got]
        specs += [*strip_specs(r, w, index), block]
    return call(body, "first_sums", (4,), ins, specs, [shape_of((4, r, w)) for r, w in sizes], blocks, flops=4 * sum(r * w for r, w in sizes))


def clip(own, count, devices, ids):
    others = [tuple(a for a in (8, 4, 2, 1) if n & a) for n in range(1, devices)]

    def body(own, out, sums, local_sem, out_sem, in_sem):
        me = lax.axis_index("dp")
        barrier = pltpu.get_barrier_semaphore()
        mine = pltpu.make_async_copy(own, sums.at[me], local_sem)
        mine.start()
        for axes in others:
            pl.semaphore_signal(barrier, 1, device_id={"dp": across(me, axes)}, device_id_type=pl.DeviceIdType.MESH)
        pl.semaphore_wait(barrier, len(others))
        moves = [pltpu.make_async_remote_copy(own, sums.at[me], out_sem.at[n], in_sem.at[n], device_id={"dp": across(me, axes)},
                                              device_id_type=pl.DeviceIdType.MESH) for n, axes in enumerate(others)]
        for move in moves:
            move.start()
        mine.wait()
        for move in moves:
            move.wait()
        total = sums[0]
        for n in range(1, devices):
            total = total + sums[n]
        out[...] = jnp.broadcast_to(jnp.minimum(1.0, 0.5 * lax.rsqrt(jnp.sum(total) / count + 1e-30)), (8, 128))

    return pl.pallas_call(body, name="clip", in_specs=[IN_HBM], out_specs=pl.BlockSpec(memory_space=pltpu.VMEM), out_shape=shape_of((8, 128), F32),
                          scratch_shapes=[pltpu.VMEM((devices, 8, 128), F32), pltpu.SemaphoreType.DMA, pltpu.SemaphoreType.DMA((devices - 1,)),
                                          pltpu.SemaphoreType.DMA((devices - 1,))],
                          compiler_params=pltpu.CompilerParams(collective_id=next(ids), has_side_effects=True))(own)


def adamw(number, parts, factor, earlier=None, **more):
    count = len(parts)
    halves = lambda a: a.reshape(a.shape[0], 2, a.shape[1] // 2, a.shape[2])
    lay = [halves if part[5] else (lambda a: a) for part in parts]
    ws, ms, vs = ([f(part[n]) for f, part in zip(lay, parts)] for n in range(3))

    def body(*refs):
        f, refs = refs[0][0, 0], refs[1:]
        g, refs = refs[: 6 * count], refs[6 * count :]
        w, m, v = refs[:count], refs[count : 2 * count], refs[2 * count : 3 * count]
        out = refs[-3 * count :]
        for n, (w_, *_, by_rows) in enumerate(parts):
            for side in range(2):
                for part, (at, size) in zip(g[6 * n + 3 * side : 6 * n + 3 * side + 3], strips(w_.shape[1] // (16 if by_rows else 8))):
                    width = part.shape[2]
                    here = (side, slice(at, at + size)) if by_rows else (slice(at, at + size), slice(side * width, (side + 1) * width))
                    x = part[0].astype(F32) * f
                    m2 = 0.9 * m[n][here] + 0.1 * x
                    v2 = 0.95 * v[n][here] + 0.05 * x * x
                    wide = w[n][here].astype(F32)
                    out[n][here] = (wide - 0.02 * (m2 * lax.rsqrt(v2 + 1e-8) + 0.1 * wide)).astype(BF)
                    out[count + n][here] = m2
                    out[2 * count + n][here] = v2

    specs, own = [pl.BlockSpec(memory_space=pltpu.SMEM)], []
    for w, _, _, _, start, by_rows in parts:
        r = w.shape[1] // (16 if by_rows else 8)
        width = w.shape[2] if by_rows else w.shape[2] // 2
        own.append(pl.BlockSpec((None, 2, r, width), lambda i: (number, 0, i, 0)) if by_rows else pl.BlockSpec((None, r, 2 * width), lambda i: (number, i, 0)))
        for side in range(2):
            specs += strip_specs(r, width, lambda axes, i, side=side, start=start:
                                 (axes[0] * (i // 4) + axes[1] * (i // 2 % 2) + axes[2] * (i % 2) + side, start))
    ins = [factor, *[part[3] for part in parts for _ in range(6)], *ws, *ms, *vs]
    own = own * 3
    specs += own
    aliases = {}
    if earlier is not None:
        aliases = {len(ins) + n: n for n in range(3 * count)}
        ins += [f(a) for f, a in zip(lay * 3, earlier)]
        specs += [IN_HBM] * (3 * count)
    outs = [shape_of(a.shape, a.dtype) for a in (*ws, *ms, *vs)]
    got = call(body, "adamw", (8,), ins, specs, outs, own, flops=20 * sum(w.size // w.shape[0] for w in ws), aliases=aliases, **more)
    return [a.reshape(a.shape[0], -1, a.shape[-1]) for a in got]


def solution(mesh):
    def step(x, dy, *arrays):
        weights, moments, squares = (arrays[i : i + 7] for i in (0, 7, 14))
        wq, wk, wv, wo, wg, wu, wd = weights
        count = sum(w.size for w in weights)
        ids = itertools.count()
        tokens, d = x.shape[1:]
        f, half = wg.shape[2], wg.shape[2] // 2
        table = jnp.asarray(angles(tokens))
        x, dy = x[0], dy[0]
        more = dict(ids=ids)
        core_half = lambda a, width, lead=0: to_core(a, (*a.shape[:-1], width), lambda me: (slice(None),) * (a.ndim - 1) + (pl.ds(pl.multiple_of((1 - bit(me, 1)) * width, 128), width),))
        other_head = lambda a: to_core(a, a.shape[1:], lambda me: (1 - bit(me, 1),))

        a0, q0, k0, v0 = qkv(x, 0, wq, wk, wv, table)
        (attn0, lse0), (a0_,) = attend(q0, k0, v0, sends=[to_core(a0)], **more)
        (h1_0, b0, gate0, up0, p0), (attn0_,) = post(x, attn0, 0, wo, wg, wu, sends=[to_core(attn0)], **more)
        (h,), (p0_,) = down(h1_0, p0, 0, wd, sends=[core_half(p0, half)], **more)
        a1, q1, k1, v1 = qkv(h, 1, wq, wk, wv, table)
        (attn1, lse1), (a1_, dy_, b0_) = attend(q1, k1, v1, sends=[to_core(a1), to_core(dy), to_core(b0)], **more)
        (h1_1, b1, p1, by_gu1), (attn1_,) = turnaround(h, attn1, dy, 1, wo, wg, wu, wd, sends=[to_core(attn1)], **more)

        (by_h1, by_attn1), (b1_, p1_, by_gu1_) = ffn_bwd(by_gu1, 1, wg, wu, h1_1, dy, wo, sends=[to_core(b1), core_half(p1, half), core_half(by_gu1, half)], **more)
        d1, (by_h1_,) = for_down(p1, p1_, dy, dy_, sends=[core_half(by_h1, d // 2)], **more)
        gu1, (d1_,) = for_gate_up(b1, b1_, by_gu1, by_gu1_, sends=[first_sends(d1)], **more)
        (d1,) = first_sum(d1, d1_)
        (by_qkv1,), (gu1_, d1_) = attend_bwd(q1, k1, v1, attn1, by_attn1, lse1, table, sends=[first_sends(gu1), second_sends(d1)], **more)
        d1, ss = second_sum(d1, d1_, jnp.zeros((8, 128), F32))
        (gu1,) = first_sum(gu1, gu1_, after=[ss])
        o1, (by_qkv1_,) = for_o(attn1, attn1_, by_h1, by_h1_, sends=[other_head(by_qkv1)], after=[gu1], **more)
        qkv1, (o1_,) = for_qkv(a1, a1_, by_qkv1, by_qkv1_, sends=[first_sends(o1)], **more)
        (by_h,), (qkv1_,) = qkv_bwd(by_qkv1, 1, wq, wk, wv, h, by_h1, sends=[first_sends(qkv1)], **more)
        qkv1, o1 = first_sums([(qkv1, qkv1_), (o1, o1_)])

        (by_gu0,), (by_h_, gu1_) = gate_bwd(by_h, 0, wd, gate0, up0, sends=[to_core(by_h), second_sends(gu1)], eager=True, after=[o1], **more)
        gu1, ss = second_sum(gu1, gu1_, ss)
        d0, (by_gu0_, o1_, qkv1_) = for_down(p0, p0_, by_h, by_h_, sends=[core_half(by_gu0, half), second_sends(o1), second_sends(qkv1)], eager=True, after=[ss], **more)
        oq1, ss = second_sums([(qkv1, qkv1_), (o1, o1_)], ss)
        gu0, (d0_,) = for_gate_up(b0, b0_, by_gu0, by_gu0_, sends=[first_sends(d0)], after=[ss], **more)
        (d0,) = first_sum(d0, d0_)
        (by_h1, by_attn0), (gu0_,) = ffn_bwd(by_gu0, 0, wg, wu, h1_0, by_h, wo, sends=[first_sends(gu0)], after=[d0], eager=True, **more)
        (gu0,) = first_sum(gu0, gu0_)
        (by_qkv0,), (d0_, gu0_, by_h1_) = attend_bwd(q0, k0, v0, attn0, by_attn0, lse0, table, sends=[second_sends(d0), second_sends(gu0), core_half(by_h1, d // 2)], **more)
        o0, (by_qkv0_,) = for_o(attn0, attn0_, by_h1, by_h1_, sends=[other_head(by_qkv0)], **more)
        qkv0, (o0_,) = for_qkv(a0, a0_, by_qkv0, by_qkv0_, sends=[first_sends(o0)], **more)
        (gu0, ss), (qkv0_,) = second_sum(gu0, gu0_, ss, sends=[first_sends(qkv0)], eager=True, **more)
        qkv0, o0 = first_sums([(qkv0, qkv0_), (o0, o0_)])
        (d0, ss), (qkv0_, o0_) = second_sum(d0, d0_, ss, sends=[second_sends(qkv0), second_sends(o0)], eager=True, **more)
        oq0, ss = second_sums([(qkv0, qkv0_), (o0, o0_)], ss)

        factor = clip(ss, count, mesh.shape["dp"], ids)
        everyone = lambda g: lax.all_gather(g, "dp", axis=0)
        starts = {0: 0, 1: wq.shape[2] // 2, 2: (wq.shape[2] + wk.shape[2]) // 2, 3: (wq.shape[2] + wk.shape[2] + wv.shape[2]) // 2, 4: 0, 5: half, 6: 0}

        def update(number, take, g, after, earlier=None):
            return adamw(number, [(weights[n], moments[n], squares[n], g, starts[n], n == 6) for n in take], factor, earlier, after=after)

        d_, gu_, oq_ = (6,), (4, 5), (3, 0, 1, 2)
        d1, gu1 = everyone(d1), everyone(gu1)
        oq1, gu0, d0, oq0, _ = lax.optimization_barrier((oq1, gu0, d0, oq0, factor))
        got_d = update(1, d_, d1, ())
        got_gu = update(1, gu_, gu1, got_d[:1])
        got_oq = update(1, oq_, everyone(oq1), got_gu[:1])
        got_gu = update(0, gu_, everyone(gu0), got_oq[:1], got_gu)
        got_d = update(0, d_, everyone(d0), got_gu[:1], got_d)
        got_oq = update(0, oq_, everyone(oq0), got_d[:1], got_oq)
        new = [None] * 21
        for take, got in ((d_, got_d), (gu_, got_gu), (oq_, got_oq)):
            for i, n in enumerate(take):
                for part in range(3):
                    new[7 * part + n] = got[part * len(take) + i]
        return tuple(new)

    states, all_of = P(("rep", "dp"), None, None), P(None, None, None)
    return jax.shard_map(step, mesh=mesh, in_specs=(states, states) + (all_of,) * 21, out_specs=(P("rep", None, None),) * 21, check_vma=False)
```

```python
import itertools

import jax
import jax.numpy as jnp
import numpy as np
from jax import lax
from jax.experimental import pallas as pl
from jax.experimental.pallas import tpu as pltpu
from jax.sharding import PartitionSpec as P

NAMES = ("wq", "wk", "wv", "wo", "w_gate", "w_up", "w_down")
HEAD = 128
THETA = 10000
NEG = -1e30
HIDDEN = 2 * NEG
LOG2E = 1.4426950408889634
BF, F32 = jnp.bfloat16, jnp.float32
MIB = 2**20


def _dot(a, b, ca, cb):
    return lax.dot_general(a, b, (((ca,), (cb,)), ((), ())), preferred_element_type=F32)


def shape_of(shape, dtype=BF):
    return jax.ShapeDtypeStruct(shape, dtype)


def rows(bt, width):
    return pl.BlockSpec((bt, width), lambda i, *_: (i, 0))


def whole(*shape):
    return pl.BlockSpec(shape, lambda *_: (0,) * len(shape), pipeline_mode=pl.Buffered(1))


def layer_of(number, *shape):
    return pl.BlockSpec((None, *shape), lambda *_: (number,) + (0,) * len(shape), pipeline_mode=pl.Buffered(1))


IN_HBM = pl.BlockSpec(memory_space=pltpu.HBM)


def bit(me, axis):
    return (me // axis) % 2


def across(me, axes):
    return me + sum(axis * (1 - 2 * bit(me, axis)) for axis in axes)


CORE = (1,)


class Send:
    def __init__(self, array, shape, copies):
        self.array, self.result, self.copies = array, shape_of(shape, array.dtype), copies


def everything(me):
    return ()


def to_core(array, shape=None, part=everything):
    return Send(array, shape or array.shape, [(part, everything, CORE)])


def place(ref, at):
    return ref.at[at] if at else ref


class Kept:
    def __init__(self, array, size, axis=0, number=None):
        self.array, self.size, self.axis, self.number = array, size, axis, number
        self.shape = array.shape[-2:]
        self.pieces = self.shape[axis] // size

    def copy(self, source, to, sems, n):
        part = pl.ds(n * self.size, self.size)
        at = (slice(None),) * self.axis + (part,)
        source = source if self.number is None else source.at[self.number]
        return pltpu.make_async_copy(source.at[at], to.at[at], sems.at[n])


WINDOW = 4


def FREE(n, piece):
    pass


def call(body, name, grid, ins, in_specs, outs, out_specs, scratch=(), flops=0, sends=(), ids=None, eager=False, aliases={}, after=(), kept=()):
    size = lambda a: a.size * jnp.dtype(a.dtype).itemsize
    cost = pl.CostEstimate(flops=int(flops), transcendentals=0, bytes_accessed=sum(map(size, ins)) + sum(map(size, outs)))
    n_in, n_kept, n_after, n_s, n_out = len(ins), len(kept), len(after), len(sends), len(outs)
    copies = [(s, c) for s, send in enumerate(sends) for c in send.copies]
    partners = sorted({c[2] for _, c in copies})
    order = [(n, piece) for piece in range(max([k.pieces for k in kept], default=0)) for n, k in enumerate(kept) if piece < k.pieces]

    def whole_body(*refs):
        take = iter(refs)
        part = lambda n: [next(take) for _ in range(n)]
        given, held, _, sources, made, landed = (part(n) for n in (n_in, n_kept, n_after, n_s, n_out, n_s))
        rest = list(take)
        rest, vmem, sems, remote = rest[: len(scratch)], rest[len(scratch) :][:n_kept], rest[len(scratch) + n_kept :][:n_kept], rest[len(scratch) + 2 * n_kept :]
        step, last = pl.program_id(0), grid[0] - 1
        if sends:
            out_sem, in_sem = remote
            me = lax.axis_index("dp")
            barrier = pltpu.get_barrier_semaphore()
            moves = [pltpu.make_async_remote_copy(place(sources[s], a(me)), place(landed[s], b(me)), out_sem.at[n], in_sem.at[n],
                                                  device_id={"dp": across(me, axes)}, device_id_type=pl.DeviceIdType.MESH)
                     for n, (s, (a, b, axes)) in enumerate(copies)]

            def begin():
                pl.semaphore_wait(barrier, len(partners))
                for move in moves:
                    move.start()

            @pl.when(step == 0)
            def _():
                for axes in partners:
                    pl.semaphore_signal(barrier, 1, device_id={"dp": across(me, axes)}, device_id_type=pl.DeviceIdType.MESH)
                if eager or last == 0:
                    begin()

        if kept:
            fetch = [kept[n].copy(held[n], vmem[n], sems[n], piece) for n, piece in order]

            @pl.when(step == 0)
            def _():
                for copy in fetch[:WINDOW]:
                    copy.start()
                done = [0]

                def need(n, piece):
                    while done[0] <= order.index((n, piece)):
                        fetch[done[0]].wait()
                        if done[0] + WINDOW < len(fetch):
                            fetch[done[0] + WINDOW].start()
                        done[0] += 1

                body(need, *given, *vmem, *made, *rest)

            @pl.when(step > 0)
            def _():
                body(FREE, *given, *vmem, *made, *rest)

        elif body is not None:
            body(*given, *made, *rest)
        if sends:
            if not (eager or last == 0):

                @pl.when(step == 0)
                def _():
                    begin()

            @pl.when(step == last)
            def _():
                for move in moves:
                    move.wait()

    more = dict(collective_id=next(ids), has_side_effects=True) if sends else {}
    remote = [pltpu.SemaphoreType.DMA((len(copies),))] * 2 if sends else []
    got = pl.pallas_call(whole_body, name=name, grid=grid, in_specs=[*in_specs, *[IN_HBM] * (n_kept + n_after + n_s)],
                         out_specs=[*out_specs, *[IN_HBM] * n_s], out_shape=[*outs, *[send.result for send in sends]],
                         scratch_shapes=[*scratch, *[pltpu.VMEM(k.shape, k.array.dtype) for k in kept],
                                         *[pltpu.SemaphoreType.DMA((k.pieces,)) for k in kept], *remote],
                         input_output_aliases=aliases, compiler_params=pltpu.CompilerParams(vmem_limit_bytes=60 * MIB, **more), cost_estimate=cost,
                         )(*ins, *[k.array for k in kept], *after, *[send.array for send in sends])
    return (got[:n_out], got[n_out:]) if sends else got


def scale_of(wide):
    return lax.rsqrt(jnp.mean(wide * wide, -1, keepdims=True) + 1e-6)


def through_norm(by_out, wide):
    scale = scale_of(wide)
    return (scale * by_out - wide * (scale * scale * scale * jnp.mean(by_out * wide, -1, keepdims=True))).astype(BF)


def added(a, b):
    return (a.astype(F32) + b.astype(F32)).astype(BF)


def turn(t, cos, sin):
    return t * cos + pltpu.roll(t, HEAD // 2, 1) * sin


def angles(tokens):
    angle = np.arange(tokens)[:, None] * float(THETA) ** (-np.arange(HEAD // 2) / (HEAD // 2))
    return np.concatenate([np.cos(angle), np.sin(angle)], 1).astype(np.float32)


def turns(angles):
    other, first = pltpu.roll(angles, HEAD // 2, 1), lax.broadcasted_iota(jnp.int32, angles.shape, 1) < HEAD // 2
    return jnp.where(first, angles, other), jnp.where(first, -other, angles)


def project(h, wq, wk, wv, table, a, q, k, v):
    wide = h.astype(F32)
    n = (wide * scale_of(wide)).astype(BF)
    a[...] = n
    c, s = turns(table[...])
    for w, out in ((wq, q), (wk, k)):
        for at in range(0, w.shape[1], 256):
            r = _dot(n, w[:, at : at + 256], 1, 0).astype(BF).astype(F32)
            for x in range(0, 256, HEAD):
                out[:, at + x : at + x + HEAD] = turn(r[:, x : x + HEAD], c, s).astype(BF)
    v[...] = _dot(n, wv[...], 1, 0).astype(BF)


def qkv(h, number, wq, wk, wv, table, bt=512):
    (t, d), nq, nk = h.shape, wq.shape[2], wk.shape[2]

    def body(h, wq, wk, wv, table, a, q, k, v):
        project(h[...], wq, wk, wv, table, a, q, k, v)

    return call(body, "qkv", (t // bt,), (h, wq, wk, wv, table),
                [rows(bt, d), layer_of(number, d, nq), layer_of(number, d, nk), layer_of(number, d, nk), rows(bt, HEAD)],
                [shape_of((t, d)), shape_of((t, nq)), shape_of((t, nk)), shape_of((t, nk))],
                [rows(bt, d), rows(bt, nq), rows(bt, nk), rows(bt, nk)], flops=2 * t * d * (nq + 2 * nk))


def _gap(bk, cols, bq):
    return lax.rem(lax.broadcasted_iota(jnp.int32, (bk, cols), 1), bq) - lax.broadcasted_iota(jnp.int32, (bk, cols), 0)


def attend(q, k, v, bq=512, bk=512, **more):
    t, nq = q.shape
    heads, kv = nq // HEAD, k.shape[1] // HEAD
    g = heads // kv
    e, scale = HEAD**-0.5 * LOG2E, HEAD**-0.5

    def body(q, k, v, out, lse, top_s, mix_s, gap_s):
        iq = pl.program_id(0)

        @pl.when(iq == 0)
        def _():
            gap_s[...] = _gap(bk, bq, bq)

        top_s[...] = jnp.full(top_s.shape, NEG, F32)
        mix_s[...] = jnp.zeros(mix_s.shape, F32)
        def block(start, size, first=0, masked=False):
            here = pl.ds(start, size)
            keys = [k[here, i * HEAD : (i + 1) * HEAD] for i in range(kv)]
            ones = jnp.ones((8, size), BF)
            values = [jnp.concatenate([v[here, i * HEAD : (i + 1) * HEAD].T, ones], axis=0) for i in range(kv)]
            scores = [_dot(keys[n // g], q[first:, n * HEAD : (n + 1) * HEAD], 1, 1) for n in range(heads)]
            ok = gap_s[:size, first:] >= (start - iq * bq) if masked else None
            weights, keeps = [], []
            for n, s in enumerate(scores):
                if masked:
                    s = jnp.where(ok, s, HIDDEN)
                old = top_s[n : n + 1, first:]
                top = jnp.maximum(old, s.max(axis=0, keepdims=True))
                top_s[n : n + 1, first:] = top
                weights.append(jnp.exp2((s - top) * e).astype(BF))
                keeps.append(jnp.exp2((old - top) * e))
            for n, (p, keep) in enumerate(zip(weights, keeps)):
                mix_s[n, :, first:] = mix_s[n, :, first:] * keep + _dot(values[n // g], p, 1, 0)

        lax.fori_loop(0, iq, lambda j, _: block(pl.multiple_of(j * bk, bk), bk), None)
        for part in range(2):
            block(pl.multiple_of(iq * bq + part * bq // 2, bq // 2), bq // 2, part * bq // 2, True)
        for n in range(heads):
            total = mix_s[n, HEAD : HEAD + 1, :]
            out[:, n * HEAD : (n + 1) * HEAD] = (mix_s[n, :HEAD, :] * (1 / total)).T.astype(BF)
            lse[n : n + 1, :] = top_s[n : n + 1, :] * scale + jnp.log(total)

    return call(body, "attend", (t // bq,), (q, k, v), [rows(bq, nq), whole(*k.shape), whole(*v.shape)],
                [shape_of((t, nq)), shape_of((heads, t), F32)], [rows(bq, nq), pl.BlockSpec((heads, bq), lambda i: (0, i))],
                [pltpu.VMEM((heads, bq), F32), pltpu.VMEM((heads, HEAD + 8, bq), F32), pltpu.VMEM((bk, bq), jnp.int32)],
                flops=4 * heads * t * t * HEAD, **more)


def post(h, attn, number, wo, wg, wu, bt=256, step=512, **more):
    (t, d), n, f = h.shape, wo.shape[1], wg.shape[2]

    def body(need, h, attn, wo, wg, wu, h1, b, gate, up, p):
        need(0, 0)
        s = added(h[...], _dot(attn[...], wo[...], 1, 0).astype(BF))
        h1[...] = s
        wide = s.astype(F32)
        c = (wide * scale_of(wide)).astype(BF)
        b[...] = c
        for at in range(0, f, step):
            need(1, at // step)
            need(2, at // step)
            x = _dot(c, wg[:, at : at + step], 1, 0)
            y = _dot(c, wu[:, at : at + step], 1, 0)
            gate[:, at : at + step] = x
            up[:, at : at + step] = y
            p[:, at : at + step] = (jax.nn.silu(x) * y).astype(BF)

    return call(body, "post", (t // bt,), (h, attn), [rows(bt, d), rows(bt, n)],
                [shape_of((t, d)), shape_of((t, d)), shape_of((t, f), F32), shape_of((t, f), F32), shape_of((t, f))],
                [rows(bt, d), rows(bt, d), rows(bt, f), rows(bt, f), rows(bt, f)], flops=2 * t * d * (2 * f + n),
                kept=[Kept(wo, n, 0, number), Kept(wg, step, 1, number), Kept(wu, step, 1, number)], **more)


def down(h1, p, number, wd, bt=512, **more):
    (t, d), f = h1.shape, p.shape[1]

    def body(h1, p, wd, out):
        out[...] = added(h1[...], _dot(p[...], wd[...], 1, 0).astype(BF))

    return call(body, "down", (t // bt,), (h1, p, wd), [rows(bt, d), rows(bt, f), layer_of(number, f, d)], [shape_of((t, d))], [rows(bt, d)],
                flops=2 * t * d * f, **more)


def _through_gate(by_p, x, y):
    s = 1 / (1 + jnp.exp(-x))
    act = x * s
    return (by_p * y * (s + act * (1 - s))).astype(BF), (by_p * act).astype(BF)


def gate_bwd(dy, number, wd, gate, up, bt=256, step=512, **more):
    (t, d), f = dy.shape, wd.shape[1]

    def body(need, dy, gate, up, wd, by):
        x = dy[...]
        for at in range(0, f, step):
            need(0, at // step)
            here = slice(at, at + step)
            by_p = _dot(x, wd[here, :], 1, 1).astype(BF).astype(F32)
            by[0, :, here], by[1, :, here] = _through_gate(by_p, gate[:, here], up[:, here])

    return call(body, "gate_bwd", (t // bt,), (dy, gate, up), [rows(bt, d), rows(bt, f), rows(bt, f)],
                [shape_of((2, t, f))], [pl.BlockSpec((2, bt, f), lambda i: (0, i, 0))], flops=2 * t * d * f,
                kept=[Kept(wd, step, 0, number)], **more)


def turnaround(h, attn, dy, number, wo, wg, wu, wd, bt=256, step=512, **more):
    (t, d), n, f = h.shape, wo.shape[1], wg.shape[2]

    def body(need, h, attn, dy, wo, wg, wu, wd, h1, b, p, by):
        need(0, 0)
        s = added(h[...], _dot(attn[...], wo[...], 1, 0).astype(BF))
        h1[...] = s
        wide = s.astype(F32)
        c = (wide * scale_of(wide)).astype(BF)
        b[...] = c
        back = dy[...]
        for at in range(0, f, step):
            here = slice(at, at + step)
            for n in (1, 2, 3):
                need(n, at // step)
            x, y = _dot(c, wg[:, here], 1, 0), _dot(c, wu[:, here], 1, 0)
            p[:, here] = (jax.nn.silu(x) * y).astype(BF)
            by_p = _dot(back, wd[here, :], 1, 1).astype(BF).astype(F32)
            by[0, :, here], by[1, :, here] = _through_gate(by_p, x, y)

    return call(body, "turnaround", (t // bt,), (h, attn, dy), [rows(bt, d), rows(bt, n), rows(bt, d)],
                [shape_of((t, d)), shape_of((t, d)), shape_of((t, f)), shape_of((2, t, f))],
                [rows(bt, d), rows(bt, d), rows(bt, f), pl.BlockSpec((2, bt, f), lambda i: (0, i, 0))],
                flops=2 * t * d * (3 * f + n),
                kept=[Kept(wo, n, 0, number), Kept(wg, step, 1, number), Kept(wu, step, 1, number), Kept(wd, step, 0, number)], **more)


def ffn_bwd(by_gu, number, wg, wu, h1, dy, wo, bt=256, step=256, **more):
    (_, t, f), d, n = by_gu.shape, h1.shape[1], wo.shape[1]

    def body(need, by_gu, h1, dy, wg, wu, wo, by_h, by_attn, by_b):
        for at in range(0, d, step):
            here = slice(at, at + step)
            need(0, at // step)
            need(1, at // step)
            by_b[:, here] = added(_dot(by_gu[0], wg[here, :], 1, 1).astype(BF), _dot(by_gu[1], wu[here, :], 1, 1).astype(BF)).astype(F32)
        total = added(dy[...], through_norm(by_b[...], h1[...].astype(F32)))
        by_h[...] = total
        need(2, 0)
        by_attn[...] = _dot(total, wo[...], 1, 1).astype(BF)

    return call(body, "ffn_bwd", (t // bt,), (by_gu, h1, dy), [pl.BlockSpec((2, bt, f), lambda i: (0, i, 0)), rows(bt, d), rows(bt, d)],
                [shape_of((t, d)), shape_of((t, n))], [rows(bt, d), rows(bt, n)], [pltpu.VMEM((bt, d), F32)], flops=2 * t * d * (2 * f + n),
                kept=[Kept(wg, step, 0, number), Kept(wu, step, 0, number), Kept(wo, n, 0, number)], **more)


def attend_bwd(q, k, v, out, by_out, lse, table, bq=256, bk=512, **more):
    t, nq = q.shape
    heads, kv = nq // HEAD, k.shape[1] // HEAD
    g = heads // kv
    e, scale = HEAD**-0.5 * LOG2E, HEAD**-0.5
    pair = 2
    wide = pair * bq
    strips = range(0, heads, pair)
    width = (g + 2) * HEAD

    def laid(ref, n):
        return jnp.concatenate([ref[:, (n + x) * HEAD : (n + x + 1) * HEAD] for x in range(pair)], axis=0)

    def body(q, k, v, out, by_out, lse, table, res, dq_s, dk_s, dv_s, gap_s):
        iq = pl.program_id(0)

        @pl.when(iq == 0)
        def _():
            gap_s[...] = _gap(bk, wide, bq)
            dk_s[...] = jnp.zeros_like(dk_s)
            dv_s[...] = jnp.zeros_like(dv_s)

        dq_s[...] = jnp.zeros_like(dq_s)
        lses = [jnp.concatenate([lse[n + x : n + x + 1, :] for x in range(pair)], axis=1) * LOG2E for n in strips]
        deltas = [(laid(by_out, n).astype(F32) * laid(out, n).astype(F32)).T.sum(axis=0, keepdims=True) for n in strips]

        def block(start, size, masked=False):
            here = pl.ds(start, size)
            qs, dos = [laid(q, n) for n in strips], [laid(by_out, n) for n in strips]
            keys = [k[here, i * HEAD : (i + 1) * HEAD] for i in range(kv)]
            values = [v[here, i * HEAD : (i + 1) * HEAD] for i in range(kv)]
            scores = [_dot(keys[n // g], x, 1, 1) for n, x in zip(strips, qs)]
            dps = [_dot(values[n // g], x, 1, 1) for n, x in zip(strips, dos)]
            ok = gap_s[:size] >= (start - iq * bq) if masked else None
            for s, n in enumerate(strips):
                i = n // g
                p = jnp.exp2(scores[s] * e - lses[s])
                if masked:
                    p = jnp.where(ok, p, 0.0)
                ds = (p * (dps[s] - deltas[s])).astype(BF)
                dv_s[i, here, :] += _dot(p.astype(BF), dos[s], 1, 0)
                dk_s[i, here, :] += _dot(ds, qs[s], 1, 0)
                dq_s[s] += _dot(keys[i].T, ds, 1, 0)

        whole_blocks = (iq * bq) // bk
        lax.fori_loop(0, whole_blocks, lambda j, _: block(pl.multiple_of(j * bk, bk), bk), None)
        lax.fori_loop(whole_blocks * (bk // bq), iq, lambda j, _: block(pl.multiple_of(j * bq, bq), bq), None)
        block(pl.multiple_of(iq * bq, bq), bq, True)
        at = pl.ds(pl.multiple_of(iq * bq, bq), bq)
        c, s_ = turns(table[at, :])
        for s, n in enumerate(strips):
            got = (dq_s[s] * scale).T.astype(BF).astype(F32)
            for x in range(pair):
                m = (n + x) % g
                res[(n + x) // g, at, m * HEAD : (m + 1) * HEAD] = turn(got[x * bq : (x + 1) * bq], c, -s_).astype(BF)

        @pl.when(iq == pl.num_programs(0) - 1)
        def _():
            for i in range(kv):
                for r in range(0, t, bk):
                    part = pl.ds(r, bk)
                    got = (dk_s[i, part, :] * scale).astype(BF).astype(F32)
                    c, s_ = turns(table[part, :])
                    res[i, part, g * HEAD : (g + 1) * HEAD] = turn(got, c, -s_).astype(BF)
                    res[i, part, (g + 1) * HEAD :] = dv_s[i, part, :].astype(BF)

    return call(body, "attend_bwd", (t // bq,), (q, k, v, out, by_out, lse, table),
                [rows(bq, nq), whole(*k.shape), whole(*v.shape), rows(bq, nq), rows(bq, nq), pl.BlockSpec((heads, bq), lambda i: (0, i)),
                 whole(t, HEAD)],
                [shape_of((kv, t, width))], [whole(kv, t, width)],
                [pltpu.VMEM((heads // pair, HEAD, wide), F32), pltpu.VMEM((kv, t, HEAD), F32), pltpu.VMEM((kv, t, HEAD), F32),
                 pltpu.VMEM((bk, wide), jnp.int32)],
                flops=10 * heads * t * t * HEAD, **more)


def qkv_bwd(by_qkv, number, wq, wk, wv, h, by_h1, bt=512, **more):
    (t, d), kv = h.shape, by_qkv.shape[0]
    nq = wq.shape[2] // kv

    def body(by, wq, wk, wv, h, by_h1, out):
        got = [sum(_dot(by[i, :, a:b], w[:, i * (b - a) : (i + 1) * (b - a)], 1, 1) for i in range(kv)).astype(BF).astype(F32)
               for w, a, b in ((wq, 0, nq), (wk, nq, nq + HEAD), (wv, nq + HEAD, nq + 2 * HEAD))]
        by_a = (got[0] + got[1]).astype(BF).astype(F32) + got[2]
        out[...] = added(by_h1[...], through_norm(by_a.astype(BF).astype(F32), h[...].astype(F32)))

    return call(body, "qkv_bwd", (t // bt,), (by_qkv, wq, wk, wv, h, by_h1),
                [pl.BlockSpec((kv, bt, nq + 2 * HEAD), lambda i: (0, i, 0)), *[layer_of(number, *w.shape[1:]) for w in (wq, wk, wv)],
                 rows(bt, d), rows(bt, d)],
                [shape_of((t, d))], [rows(bt, d)], flops=2 * t * d * (kv * (nq + 2 * HEAD)), **more)


AXES = ((8, 4, 2), (4, 2, 8), (2, 8, 4))


def strips(block):
    tiles = block // 8
    sizes = [8 * ((tiles + 2 - n) // 3) for n in range(3)]
    return [(sum(sizes[:n]), sizes[n]) for n in range(3)]


def gradient(name, blocks, lhs, rhs, lhs_specs, rhs_specs, grid, shape, out_spec, flops, **more):
    def body(l0, l1, r0, r1, out):
        out[...] = (_dot(l0[...], r0[...], 0, 0) + _dot(l1[...], r1[...], 0, 0)).astype(BF)

    got = call(body, name, grid, (*lhs, *rhs), [*lhs_specs, *rhs_specs], [shape_of(shape)], [out_spec], flops=flops, **more)
    made, landed = got if "sends" in more and more["sends"] else (got, [])
    return made[0].reshape(blocks, shape[0] // blocks, shape[1]), landed


def core():
    return lax.axis_index("dp") % 2


def for_down(p, p_other, by, by_other, bn=256, **more):
    (t, half), d = p_other.shape, by.shape[1]
    n = half // bn
    return gradient("for_down", 8, (p, p_other), (by, by_other),
                    [pl.BlockSpec((t, bn), lambda i: (0, core() * n + i)), pl.BlockSpec((t, bn), lambda i: (0, i))], [whole(t, d)] * 2,
                    (n,), (half, d), pl.BlockSpec((bn, d), lambda i: (i, 0)), 4 * t * half * d, **more)


def for_gate_up(b, b_other, by, by_other, bn=256, **more):
    (_, t, half), d = by_other.shape, b.shape[1]
    n = half // bn
    return gradient("for_gate_up", 8, (b, b_other), (by, by_other), [whole(t, d)] * 2,
                    [pl.BlockSpec((None, t, bn), lambda i: (i // n, 0, core() * n + i % n)), pl.BlockSpec((None, t, bn), lambda i: (i // n, 0, i % n))],
                    (2 * n,), (d, 2 * half), pl.BlockSpec((d, bn), lambda i: (0, i)), 8 * t * half * d, **more)


def for_o(attn, attn_other, by, by_other, bn=256, **more):
    (t, n), half = attn.shape, by_other.shape[1]
    return gradient("for_o", 8, (attn, attn_other), (by, by_other), [pl.BlockSpec((t, bn), lambda i: (0, i))] * 2,
                    [pl.BlockSpec((t, half), lambda i: (0, core())), whole(t, half)],
                    (n // bn,), (n, half), pl.BlockSpec((bn, half), lambda i: (i, 0)), 4 * t * half * n, **more)


def for_qkv(a, a_other, by, by_other, bn=256, **more):
    (t, d), width = a.shape, by_other.shape[1]
    return gradient("for_qkv", 8, (a, a_other), (by, by_other), [pl.BlockSpec((t, bn), lambda i: (0, i))] * 2,
                    [pl.BlockSpec((None, t, width), lambda i: (core(), 0, 0), pipeline_mode=pl.Buffered(1)), whole(t, width)],
                    (d // bn,), (d, width), pl.BlockSpec((bn, width), lambda i: (i, 0)), 4 * t * d * width, **more)


def first_sends(g):
    _, r, w = g.shape
    return Send(g, (4, r, w), [(lambda me, a=axes[0], at=at, n=n: (pl.ds(4 * (1 - bit(me, a)), 4), pl.ds(at, n)), lambda me, at=at, n=n: (slice(None), pl.ds(at, n)), axes[:1])
                               for axes, (at, n) in zip(AXES, strips(r))])


def second_sends(g, first=0, width=None):
    _, r, w = g.shape
    w = width or w
    columns = pl.ds(first, w)
    copies = []
    for axes, (at, n) in zip(AXES, strips(r)):
        for turn_ in (1, 2, 3):
            r1, r0 = turn_ // 2, turn_ % 2

            def source(me, axes=axes, r1=r1, r0=r0, at=at, n=n):
                b1, b0 = bit(me, axes[1]), bit(me, axes[2])
                return 2 * (b1 + r1 * (1 - 2 * b1)) + b0 + r0 * (1 - 2 * b0), pl.ds(at, n), columns

            copies.append((source, lambda me, k=turn_ - 1, at=at, n=n: (k, pl.ds(at, n)), axes[1:2] * r1 + axes[2:] * r0))
    return Send(g, (3, r, w), copies)


def block_specs(block, width, index):
    def spec(axes):
        def where(*i):
            first, column = index(axes, *i)
            return first, 0, column // width
        return pl.BlockSpec((1, block, width), where)
    return [spec(axes) for axes in AXES]


def strip_specs(block, width, index):
    def spec(axes, at, n):
        def where(*i):
            first, column = index(axes, *i)
            return first, at, column
        return pl.BlockSpec((pl.Element(1), pl.Element(n), pl.Element(width)), where)
    return [spec(axes, at, n) for axes, (at, n) in zip(AXES, strips(block))]


def first_sum(g, got, **more):
    _, r, w = g.shape
    sending = "sends" in more

    def body(*refs):
        own, (got, out) = refs[:3], refs[3:]
        for part, (at, n) in zip(own, strips(r)):
            mine = part[0, at : at + n] if sending else part[0]
            out[0, at : at + n] = added(mine, got[0, at : at + n])

    def index(axes, i):
        return 4 * bit(lax.axis_index("dp"), axes[0]) + i, 0

    block = pl.BlockSpec((1, r, w), lambda i: (i, 0, 0))
    return call(body, "first_sum", (4,), (g, g, g, got), [*(block_specs if sending else strip_specs)(r, w, index), block], [shape_of((4, r, w))], [block], flops=4 * r * w, **more)


def second_sum(g, got, so_far, first=0, **more):
    _, r, w = got.shape
    sending = "sends" in more
    wide = max(n for n in range(128, min(w, 1024) + 1, 128) if w % n == 0)

    def body(*refs):
        own, (got, so_far, out, squares) = refs[:3], refs[3:]
        total = jnp.zeros((8, 128), F32)
        for part, (at, n) in zip(own, strips(r)):
            here = slice(at, at + n)
            mine = part[0, here] if sending else part[0]
            g = mine.astype(F32) + got[0, here].astype(F32) + got[1, here].astype(F32) + got[2, here].astype(F32)
            g = g.astype(BF)
            out[here] = g
            g = g.astype(F32)
            g = jnp.sum((g * g).reshape(n // 8, 8, wide), axis=0)
            total += sum(g[:, x : x + 128] for x in range(0, wide, 128))

        @pl.when(pl.program_id(0) == 0)
        def _():
            squares[...] = so_far[...]

        squares[...] += total

    def index(axes, j):
        me = lax.axis_index("dp")
        return 2 * bit(me, axes[1]) + bit(me, axes[2]), j * wide if sending else pl.multiple_of(first + j * wide, 128)

    small = pl.BlockSpec((8, 128), lambda j: (0, 0))
    return call(body, "second_sum", (w // wide,), (g, g, g, got, so_far),
                [*(block_specs if sending else strip_specs)(r, wide, index), pl.BlockSpec((3, r, wide), lambda j: (0, 0, j)), small],
                [shape_of((r, w)), shape_of((8, 128), F32)], [pl.BlockSpec((r, wide), lambda j: (0, j)), small],
                flops=4 * r * w, **more)


def second_sums(pairs, so_far):
    sizes = [got.shape[1:] for _, got in pairs]
    starts = [sum(w for _, w in sizes[:n]) for n in range(len(sizes))]
    tall, all_columns = max(r for r, _ in sizes), sum(w for _, w in sizes)

    def body(*refs):
        so_far, out, squares = refs[-3:]
        total = so_far[...]
        for k, ((r, w), start) in enumerate(zip(sizes, starts)):
            columns, own, got = slice(start, start + w), refs[4 * k : 4 * k + 3], refs[4 * k + 3]
            for part, (at, n) in zip(own, strips(r)):
                here = slice(at, at + n)
                g = part[0].astype(F32) + got[0, here].astype(F32) + got[1, here].astype(F32) + got[2, here].astype(F32)
                g = g.astype(BF)
                out[here, columns] = g
                g = g.astype(F32)
                g = jnp.sum((g * g).reshape(n // 8, 8, w), axis=0)
                total += sum(g[:, x : x + 128] for x in range(0, w, 128))
            if r < tall:
                out[r:, columns] = jnp.zeros((tall - r, w), BF)
        squares[...] = total

    def index(axes, j):
        me = lax.axis_index("dp")
        return 2 * bit(me, axes[1]) + bit(me, axes[2]), 0

    ins, specs = [], []
    for (g, got), (r, w) in zip(pairs, sizes):
        ins += [g, g, g, got]
        specs += [*strip_specs(r, w, index), pl.BlockSpec((3, r, w), lambda j: (0, 0, 0))]
    small = pl.BlockSpec((8, 128), lambda j: (0, 0))
    return call(body, "second_sums", (1,), [*ins, so_far], [*specs, small], [shape_of((tall, all_columns)), shape_of((8, 128), F32)],
                [pl.BlockSpec((tall, all_columns), lambda j: (0, 0)), small], flops=4 * tall * all_columns)


def first_sums(pairs):
    sizes = [g.shape[1:] for g, _ in pairs]

    def body(*refs):
        outs = refs[4 * len(pairs) :]
        for k, (r, _) in enumerate(sizes):
            for part, (at, n) in zip(refs[4 * k : 4 * k + 3], strips(r)):
                outs[k][0, at : at + n] = added(part[0], refs[4 * k + 3][0, at : at + n])

    def index(axes, i):
        return 4 * bit(lax.axis_index("dp"), axes[0]) + i, 0

    blocks = [pl.BlockSpec((1, r, w), lambda i: (i, 0, 0)) for r, w in sizes]
    ins, specs = [], []
    for (g, got), (r, w), block in zip(pairs, sizes, blocks):
        ins += [g, g, g, got]
        specs += [*strip_specs(r, w, index), block]
    return call(body, "first_sums", (4,), ins, specs, [shape_of((4, r, w)) for r, w in sizes], blocks, flops=4 * sum(r * w for r, w in sizes))


def clip(own, count, devices, ids):
    others = [tuple(a for a in (8, 4, 2, 1) if n & a) for n in range(1, devices)]

    def body(own, out, sums, local_sem, out_sem, in_sem):
        me = lax.axis_index("dp")
        barrier = pltpu.get_barrier_semaphore()
        mine = pltpu.make_async_copy(own, sums.at[me], local_sem)
        mine.start()
        for axes in others:
            pl.semaphore_signal(barrier, 1, device_id={"dp": across(me, axes)}, device_id_type=pl.DeviceIdType.MESH)
        pl.semaphore_wait(barrier, len(others))
        moves = [pltpu.make_async_remote_copy(own, sums.at[me], out_sem.at[n], in_sem.at[n], device_id={"dp": across(me, axes)},
                                              device_id_type=pl.DeviceIdType.MESH) for n, axes in enumerate(others)]
        for move in moves:
            move.start()
        mine.wait()
        for move in moves:
            move.wait()
        total = sums[0]
        for n in range(1, devices):
            total = total + sums[n]
        out[...] = jnp.broadcast_to(jnp.minimum(1.0, 0.5 * lax.rsqrt(jnp.sum(total) / count + 1e-30)), (8, 128))

    return pl.pallas_call(body, name="clip", in_specs=[IN_HBM], out_specs=pl.BlockSpec(memory_space=pltpu.VMEM), out_shape=shape_of((8, 128), F32),
                          scratch_shapes=[pltpu.VMEM((devices, 8, 128), F32), pltpu.SemaphoreType.DMA, pltpu.SemaphoreType.DMA((devices - 1,)),
                                          pltpu.SemaphoreType.DMA((devices - 1,))],
                          compiler_params=pltpu.CompilerParams(collective_id=next(ids), has_side_effects=True))(own)


def adamw(number, parts, factor, earlier=None, **more):
    count = len(parts)
    halves = lambda a: a.reshape(a.shape[0], 2, a.shape[1] // 2, a.shape[2])
    lay = [halves if part[5] else (lambda a: a) for part in parts]
    ws, ms, vs = ([f(part[n]) for f, part in zip(lay, parts)] for n in range(3))

    def body(*refs):
        f, refs = refs[0][0, 0], refs[1:]
        g, refs = refs[: 6 * count], refs[6 * count :]
        w, m, v = refs[:count], refs[count : 2 * count], refs[2 * count : 3 * count]
        out = refs[-3 * count :]
        for n, (w_, *_, by_rows) in enumerate(parts):
            for side in range(2):
                for part, (at, size) in zip(g[6 * n + 3 * side : 6 * n + 3 * side + 3], strips(w_.shape[1] // (16 if by_rows else 8))):
                    width = part.shape[2]
                    here = (side, slice(at, at + size)) if by_rows else (slice(at, at + size), slice(side * width, (side + 1) * width))
                    x = part[0].astype(F32) * f
                    m2 = 0.9 * m[n][here] + 0.1 * x
                    v2 = 0.95 * v[n][here] + 0.05 * x * x
                    wide = w[n][here].astype(F32)
                    out[n][here] = (wide - 0.02 * (m2 * lax.rsqrt(v2 + 1e-8) + 0.1 * wide)).astype(BF)
                    out[count + n][here] = m2
                    out[2 * count + n][here] = v2

    specs, own = [pl.BlockSpec(memory_space=pltpu.SMEM)], []
    for w, _, _, _, start, by_rows in parts:
        r = w.shape[1] // (16 if by_rows else 8)
        width = w.shape[2] if by_rows else w.shape[2] // 2
        own.append(pl.BlockSpec((None, 2, r, width), lambda i: (number, 0, i, 0)) if by_rows else pl.BlockSpec((None, r, 2 * width), lambda i: (number, i, 0)))
        for side in range(2):
            specs += strip_specs(r, width, lambda axes, i, side=side, start=start:
                                 (axes[0] * (i // 4) + axes[1] * (i // 2 % 2) + axes[2] * (i % 2) + side, start))
    ins = [factor, *[part[3] for part in parts for _ in range(6)], *ws, *ms, *vs]
    own = own * 3
    specs += own
    aliases = {}
    if earlier is not None:
        aliases = {len(ins) + n: n for n in range(3 * count)}
        ins += [f(a) for f, a in zip(lay * 3, earlier)]
        specs += [IN_HBM] * (3 * count)
    outs = [shape_of(a.shape, a.dtype) for a in (*ws, *ms, *vs)]
    got = call(body, "adamw", (8,), ins, specs, outs, own, flops=20 * sum(w.size // w.shape[0] for w in ws), aliases=aliases, **more)
    return [a.reshape(a.shape[0], -1, a.shape[-1]) for a in got]


def solution(mesh):
    def step(x, dy, *arrays):
        weights, moments, squares = (arrays[i : i + 7] for i in (0, 7, 14))
        wq, wk, wv, wo, wg, wu, wd = weights
        count = sum(w.size for w in weights)
        ids = itertools.count()
        tokens, d = x.shape[1:]
        f, half = wg.shape[2], wg.shape[2] // 2
        table = jnp.asarray(angles(tokens))
        x, dy = x[0], dy[0]
        more = dict(ids=ids)
        core_half = lambda a, width, lead=0: to_core(a, (*a.shape[:-1], width), lambda me: (slice(None),) * (a.ndim - 1) + (pl.ds(pl.multiple_of((1 - bit(me, 1)) * width, 128), width),))
        other_head = lambda a: to_core(a, a.shape[1:], lambda me: (1 - bit(me, 1),))

        a0, q0, k0, v0 = qkv(x, 0, wq, wk, wv, table)
        (attn0, lse0), (a0_,) = attend(q0, k0, v0, sends=[to_core(a0)], **more)
        (h1_0, b0, gate0, up0, p0), (attn0_,) = post(x, attn0, 0, wo, wg, wu, sends=[to_core(attn0)], **more)
        (h,), (p0_,) = down(h1_0, p0, 0, wd, sends=[core_half(p0, half)], **more)
        a1, q1, k1, v1 = qkv(h, 1, wq, wk, wv, table)
        (attn1, lse1), (a1_, dy_, b0_) = attend(q1, k1, v1, sends=[to_core(a1), to_core(dy), to_core(b0)], **more)
        (h1_1, b1, p1, by_gu1), (attn1_,) = turnaround(h, attn1, dy, 1, wo, wg, wu, wd, sends=[to_core(attn1)], **more)

        (by_h1, by_attn1), (b1_, p1_, by_gu1_) = ffn_bwd(by_gu1, 1, wg, wu, h1_1, dy, wo, sends=[to_core(b1), core_half(p1, half), core_half(by_gu1, half)], **more)
        d1, (by_h1_,) = for_down(p1, p1_, dy, dy_, sends=[core_half(by_h1, d // 2)], **more)
        gu1, (d1_,) = for_gate_up(b1, b1_, by_gu1, by_gu1_, sends=[first_sends(d1)], **more)
        (d1,) = first_sum(d1, d1_)
        (by_qkv1,), (gu1_, d1_) = attend_bwd(q1, k1, v1, attn1, by_attn1, lse1, table, sends=[first_sends(gu1), second_sends(d1)], eager=True, **more)
        d1, ss = second_sum(d1, d1_, jnp.zeros((8, 128), F32))
        (gu1,) = first_sum(gu1, gu1_, after=[ss])
        o1, (by_qkv1_,) = for_o(attn1, attn1_, by_h1, by_h1_, sends=[other_head(by_qkv1)], after=[gu1], **more)
        qkv1, (o1_,) = for_qkv(a1, a1_, by_qkv1, by_qkv1_, sends=[first_sends(o1)], **more)
        (by_h,), (qkv1_,) = qkv_bwd(by_qkv1, 1, wq, wk, wv, h, by_h1, sends=[first_sends(qkv1)], **more)
        qkv1, o1 = first_sums([(qkv1, qkv1_), (o1, o1_)])

        (by_gu0,), (by_h_, gu1_) = gate_bwd(by_h, 0, wd, gate0, up0, sends=[to_core(by_h), second_sends(gu1)], eager=True, after=[o1], **more)
        gu1, ss = second_sum(gu1, gu1_, ss)
        d0, (by_gu0_, o1_, qkv1_) = for_down(p0, p0_, by_h, by_h_, sends=[core_half(by_gu0, half), second_sends(o1), second_sends(qkv1)], eager=True, after=[ss], **more)
        oq1, ss = second_sums([(qkv1, qkv1_), (o1, o1_)], ss)
        gu0, (d0_,) = for_gate_up(b0, b0_, by_gu0, by_gu0_, sends=[first_sends(d0)], after=[ss], **more)
        (d0,) = first_sum(d0, d0_)
        (by_h1, by_attn0), (gu0_,) = ffn_bwd(by_gu0, 0, wg, wu, h1_0, by_h, wo, sends=[first_sends(gu0)], after=[d0], eager=True, **more)
        (gu0,) = first_sum(gu0, gu0_)
        (by_qkv0,), (d0_, gu0_, by_h1_) = attend_bwd(q0, k0, v0, attn0, by_attn0, lse0, table, sends=[second_sends(d0), second_sends(gu0), core_half(by_h1, d // 2)], eager=True, **more)
        o0, (by_qkv0_,) = for_o(attn0, attn0_, by_h1, by_h1_, sends=[other_head(by_qkv0)], **more)
        qkv0, (o0_,) = for_qkv(a0, a0_, by_qkv0, by_qkv0_, sends=[first_sends(o0)], **more)
        (gu0, ss), (qkv0_,) = second_sum(gu0, gu0_, ss, sends=[first_sends(qkv0)], eager=True, **more)
        qkv0, o0 = first_sums([(qkv0, qkv0_), (o0, o0_)])
        (d0, ss), (qkv0_, o0_) = second_sum(d0, d0_, ss, sends=[second_sends(qkv0), second_sends(o0)], eager=True, **more)
        oq0, ss = second_sums([(qkv0, qkv0_), (o0, o0_)], ss)

        factor = clip(ss, count, mesh.shape["dp"], ids)
        everyone = lambda g: lax.all_gather(g, "dp", axis=0)
        starts = {0: 0, 1: wq.shape[2] // 2, 2: (wq.shape[2] + wk.shape[2]) // 2, 3: (wq.shape[2] + wk.shape[2] + wv.shape[2]) // 2, 4: 0, 5: half, 6: 0}

        def update(number, take, g, after, earlier=None):
            return adamw(number, [(weights[n], moments[n], squares[n], g, starts[n], n == 6) for n in take], factor, earlier, after=after)

        d_, gu_, oq_ = (6,), (4, 5), (3, 0, 1, 2)
        d1, gu1 = everyone(d1), everyone(gu1)
        oq1, gu0, d0, oq0, _ = lax.optimization_barrier((oq1, gu0, d0, oq0, factor))
        got_d = update(1, d_, d1, ())
        got_gu = update(1, gu_, gu1, got_d[:1])
        got_oq = update(1, oq_, everyone(oq1), got_gu[:1])
        got_gu = update(0, gu_, everyone(gu0), got_oq[:1], got_gu)
        got_d = update(0, d_, everyone(d0), got_gu[:1], got_d)
        got_oq = update(0, oq_, everyone(oq0), got_d[:1], got_oq)
        new = [None] * 21
        for take, got in ((d_, got_d), (gu_, got_gu), (oq_, got_oq)):
            for i, n in enumerate(take):
                for part in range(3):
                    new[7 * part + n] = got[part * len(take) + i]
        return tuple(new)

    states, all_of = P(("rep", "dp"), None, None), P(None, None, None)
    return jax.shard_map(step, mesh=mesh, in_specs=(states, states) + (all_of,) * 21, out_specs=(P("rep", None, None),) * 21, check_vma=False)
```
